32 devices in a mesh: mem: 4 (over z), lat: 8 (over y, x, core).
Axes of the slice: x: 2, y: 2, z: 4, core: 2. Of those that a mesh axis runs over, the one named last changes fastest.
Arguments:
- members: float32 [32, 2, 512, 1024], P('mem', None, 'lat'), may hold values from -0.75 to 0.75
- lat_root: float32 [512, 512], replicated, may hold values from -1 to 2
- lon_root: float32 [1024, 1024], replicated, may hold values from -1 to 2
- innovation: float32 [512, 256], P('lat', 'mem'), may hold values from -6 to 6
- obs_weight: float32 [512, 256], P('lat', 'mem'), may hold values from 0.5 to 4
- obs_mask: int32 [512, 256], P('lat', 'mem'), may hold values 0 or 1
- obs_cell: int32 [512, 256], P('lat', 'mem'), may hold values from 0 to 2047, as said below
Outputs:
- increment: float32 [2, 512, 1024], P(None, 'lat', 'mem')
- control: float32 [32, 2, 512, 1024], P('mem', None, 'lat')
The draws below stay inside these ranges and needn't reach their ends.
Inputs may be any that keep to these rules, and one draw needn't show every extreme that they name: `obs_cell`: entry e in column c has (e % 1024) // 256 equal to c // 64.
All inputs are finite; a program needn't handle non-finite values. No bound on the sum of `obs_mask` on one device may be relied on, other than what follows from the above.
Results may differ from the reference program's by a relative error of at most 0.0003.
Values sent between devices are 32-bit elements; how exact they have to be, the bound alone decides.
No kernel may reach another device: no remote copies, remote signals or barrier semaphores. Data moves between devices by JAX's collectives and lax.ppermute only.
A program may use at most 128 MiB of HBM per device.

```python
import math
import jax
import jax.numpy as jnp
from jax import lax

NLAT = 512
NLON = 1024
LEV = 2
INNER = 2
OBS_ROW = 256
MEMBERS = 32
N_MEM = 4


def root_matrix(key, order):
    noise = jnp.clip(jax.random.normal(key, (order, order), jnp.float32), -4.0, 4.0)
    return jnp.eye(order, dtype=jnp.float32) + 0.5 * noise / math.sqrt(order)


def draw_lat_root(key, part):
    return root_matrix(jax.random.fold_in(key, 11), NLAT)


def draw_lon_root(key, part):
    return root_matrix(jax.random.fold_in(key, 13), NLON)


def draw_obs_cell(key, part):
    per_block = OBS_ROW // N_MEM
    quarter = NLON // N_MEM
    column_block = jnp.arange(OBS_ROW, dtype=jnp.int32) // per_block
    offset = jax.random.randint(jax.random.fold_in(key, 21), (NLAT, OBS_ROW), 0, quarter, dtype=jnp.int32)
    level = jax.random.randint(jax.random.fold_in(key, 23), (NLAT, OBS_ROW), 0, LEV, dtype=jnp.int32)
    return (level * NLON + column_block[None, :] * quarter + offset).astype(jnp.int32)


def plant(drawn, stream_key, low, largest):
    shape = drawn.shape
    place = [jax.random.randint(jax.random.fold_in(stream_key, axis), (), 0, shape[axis]) for axis in range(len(shape))]
    drawn = drawn.at[tuple(place)].set(low)
    longest = shape.index(max(shape))
    place[longest] = (place[longest] + 1) % shape[longest]
    return drawn.at[tuple(place)].set(largest)


def level_of(stream_key, shape, split, smallest, high):
    gain = 1.0
    for position, blocks in split:
        steps = jax.random.uniform(jax.random.fold_in(jax.random.fold_in(stream_key, 6), position), (blocks,), jnp.float32, smallest / len(split), high / len(split))
        gain = gain * jnp.repeat(jnp.exp(steps), shape[position] // blocks).reshape((-1,) + (1,) * (len(shape) - 1 - position))
    return gain


def bell_draw(rng, shape, width, most, pieces=(), kind=jnp.bfloat16):
    gain = level_of(rng, shape, pieces, -0.22, 0.18) if pieces else 1.0
    result = jax.random.normal(rng, shape, jnp.float32) * width * gain
    return jnp.minimum(jnp.maximum(result, -most), most).astype(kind)


def setup_inputs(seed: int = 0) -> dict:
    key_list = jax.random.split(jax.random.key(seed), 8)
    members = bell_draw(key_list[0], (MEMBERS, LEV, NLAT, NLON), 0.125, 0.75, ((0, 4), (2, 8)), jnp.float32)
    lat_root = draw_lat_root(jax.random.fold_in(key_list[7], 71), 0)
    lon_root = draw_lon_root(jax.random.fold_in(key_list[7], 71), 0)
    innovation = bell_draw(key_list[3], (NLAT, OBS_ROW), 1.0, 6.0, ((0, 8), (1, 4)), jnp.float32)
    obs_weight = jnp.clip(jnp.exp(math.log(4.0) - 2.0794415 * jax.random.uniform(key_list[4], (NLAT, OBS_ROW), jnp.float32) ** level_of(key_list[4], (NLAT, OBS_ROW), ((0, 8), (1, 4)), -0.2, 0.2)), 0.5, 4.0)
    obs_mask = plant((jax.random.randint(key_list[5], (NLAT, OBS_ROW), 0, 4) < 3).astype(jnp.int32), jax.random.fold_in(key_list[5], 1), 0, 1)
    obs_cell = draw_obs_cell(jax.random.fold_in(key_list[7], 71), 0)
    return dict(members=members, lat_root=lat_root, lon_root=lon_root, innovation=innovation, obs_weight=obs_weight, obs_mask=obs_mask, obs_cell=obs_cell)


HIGH = lax.Precision.HIGHEST


def root(field, lat_root, lon_root):
    inner = jnp.einsum("ij,mljn->mlin", lat_root, field, precision=HIGH)
    return jnp.einsum("mlin,kn->mlik", inner, lon_root, precision=HIGH)


def root_t(field, lat_root, lon_root):
    inner = jnp.einsum("ji,mljn->mlin", lat_root, field, precision=HIGH)
    return jnp.einsum("mlin,nk->mlik", inner, lon_root, precision=HIGH)


def reference(members, lat_root, lon_root, innovation, obs_weight, obs_mask, obs_cell):
    weights = obs_weight * obs_mask.astype(jnp.float32)
    row_ids = jnp.broadcast_to(jnp.arange(NLAT, dtype=jnp.int32)[:, None], obs_cell.shape)

    def forward(control):
        return jnp.sum(members * root(control, lat_root, lon_root), axis=0)

    def observe(field):
        flat = field.transpose(1, 0, 2).reshape(NLAT, LEV * NLON)
        return jnp.take_along_axis(flat, obs_cell, axis=1)

    def spread(values):
        flat = jnp.zeros((NLAT, LEV * NLON), jnp.float32).at[row_ids, obs_cell].add(values)
        field = flat.reshape(NLAT, LEV, NLON).transpose(1, 0, 2)
        return root_t(members * field[None], lat_root, lon_root)

    gradient = spread(-(weights * innovation))
    control = jnp.zeros_like(gradient)
    increment = jnp.zeros((LEV, NLAT, NLON), jnp.float32)
    norm_now = jnp.sum(gradient * gradient)
    for step in range(INNER):
        image = forward(gradient)
        curved = gradient + spread(weights * observe(image))
        length = norm_now / jnp.sum(gradient * curved)
        control = control - length * gradient
        increment = increment - length * image
        gradient = gradient - length * curved
        norm_now = jnp.sum(gradient * gradient)
    return increment, control
```

```python
import functools
import jax
import jax.numpy as jnp
from jax import lax
from jax.experimental import pallas as pl
from jax.experimental.pallas import tpu as pltpu
from jax.sharding import PartitionSpec as P

INNER = 2
LANES = 128
HIGHEST = lax.Precision.HIGHEST
F32 = jnp.float32
BF16 = jnp.bfloat16
VMEM_LIMIT = 60 * 1024 * 1024


VM = pl.BlockSpec(memory_space=pltpu.VMEM)
ANY = pl.BlockSpec(memory_space=pl.ANY)


def params():
    return pltpu.CompilerParams(vmem_limit_bytes=VMEM_LIMIT)


def cost(flops, nbytes):
    return pl.CostEstimate(flops=flops, bytes_accessed=nbytes, transcendentals=0)


def take_lanes(values, index):
    return jnp.take_along_axis(values, index, axis=1, mode="promise_in_bounds")


def split(value):
    high = value.astype(BF16)
    return high, (value - high.astype(F32)).astype(BF16)


def split_outside(value):
    high = lax.reduce_precision(value, exponent_bits=8, mantissa_bits=7)
    return high.astype(BF16), (value - high).astype(BF16)


def lane_iota(rows):
    return lax.broadcasted_iota(jnp.int32, (rows, LANES), 1)


def sort_kernel(width, cell_ref, weight_ref, value_ref, out_ref):
    rows = cell_ref.shape[0]
    lane = lane_iota(rows)
    key = cell_ref[...] * width + lane % width
    block = 2
    while block <= width:
        hop = block // 2
        while hop:
            other = take_lanes(key, lane ^ hop)
            keep_low = ((lane & block) == 0) == ((lane & hop) == 0)
            if block == width:
                keep_low = (lane & hop) == 0
            key = jnp.where(keep_low, jnp.minimum(key, other), jnp.maximum(key, other))
            hop //= 2
        block *= 2
    slot = key % width
    inside = lane < width
    out_ref[0] = jnp.where(inside, (key // width).astype(F32), 0.0)
    out_ref[1] = jnp.where(inside, take_lanes(weight_ref[...], slot), 0.0)
    out_ref[2] = jnp.where(inside, take_lanes(value_ref[...], slot), 0.0)


def run_totals(cells, values, width):
    hop = 1
    while hop < width:
        same = pltpu.roll(cells, LANES - hop, axis=1) == cells
        values = values + jnp.where(same, pltpu.roll(values, LANES - hop, axis=1), 0.0)
        hop *= 2
    return values


def pick_cells(cells, read, width, levels, quarter, lon):
    per = LANES // width
    halves = quarter // LANES
    lane = lane_iota(cells.shape[0])
    position = cells % LANES
    kind = (cells // lon) * halves + (cells % quarter) // LANES
    out = jnp.zeros(cells.shape, F32)
    for side in range(per):
        here = (lane // width) == side
        for level in range(levels):
            for half in range(halves):
                got = take_lanes(read(side, level, half), position)
                out = jnp.where(here & (kind == level * halves + half), got, out)
    return out


def observe_kernel(width, blocks_ref, members_ref, obs_ref, local_ref, seen_ref):
    nblocks, _, rows, _ = blocks_ref.shape
    count, levels, _, lon = members_ref.shape
    per = LANES // width
    quarter = lon // nblocks
    for group in range(nblocks // per):
        columns = slice(group * LANES, (group + 1) * LANES)
        for kind in range(3):
            total = blocks_ref[group * per, kind]
            for side in range(1, per):
                total = total + pltpu.roll(blocks_ref[group * per + side, kind], side * width, axis=1)
            obs_ref[kind, :, columns] = total
        cells = obs_ref[0, :, columns].astype(jnp.int32)
        local_ref[0, :, columns] = obs_ref[0, :, columns]
        local_ref[1, :, columns] = run_totals(cells, obs_ref[2, :, columns], width)

    step = 8

    def one(index, carry):
        member = index // (rows // step)
        start = pl.multiple_of((index % (rows // step)) * step, step)
        for group in range(nblocks // per):
            columns = slice(group * LANES, (group + 1) * LANES)
            cells = obs_ref[0, pl.ds(start, step), columns].astype(jnp.int32)

            def read(side, level, half):
                first = (group * per + side) * quarter + half * LANES
                return members_ref[member, level, pl.ds(start, step), first : first + LANES]

            seen_ref[member, pl.ds(start, step), columns] = pick_cells(
                cells, read, width, levels, quarter, lon
            )
        return carry

    lax.fori_loop(0, count * (rows // step), one, 0, unroll=2)


def inverse_kernel(width, levels, lon, nlat_blocks, *refs):
    local_refs, (inverse_ref, value_ref) = refs[:nlat_blocks], refs[nlat_blocks:]
    rows = local_refs[0].shape[1]
    slots = local_refs[0].shape[2]
    nblocks = slots // width
    quarter = lon // nblocks
    per = LANES // width
    step = 8
    for number, local_ref in enumerate(local_refs):
        value_ref[number * rows : (number + 1) * rows, :] = local_ref[1]

        def one(index, carry, local_ref=local_ref, number=number):
            start = pl.multiple_of(index * step, step)
            target_row = pl.multiple_of(number * rows + index * step, step)
            lane = lane_iota(step)
            for block in range(nblocks):
                group, offset = block // per, (block % per) * width
                cells = local_ref[0, pl.ds(start, step), group * LANES : (group + 1) * LANES].astype(jnp.int32)
                nothing = (offset - 1) % LANES
                for level in range(levels):
                    for half in range(quarter // LANES):
                        target = lane + (level * lon + block * quarter + half * LANES)
                        place = jnp.full((step, LANES), offset, jnp.int32)
                        hop = width // 2
                        while hop:
                            ahead = place + (hop - 1)
                            place = jnp.where(take_lanes(cells, ahead) < target, place + hop, place)
                            hop //= 2
                        found = take_lanes(cells, place) == target
                        inverse_ref[
                            level * nblocks + block,
                            pl.ds(target_row, step),
                            half * LANES : (half + 1) * LANES,
                        ] = jnp.where(found, place, nothing)
            return carry

        lax.fori_loop(0, rows // step, one, 0)


def apply_kernel(width, levels, nlat_blocks, first, *refs):
    seen_refs = refs[:nlat_blocks]
    refs = refs[nlat_blocks:]
    if not first:
        pay_refs = refs[:nlat_blocks]
        refs = refs[nlat_blocks:]
    (value_ref, inverse_ref, lhs_ref, local_ref, cn_high_ref, cn_low_ref, members_ref) = refs[:7]
    refs = refs[7:]
    if first:
        (seen_out_ref, image_ref, back_high_ref, back_low_ref) = refs[:4]
        refs = refs[4:]
    else:
        (seen_out_ref, image_ref, back_high_ref, back_low_ref, length_ref) = refs[:5]
        refs = refs[5:]
    (seen, value, inverse, cn_high, cn_low, members, x_high, x_low, w_high, w_low, sems, seen_sems, inv_sems) = refs
    count, nlat, slots = seen.shape
    rows = nlat // nlat_blocks
    nblocks = slots // width
    per = LANES // width
    nchunks = levels * nblocks
    quarter = inverse.shape[2]
    lon = quarter * nblocks

    def seen_copies(member):
        return [
            pltpu.make_async_copy(
                ref.at[member], seen.at[member, pl.ds(number * rows, rows)], seen_sems.at[member, number]
            )
            for number, ref in enumerate(seen_refs)
        ]

    def inverse_copy(chunk):
        return pltpu.make_async_copy(inverse_ref.at[chunk], inverse.at[chunk], inv_sems.at[chunk])

    late = [
        pltpu.make_async_copy(cn_high_ref, cn_high, sems.at[0]),
        pltpu.make_async_copy(cn_low_ref, cn_low, sems.at[1]),
        pltpu.make_async_copy(members_ref, members, sems.at[2]),
    ]
    for copy in seen_copies(0):
        copy.start()
    for chunk in range(nchunks):
        inverse_copy(chunk).start()
    for member in range(1, count):
        for copy in seen_copies(member):
            copy.start()
    for copy in late:
        copy.start()

    if first:
        value[...] = value_ref[...]
    else:
        top = jnp.zeros((1, slots), F32)
        bottom = jnp.zeros((1, slots), F32)
        for ref in pay_refs:
            top = top + ref[rows : rows + 1, :]
            bottom = bottom + ref[rows + 1 : rows + 2, :]
        length = jnp.sum(top, axis=1, keepdims=True) / jnp.sum(bottom, axis=1, keepdims=True)
        length_ref[...] = jnp.broadcast_to(length, length_ref.shape)
        for number, ref in enumerate(pay_refs):
            part = slice(number * rows, (number + 1) * rows)
            old = value_ref[part, :]
            value[part, :] = old - length * (old + ref[:rows, :])

    tall = 16
    lane = lane_iota(tall)

    def build(member, chunk, slot):
        block = chunk % nblocks
        group, offset = block // per, (block % per) * width
        columns = slice(group * LANES, (group + 1) * LANES)
        inside = (lane >= offset) & (lane < offset + width)
        for start in range(0, nlat, tall):
            part = slice(start, start + tall)
            source = jnp.where(inside, seen[member, part, columns] * value[part, columns], 0.0)
            for half in range(quarter // LANES):
                cols = slice(half * LANES, (half + 1) * LANES)
                high, low = split(take_lanes(source, inverse[chunk, part, cols]))
                x_high[slot, part, cols] = high
                x_low[slot, part, cols] = low

    def multiply(member, chunk, slot):
        level, block = chunk // nblocks, chunk % nblocks
        full = jnp.dot(lhs_ref[...], x_high[slot], preferred_element_type=F32)
        rest = jnp.dot(lhs_ref[: 2 * rows, :], x_low[slot], preferred_element_type=F32)
        both = full[: 2 * rows] + full[2 * rows :] + rest
        high, low = split(both[:rows])
        where = pl.ds(pl.multiple_of((member * levels + level) * rows, rows), rows)
        cols = slice(block * quarter, (block + 1) * quarter)
        w_high[where, cols] = high
        w_low[where, cols] = low
        high, low = split(both[rows:])
        back_high_ref[where, cols] = high
        back_low_ref[where, cols] = low

    for copy in seen_copies(0):
        copy.wait()
    for chunk in range(nchunks):
        inverse_copy(chunk).wait()
    build(0, 0, 0)

    def one(member, carry):
        for chunk in range(nchunks):
            if chunk + 1 < nchunks:
                build(member, chunk + 1, (chunk + 1) % 2)
            else:
                after = jnp.minimum(member + 1, count - 1)

                @pl.when(member + 1 < count)
                def _():
                    for copy in seen_copies(after):
                        copy.wait()

                build(after, 0, nchunks % 2)
            multiply(member, chunk, chunk % 2)
        return carry

    lax.fori_loop(0, count, one, 0)

    for copy in late:
        copy.wait()
    pair = min(2, count)
    tile = 2 * LANES
    deep = pair * levels * rows

    for column in range(lon // tile):
        cols = slice(column * tile, (column + 1) * tile)
        total = None
        for group in range(count // pair):
            part = slice(group * deep, (group + 1) * deep)
            product = (
                jnp.dot(w_high[part, :], cn_high[:, cols], preferred_element_type=F32)
                + jnp.dot(w_low[part, :], cn_high[:, cols], preferred_element_type=F32)
                + jnp.dot(w_high[part, :], cn_low[:, cols], preferred_element_type=F32)
            )
            for extra in range(pair):
                member = group * pair + extra
                for level in range(levels):
                    begin = (extra * levels + level) * rows
                    term = members[member, level, :, cols] * product[begin : begin + rows]
                    if member == 0:
                        image_ref[level, :, cols] = term
                    else:
                        image_ref[level, :, cols] += term

    step = 8
    for start in range(0, rows, step):
        part = slice(start, start + step)
        for group in range(nblocks // per):
            columns = slice(group * LANES, (group + 1) * LANES)
            cells = local_ref[0, part, columns].astype(jnp.int32)

            def read(side, level, half):
                begin = (group * per + side) * quarter + half * LANES
                return image_ref[level, part, begin : begin + LANES]

            seen_out_ref[part, columns] = pick_cells(cells, read, width, levels, quarter, lon)


def answer_kernel(width, nparts, *refs):
    parts, (obs_ref, pay_ref, seen_ref) = refs[:nparts], refs[nparts:]
    rows = obs_ref.shape[1]
    seen = parts[0][...]
    for part in parts[1:]:
        seen = seen + part[...]
    seen_ref[...] = seen
    weighted = obs_ref[1] * seen
    value = obs_ref[2]
    for group in range(seen.shape[1] // LANES):
        columns = slice(group * LANES, (group + 1) * LANES)
        cells = obs_ref[0, :, columns].astype(jnp.int32)
        pay_ref[:rows, columns] = run_totals(cells, weighted[:, columns], width)
    pay_ref[rows:, :] = jnp.zeros((8, seen.shape[1]), F32)
    pay_ref[rows : rows + 1, :] = jnp.sum(value * seen, axis=0, keepdims=True)
    pay_ref[rows + 1 : rows + 2, :] = jnp.sum(seen * (value + weighted), axis=0, keepdims=True)


def last_kernel(nparts, *refs):
    parts, (obs_ref, before_ref, length_ref, dots_ref) = refs[:nparts], refs[nparts:]
    seen = parts[0][...]
    for part in parts[1:]:
        seen = seen + part[...]
    weight, value = obs_ref[1], obs_ref[2]
    length = length_ref[:1, :1]
    value = value - length * (value + weight * before_ref[...])
    dots_ref[...] = jnp.zeros(dots_ref.shape, F32)
    dots_ref[:1, :] = jnp.sum(value * seen, axis=0, keepdims=True)
    dots_ref[1:2, :] = jnp.sum(seen * (value + weight * seen), axis=0, keepdims=True)


def product_kernel(a_high_ref, a_low_ref, b_high_ref, b_low_ref, out_ref):
    out_ref[...] = (
        jnp.dot(a_high_ref[...], b_high_ref[...], preferred_element_type=F32)
        + jnp.dot(a_low_ref[...], b_high_ref[...], preferred_element_type=F32)
        + jnp.dot(a_high_ref[...], b_low_ref[...], preferred_element_type=F32)
    )


def product(a_high, a_low, b_high, b_low):
    rows, deep = a_high.shape
    wide = b_high.shape[1]
    tile = 2 * LANES
    whole = pl.BlockSpec((rows, deep), lambda i: (0, 0))
    panel = pl.BlockSpec((deep, tile), lambda i: (0, i))
    return pl.pallas_call(
        product_kernel,
        grid=(wide // tile,),
        in_specs=[whole, whole, panel, panel],
        out_specs=pl.BlockSpec((rows, tile), lambda i: (0, i)),
        out_shape=jax.ShapeDtypeStruct((rows, wide), F32),
        compiler_params=params(),
        cost_estimate=cost(6 * rows * deep * wide, 4 * (rows * deep + deep * wide + rows * wide)),
        name="lon_product",
    )(a_high, a_low, b_high, b_low)


def per_device(members, lat_root, lon_root, innovation, obs_weight, obs_mask, obs_cell):
    count, levels, rows, lon = members.shape
    nmem, nlat_dev = lax.axis_size("mem"), lax.axis_size("lat")
    nlat = lat_root.shape[0]
    width = obs_cell.shape[1]
    slots = width * nmem
    quarter = lon // nmem
    me_lat, me_mem = lax.axis_index("lat"), lax.axis_index("mem")
    shape = jax.ShapeDtypeStruct

    def swap(value, bits):
        return lax.ppermute(value, "lat", [(i, i ^ bits) for i in range(nlat_dev)])

    def over_lat(value):
        own = [value] + [swap(value, bits) for bits in range(2, nlat_dev, 2)]
        return own + [swap(block, 1) for block in own]

    order = list(range(0, nlat_dev, 2)) + [bits + 1 for bits in range(0, nlat_dev, 2)]

    def around_mem(value):
        return [value] + [
            lax.ppermute(value, "mem", [(i, (i + hop) % nmem) for i in range(nmem)]) for hop in range(1, nmem)
        ]

    weights = obs_weight * obs_mask.astype(F32)
    pad = ((0, 0), (0, LANES - width))
    block = pl.pallas_call(
        functools.partial(sort_kernel, width),
        in_specs=[VM] * 3,
        out_specs=VM,
        out_shape=shape((3, rows, LANES), F32),
        compiler_params=params(),
        name="sort_slots",
    )(jnp.pad(obs_cell, pad), jnp.pad(weights, pad), jnp.pad(-(weights * innovation), pad))
    around = jnp.stack(around_mem(block))
    around = jnp.concatenate([around[:1], around[:0:-1]])
    around = lax.dynamic_slice_in_dim(jnp.concatenate([around, around]), nmem - me_mem, nmem)
    obs, local, seen = pl.pallas_call(
        functools.partial(observe_kernel, width),
        in_specs=[VM] * 2,
        out_specs=[VM] * 3,
        out_shape=[shape((3, rows, slots), F32), shape((2, rows, slots), F32), shape((count, rows, slots), F32)],
        compiler_params=params(),
        cost_estimate=cost(10**8, 4 * members.size),
        name="members_at_slots",
    )(around, members)

    locals_ = over_lat(local)
    seens = over_lat(seen)

    lat_rows = lax.dynamic_slice_in_dim(lat_root, me_lat * rows, rows, axis=0)
    lat_columns = lax.dynamic_slice_in_dim(lat_root, me_lat * rows, rows, axis=1)
    lat_cov = jnp.einsum("ij,kj->ik", lat_rows, lat_root, precision=HIGHEST)
    both = jnp.concatenate([lat_cov, lat_columns.T])
    both = jnp.concatenate(
        [lax.dynamic_slice_in_dim(both, (me_lat ^ bits) * rows, rows, axis=1) for bits in order], axis=1
    )
    lhs = jnp.concatenate(split_outside(both))
    cn_high, cn_low = split_outside(jnp.einsum("ij,kj->ik", lon_root, lon_root, precision=lax.Precision.HIGH))
    lon_high, lon_low = split_outside(lon_root)

    nchunks = levels * nmem
    inverse, value = pl.pallas_call(
        functools.partial(inverse_kernel, width, levels, lon, nlat_dev),
        in_specs=[VM] * nlat_dev,
        out_specs=[VM] * 2,
        out_shape=[shape((nchunks, nlat, quarter), jnp.int32), shape((nlat, slots), F32)],
        compiler_params=params(),
        cost_estimate=cost(10**9, 4 * nlat * lon * levels),
        name="inverse",
    )(*locals_)

    tall = count * levels * rows

    def apply(pays):
        first = pays is None
        outs = [
            shape((rows, slots), F32),
            shape((levels, rows, lon), F32),
            shape((tall, lon), BF16),
            shape((tall, lon), BF16),
        ]
        if not first:
            outs.append(shape((8, LANES), F32))
        return pl.pallas_call(
            functools.partial(apply_kernel, width, levels, nlat_dev, first),
            in_specs=[ANY] * nlat_dev
            + ([] if first else [VM] * nlat_dev)
            + [VM, ANY, VM, VM, ANY, ANY, ANY],
            out_specs=[VM] * len(outs),
            out_shape=outs,
            scratch_shapes=[
                pltpu.VMEM((count, nlat, slots), F32),
                pltpu.VMEM((nlat, slots), F32),
                pltpu.VMEM((nchunks, nlat, quarter), jnp.int32),
                pltpu.VMEM((lon, lon), BF16),
                pltpu.VMEM((lon, lon), BF16),
                pltpu.VMEM(members.shape, F32),
                pltpu.VMEM((2, nlat, quarter), BF16),
                pltpu.VMEM((2, nlat, quarter), BF16),
                pltpu.VMEM((tall, lon), BF16),
                pltpu.VMEM((tall, lon), BF16),
                pltpu.SemaphoreType.DMA((3,)),
                pltpu.SemaphoreType.DMA((count, nlat_dev)),
                pltpu.SemaphoreType.DMA((nchunks,)),
            ],
            compiler_params=params(),
            cost_estimate=cost(12 * tall * lon * (nlat + lon), 30 * 2**20),
            name="apply_first" if first else "apply_next",
        )(*seens, *([] if first else pays), value, inverse, lhs, local, cn_high, cn_low, members)

    def to_quarters(image):
        parts = image.reshape(levels, rows, nmem, quarter).transpose(2, 0, 1, 3)

        def part(hop):
            return lax.dynamic_index_in_dim(parts, (me_mem + hop) % nmem, keepdims=False)

        total = part(0)
        for hop in range(1, nmem):
            total = total + lax.ppermute(part(hop), "mem", [(i, (i + hop) % nmem) for i in range(nmem)])
        return total

    partial0, image0, back_high, back_low = apply(None)
    pay, seen0 = pl.pallas_call(
        functools.partial(answer_kernel, width, nmem),
        in_specs=[VM] * (nmem + 1),
        out_specs=[VM] * 2,
        out_shape=[shape((rows + 8, slots), F32), shape((rows, slots), F32)],
        compiler_params=params(),
        name="answer",
    )(*around_mem(partial0), obs)
    pays = over_lat(pay)
    grad0 = product(back_high, back_low, lon_high, lon_low)

    partial1, image1, back_high, back_low, length0 = apply(pays)
    dots = pl.pallas_call(
        functools.partial(last_kernel, nmem),
        in_specs=[VM] * (nmem + 3),
        out_specs=VM,
        out_shape=shape((8, slots), F32),
        compiler_params=params(),
        name="last_dots",
    )(*around_mem(partial1), obs, seen0, length0)
    for bits in [2**k for k in range((nlat_dev - 1).bit_length())]:
        dots = dots + swap(dots, bits)
    grad1 = product(back_high, back_low, lon_high, lon_low)
    quarter0, quarter1 = to_quarters(image0), to_quarters(image1)
    sums = jnp.sum(dots, axis=1)
    length1 = sums[0] / sums[1]
    length0 = length0[0, 0]
    increment = -(length0 * quarter0 + length1 * quarter1)
    control = -(length0 * grad0 + length1 * grad1)
    return increment, control.reshape(members.shape)


def solution(mesh):
    return jax.shard_map(
        per_device,
        mesh=mesh,
        in_specs=(
            P("mem", None, "lat", None),
            P(),
            P(),
            P("lat", "mem"),
            P("lat", "mem"),
            P("lat", "mem"),
            P("lat", "mem"),
        ),
        out_specs=(P(None, "lat", "mem"), P("mem", None, "lat", None)),
        check_vma=False,
    )
```

```python
import functools
import jax
import jax.numpy as jnp
from jax import lax
from jax.experimental import pallas as pl
from jax.experimental.pallas import tpu as pltpu
from jax.sharding import PartitionSpec as P

INNER = 2
LANES = 128
HIGHEST = lax.Precision.HIGHEST
F32 = jnp.float32
BF16 = jnp.bfloat16
VMEM_LIMIT = 60 * 1024 * 1024


VM = pl.BlockSpec(memory_space=pltpu.VMEM)
ANY = pl.BlockSpec(memory_space=pl.ANY)


def params():
    return pltpu.CompilerParams(vmem_limit_bytes=VMEM_LIMIT)


def cost(flops, nbytes):
    return pl.CostEstimate(flops=flops, bytes_accessed=nbytes, transcendentals=0)


def take_lanes(values, index):
    numbers = lax.GatherDimensionNumbers(
        offset_dims=(),
        collapsed_slice_dims=(1,),
        start_index_map=(1,),
        operand_batching_dims=(0,),
        start_indices_batching_dims=(0,),
    )
    return lax.gather(
        values, index[..., None], numbers, slice_sizes=(1, 1), mode=lax.GatherScatterMode.PROMISE_IN_BOUNDS
    )


def split(value):
    high = value.astype(BF16)
    return high, (value - high.astype(F32)).astype(BF16)


def split_outside(value):
    high = lax.reduce_precision(value, exponent_bits=8, mantissa_bits=7)
    return high.astype(BF16), (value - high).astype(BF16)


def lane_iota(rows):
    return lax.broadcasted_iota(jnp.int32, (rows, LANES), 1)


def dot(a, b):
    return jnp.dot(a, b, preferred_element_type=F32)


def sort_kernel(cell_ref, weight_ref, mask_ref, innovation_ref, out_ref, cell, weight, value):
    rows, width = cell_ref.shape
    for scratch in (cell, weight, value):
        scratch[...] = jnp.zeros(scratch.shape, scratch.dtype)
    cell[:, :width] = cell_ref[...]
    used = weight_ref[...] * mask_ref[...].astype(F32)
    weight[:, :width] = used
    value[:, :width] = -(used * innovation_ref[...])
    lane = lane_iota(rows)
    key = cell[...] * width + lane % width
    block = 2
    while block <= width:
        hop = block // 2
        while hop:
            other = take_lanes(key, lane ^ hop)
            keep_low = ((lane & block) == 0) == ((lane & hop) == 0)
            if block == width:
                keep_low = (lane & hop) == 0
            key = jnp.where(keep_low, jnp.minimum(key, other), jnp.maximum(key, other))
            hop //= 2
        block *= 2
    slot = key % width
    per = LANES // width
    part = rows // per
    sorted_values = (
        (key // width).astype(F32),
        take_lanes(weight[...], slot),
        take_lanes(value[...], slot),
    )
    for kind, values in enumerate(sorted_values):
        values = jnp.where(lane < width, values, 0.0)
        total = values[:part]
        for side in range(1, per):
            total = total + pltpu.roll(values[side * part : (side + 1) * part], side * width, axis=1)
        out_ref[kind] = total


def run_totals(cells, values, width):
    hop = 1
    while hop < width:
        same = pltpu.roll(cells, LANES - hop, axis=1) == cells
        values = values + jnp.where(same, pltpu.roll(values, LANES - hop, axis=1), 0.0)
        hop *= 2
    return values


def pick_cells(cells, reads, width, levels, quarter, lon):
    per = LANES // width
    halves = quarter // LANES
    lane = lane_iota(cells.shape[0])
    position = cells % LANES
    kind = (cells // lon) * halves + (cells % quarter) // LANES
    outs = [jnp.zeros(cells.shape, F32) for _ in reads]
    for side in range(per):
        here = (lane // width) == side
        for level in range(levels):
            for half in range(halves):
                use = here & (kind == level * halves + half)
                outs = [
                    jnp.where(use, take_lanes(read(side, level, half), position), out)
                    for read, out in zip(reads, outs)
                ]
    return outs


def observe_kernel(width, nmem, *refs):
    block_refs, (members_ref, obs_ref, local_ref, mine_ref, other_ref, blocks) = refs[:nmem], refs[nmem:]
    _, part, _ = block_refs[0].shape
    count, levels, rows, lon = members_ref.shape
    me = lax.axis_index("mem")
    parity = lax.axis_index("lat") % 2
    per = LANES // width
    quarter = lon // nmem
    for hop, ref in enumerate(block_refs):
        blocks[lax.rem(me - hop + nmem, nmem)] = ref[...]
    lane = lane_iota(part)
    for group in range(nmem // per):
        columns = slice(group * LANES, (group + 1) * LANES)
        for kind in range(3):
            for piece in range(per):
                total = jnp.zeros((part, LANES), F32)
                for side in range(per):
                    raw = blocks[group * per + side, kind]
                    turn = ((side - piece) * width) % LANES
                    if turn:
                        raw = pltpu.roll(raw, turn, axis=1)
                    total = jnp.where(lane // width == side, raw, total)
                obs_ref[kind, piece * part : (piece + 1) * part, columns] = total
        cells = obs_ref[0, :, columns].astype(jnp.int32)
        local_ref[0, :, columns] = obs_ref[0, :, columns]
        local_ref[1, :, columns] = run_totals(cells, obs_ref[2, :, columns], width)

    step = 8
    half_count = count // 2

    def one(index, carry):
        start = pl.multiple_of(index * step, step)
        here = pl.ds(start, step)
        for group in range(nmem // per):
            columns = slice(group * LANES, (group + 1) * LANES)
            cells = obs_ref[0, here, columns].astype(jnp.int32)

            def reader(member):
                def read(side, level, half):
                    first = (group * per + side) * quarter + half * LANES
                    return members_ref[member, level, here, first : first + LANES]

                return read

            order = [parity * half_count + i for i in range(half_count)]
            order += [(1 - parity) * half_count + i for i in range(half_count)]
            outs = pick_cells(cells, [reader(member) for member in order], width, levels, quarter, lon)
            for i in range(half_count):
                mine_ref[i, here, columns] = outs[i]
                other_ref[i, here, columns] = outs[half_count + i]
        return carry

    lax.fori_loop(0, rows // step, one, 0)


def inverse_kernel(width, levels, lon, nblocks_lat, *refs):
    local_refs, (inverse_ref, value_ref, cells_all) = refs[:nblocks_lat], refs[nblocks_lat:]
    _, rows, slots = local_refs[0].shape
    nblocks = slots // width
    quarter = lon // nblocks
    per = LANES // width
    tall = 16
    for number, local_ref in enumerate(local_refs):
        value_ref[number * rows : (number + 1) * rows, :] = local_ref[1]
        cells_all[number * rows : (number + 1) * rows, :] = local_ref[0].astype(jnp.int32)

    def one(index, carry):
        here = pl.ds(pl.multiple_of(index * tall, tall), tall)
        lane = lane_iota(tall)
        for block in range(nblocks):
            group, offset = block // per, (block % per) * width
            cells = cells_all[here, group * LANES : (group + 1) * LANES]
            nothing = (offset - 1) % LANES
            for level in range(levels):
                for half in range(quarter // LANES):
                    target = lane + (level * lon + block * quarter + half * LANES)
                    place = jnp.full((tall, LANES), offset, jnp.int32)
                    hop = width // 2
                    while hop:
                        place = jnp.where(take_lanes(cells, place + (hop - 1)) < target, place + hop, place)
                        hop //= 2
                    found = take_lanes(cells, place) == target
                    inverse_ref[level * nblocks + block, here, half * LANES : (half + 1) * LANES] = jnp.where(
                        found, place, nothing
                    )
        return carry

    lax.fori_loop(0, cells_all.shape[0] // tall, one, 0)


def apply_kernel(width, levels, nlat_blocks, first, *refs):
    seen_refs = refs[:nlat_blocks]
    refs = refs[nlat_blocks:]
    if not first:
        pay_refs = refs[:nlat_blocks]
        refs = refs[nlat_blocks:]
    value_refs, inverse_refs = refs[:2], refs[2:4]
    lhs_high_ref, lhs_low_ref, local_refs, cn_high_ref, cn_low_ref = refs[4], refs[5], refs[6:8], refs[8], refs[9]
    members_ref, members_sib_ref = refs[10], refs[11]
    refs = refs[12:]
    seen_out_refs, image_refs = refs[:2], refs[2:4]
    back_high_refs, back_low_refs = refs[4:6], refs[6:8]
    refs = refs[8:]
    if not first:
        length_ref = refs[0]
        refs = refs[1:]
    (seen, value, inverse, cn_high, cn_low, members, xa_high, xa_low, xb_high, xb_low, w_high, w_low,
     sems, seen_sems, inv_sems) = refs
    count, nlat, slots = seen.shape
    rows = nlat // nlat_blocks
    wide = 2 * rows
    nblocks = slots // width
    per = LANES // width
    nchunks = levels * nblocks
    quarter = inverse.shape[2]
    lon = quarter * nblocks
    parity = lax.axis_index("lat") % 2

    seen_copies = [
        pltpu.make_async_copy(ref, seen.at[:, pl.ds(number * rows, rows)], seen_sems.at[number])
        for number, ref in enumerate(seen_refs)
    ]
    inverse_copies = [
        [
            pltpu.make_async_copy(
                ref.at[chunk], inverse.at[chunk, pl.ds(side * (nlat // 2), nlat // 2)], inv_sems.at[chunk, side]
            )
            for side, ref in enumerate(inverse_refs)
        ]
        for chunk in range(nchunks)
    ]
    late = [
        pltpu.make_async_copy(cn_high_ref, cn_high, sems.at[0]),
        pltpu.make_async_copy(cn_low_ref, cn_low, sems.at[1]),
        pltpu.make_async_copy(members_ref.at[pl.ds(parity * count, count)], members.at[0], sems.at[2]),
        pltpu.make_async_copy(members_sib_ref, members.at[1], sems.at[3]),
    ]
    early = seen_copies + [copy for both in inverse_copies for copy in both]
    for copy in early + late:
        copy.start()

    if first:
        for side, ref in enumerate(value_refs):
            value[side * (nlat // 2) : (side + 1) * (nlat // 2), :] = ref[...]
    else:
        top = jnp.zeros((1, slots), F32)
        bottom = jnp.zeros((1, slots), F32)
        for ref in pay_refs:
            top = top + ref[rows : rows + 1, :]
            bottom = bottom + ref[rows + 1 : rows + 2, :]
        length = jnp.sum(top, axis=1, keepdims=True) / jnp.sum(bottom, axis=1, keepdims=True)
        length_ref[...] = jnp.broadcast_to(length, length_ref.shape)
        per_side = nlat_blocks // 2
        for number, ref in enumerate(pay_refs):
            inside = (number % per_side) * rows
            old = value_refs[number // per_side][inside : inside + rows, :]
            value[number * rows : (number + 1) * rows, :] = old - length * (old + ref[:rows, :])

    tall = 16
    lane = lane_iota(tall)

    def build(chunk, x_high, x_low):
        block = lax.rem(chunk, nblocks)
        offset = lax.rem(block, per) * width
        columns = pl.ds(pl.multiple_of((block // per) * LANES, LANES), LANES)
        inside = (lane >= offset) & (lane < offset + width)
        for start in range(0, nlat, tall):
            part = slice(start, start + tall)
            numbers = value[part, columns]
            sources = [jnp.where(inside, seen[m, part, columns] * numbers, 0.0) for m in range(count)]
            for half in range(quarter // LANES):
                cols = slice(half * LANES, (half + 1) * LANES)
                index = inverse[chunk, part, cols]
                for m in range(count):
                    high, low = split(take_lanes(sources[m], index))
                    x_high[m, part, cols] = high
                    x_low[m, part, cols] = low

    def multiply(chunk, x_high, x_low):
        level = chunk // nblocks
        cols = pl.ds(pl.multiple_of(lax.rem(chunk, nblocks) * quarter, quarter), quarter)
        for m in range(count):
            both = (
                dot(lhs_high_ref[...], x_high[m])
                + dot(lhs_low_ref[...], x_high[m])
                + dot(lhs_high_ref[...], x_low[m])
            )
            high, low = split(both[:wide])
            where = pl.ds(pl.multiple_of((m * levels + level) * wide, wide), wide)
            w_high[where, cols] = high
            w_low[where, cols] = low
            where = pl.ds(pl.multiple_of((m * levels + level) * rows, rows), rows)
            for side in range(2):
                high, low = split(both[wide + side * rows : wide + (side + 1) * rows])
                back_high_refs[side][where, cols] = high
                back_low_refs[side][where, cols] = low

    for copy in early:
        copy.wait()
    build(0, xa_high, xa_low)

    def one(pair, carry):
        chunk = pair * 2
        build(chunk + 1, xb_high, xb_low)
        multiply(chunk, xa_high, xa_low)
        build(jnp.minimum(chunk + 2, nchunks - 1), xa_high, xa_low)
        multiply(chunk + 1, xb_high, xb_low)
        return carry

    lax.fori_loop(0, nchunks // 2, one, 0)

    for copy in late:
        copy.wait()
    tile = 2 * LANES
    deep = levels * wide

    for column in range(lon // tile):
        cols = slice(column * tile, (column + 1) * tile)
        totals = [[None] * levels, [None] * levels]
        for member in range(count):
            part = slice(member * deep, (member + 1) * deep)
            product = (
                dot(w_high[part, :], cn_high[:, cols])
                + dot(w_low[part, :], cn_high[:, cols])
                + dot(w_high[part, :], cn_low[:, cols])
            )
            for level in range(levels):
                for side in range(2):
                    begin = level * wide + side * rows
                    term = members[side, member, level, :, cols] * product[begin : begin + rows]
                    if member == 0:
                        image_refs[side][level, :, cols] = term
                    else:
                        image_refs[side][level, :, cols] += term

    step = 8
    for side in range(2):
        for start in range(0, rows, step):
            part = slice(start, start + step)
            for group in range(nblocks // per):
                columns = slice(group * LANES, (group + 1) * LANES)
                cells = local_refs[side][0, part, columns].astype(jnp.int32)

                def read(piece, level, half):
                    begin = (group * per + piece) * quarter + half * LANES
                    return image_refs[side][level, part, begin : begin + LANES]

                seen_out_refs[side][part, columns] = pick_cells(cells, [read], width, levels, quarter, lon)[0]


def answer_kernel(width, nparts, *refs):
    parts, (obs_ref, pay_ref, seen_ref) = refs[:nparts], refs[nparts:]
    rows = obs_ref.shape[1]
    seen = parts[0][...]
    for part in parts[1:]:
        seen = seen + part[...]
    seen_ref[...] = seen
    weighted = obs_ref[1] * seen
    value = obs_ref[2]
    for group in range(seen.shape[1] // LANES):
        columns = slice(group * LANES, (group + 1) * LANES)
        cells = obs_ref[0, :, columns].astype(jnp.int32)
        pay_ref[:rows, columns] = run_totals(cells, weighted[:, columns], width)
    pay_ref[rows:, :] = jnp.zeros((8, seen.shape[1]), F32)
    pay_ref[rows : rows + 1, :] = jnp.sum(value * seen, axis=0, keepdims=True)
    pay_ref[rows + 1 : rows + 2, :] = jnp.sum(seen * (value + weighted), axis=0, keepdims=True)


def last_kernel(nparts, *refs):
    parts, (obs_ref, before_ref, length_ref, dots_ref) = refs[:nparts], refs[nparts:]
    seen = parts[0][...]
    for part in parts[1:]:
        seen = seen + part[...]
    weight, value = obs_ref[1], obs_ref[2]
    length = length_ref[:1, :1]
    value = value - length * (value + weight * before_ref[...])
    dots_ref[...] = jnp.zeros(dots_ref.shape, F32)
    dots_ref[:1, :] = jnp.sum(value * seen, axis=0, keepdims=True)
    dots_ref[1:2, :] = jnp.sum(seen * (value + weight * seen), axis=0, keepdims=True)


def covariance_kernel(root_ref, high_ref, low_ref, root_high_ref, root_low_ref):
    lon = root_ref.shape[0]
    root_high_ref[...], root_low_ref[...] = split(root_ref[...])
    tile = 2 * LANES
    numbers = (((1,), (1,)), ((), ()))

    def times(a, b):
        return lax.dot_general(a, b, numbers, preferred_element_type=F32)

    for column in range(lon // tile):
        cols = slice(column * tile, (column + 1) * tile)
        high, low = root_high_ref[cols, :], root_low_ref[cols, :]
        total = times(root_high_ref[...], high) + times(root_low_ref[...], high) + times(root_high_ref[...], low)
        high_ref[:, cols], low_ref[:, cols] = split(total)


def product_kernel(a_high_ref, a_low_ref, b_high_ref, b_low_ref, out_ref):
    out_ref[...] = (
        dot(a_high_ref[...], b_high_ref[...])
        + dot(a_low_ref[...], b_high_ref[...])
        + dot(a_high_ref[...], b_low_ref[...])
    )


def product(a_high, a_low, b_high, b_low):
    rows, deep = a_high.shape
    wide = b_high.shape[1]
    tile = 2 * LANES
    whole = pl.BlockSpec((rows, deep), lambda i: (0, 0))
    panel = pl.BlockSpec((deep, tile), lambda i: (0, i))
    return pl.pallas_call(
        product_kernel,
        grid=(wide // tile,),
        in_specs=[whole, whole, panel, panel],
        out_specs=pl.BlockSpec((rows, tile), lambda i: (0, i)),
        out_shape=jax.ShapeDtypeStruct((rows, wide), F32),
        compiler_params=params(),
        cost_estimate=cost(6 * rows * deep * wide, 4 * (rows * deep + deep * wide + rows * wide)),
        name="lon_product",
    )(a_high, a_low, b_high, b_low)


def final_kernel(parity_ref, dots_ref, length_ref, q0_ref, q1_ref, a0_ref, b0_ref, a1_ref, b1_ref,
                 increment_ref, control_ref, lengths):
    index = pl.program_id(0)

    @pl.when(index == 0)
    def _():
        top = jnp.sum(dots_ref[:1, :], axis=1, keepdims=True)
        bottom = jnp.sum(dots_ref[1:2, :], axis=1, keepdims=True)
        lengths[0] = length_ref[...]
        lengths[1] = jnp.broadcast_to(top / bottom, length_ref.shape)
        increment_ref[...] = -(lengths[0, :1, :1] * q0_ref[...] + lengths[1, :1, :1] * q1_ref[...])

    half = pl.num_programs(0) // 2

    @pl.when(index < half)
    def _():
        control_ref[...] = -(lengths[0, :1, :1] * a0_ref[...] + lengths[1, :1, :1] * a1_ref[...])

    @pl.when(index >= half)
    def _():
        control_ref[...] = -(lengths[0, :1, :1] * b0_ref[...] + lengths[1, :1, :1] * b1_ref[...])


def per_device(members, lat_root, lon_root, innovation, obs_weight, obs_mask, obs_cell):
    count, levels, rows, lon = members.shape
    half_count = count // 2
    nmem, nlat_dev = lax.axis_size("mem"), lax.axis_size("lat")
    nlat = lat_root.shape[0]
    width = obs_cell.shape[1]
    slots = width * nmem
    quarter = lon // nmem
    me_lat, me_mem = lax.axis_index("lat"), lax.axis_index("mem")
    parity = me_lat % 2
    shape = jax.ShapeDtypeStruct
    chips = list(range(0, nlat_dev, 2))
    order = chips + [bits + 1 for bits in chips]
    steps = [2**k for k in range(1, (nlat_dev - 1).bit_length())]

    def swap(value, bits):
        return lax.ppermute(value, "lat", [(i, i ^ bits) for i in range(nlat_dev)])

    def direct(value):
        return [value] + [swap(value, bits) for bits in chips[1:]]

    def relayed(value, hops):
        blocks = {0: value}
        for hop in hops:
            blocks.update({bits ^ hop: swap(block, hop) for bits, block in blocks.items()})
        return [blocks[bits] for bits in chips]

    def around_mem(value):
        return [value] + [
            lax.ppermute(value, "mem", [(i, (i + hop) % nmem) for i in range(nmem)]) for hop in range(1, nmem)
        ]

    block = pl.pallas_call(
        sort_kernel,
        in_specs=[VM] * 4,
        out_specs=VM,
        out_shape=shape((3, rows * width // LANES, LANES), F32),
        scratch_shapes=[pltpu.VMEM((rows, LANES), jnp.int32)] + [pltpu.VMEM((rows, LANES), F32)] * 2,
        compiler_params=params(),
        name="sort_slots",
    )(obs_cell, obs_weight, obs_mask, innovation)
    obs, local, mine, other = pl.pallas_call(
        functools.partial(observe_kernel, width, nmem),
        in_specs=[VM] * (nmem + 1),
        out_specs=[VM] * 4,
        out_shape=[
            shape((3, rows, slots), F32),
            shape((2, rows, slots), F32),
            shape((half_count, rows, slots), F32),
            shape((half_count, rows, slots), F32),
        ],
        scratch_shapes=[pltpu.VMEM((nmem, *block.shape), F32)],
        compiler_params=params(),
        cost_estimate=cost(10**8, 4 * members.size),
        name="members_at_slots",
    )(*around_mem(block), members)

    locals_ = direct(local)
    local_sib = swap(local, 1)
    seens = relayed(mine, steps) + relayed(swap(other, 1), steps[::-1])
    members_sib = swap(lax.dynamic_slice_in_dim(members, (1 - parity) * half_count, half_count, axis=0), 1)

    def own_rows(matrix, axis):
        return [
            lax.dynamic_slice_in_dim(matrix, (me_lat ^ side) * rows, rows, axis=axis) for side in range(2)
        ]

    lat_cov = jnp.einsum("ij,kj->ik", jnp.concatenate(own_rows(lat_root, 0)), lat_root, precision=HIGHEST)
    both = jnp.concatenate([lat_cov] + [part.T for part in own_rows(lat_root, 1)])
    both = jnp.concatenate(
        [lax.dynamic_slice_in_dim(both, (me_lat ^ bits) * rows, rows, axis=1) for bits in order], axis=1
    )
    lhs_high, lhs_low = split_outside(both)
    cn_high, cn_low, lon_high, lon_low = pl.pallas_call(
        covariance_kernel,
        in_specs=[VM],
        out_specs=[VM] * 4,
        out_shape=[shape((lon, lon), BF16)] * 4,
        compiler_params=params(),
        cost_estimate=cost(6 * lon**3, 12 * lon * lon),
        name="lon_covariance",
    )(lon_root)

    nchunks = levels * nmem
    inverse, value = pl.pallas_call(
        functools.partial(inverse_kernel, width, levels, lon, nlat_dev // 2),
        in_specs=[VM] * (nlat_dev // 2),
        out_specs=[VM] * 2,
        out_shape=[shape((nchunks, nlat // 2, quarter), jnp.int32), shape((nlat // 2, slots), F32)],
        scratch_shapes=[pltpu.VMEM((nlat // 2, slots), jnp.int32)],
        compiler_params=params(),
        cost_estimate=cost(10**10, 2 * nlat * lon * levels),
        name="inverse",
    )(*locals_)
    inverses, values = [inverse, swap(inverse, 1)], [value, swap(value, 1)]

    tall = half_count * levels * rows

    def apply(pays):
        first = pays is None
        outs = (
            [shape((rows, slots), F32)] * 2 + [shape((levels, rows, lon), F32)] * 2 + [shape((tall, lon), BF16)] * 4
        )
        if not first:
            outs.append(shape((8, LANES), F32))
        return pl.pallas_call(
            functools.partial(apply_kernel, width, levels, nlat_dev, first),
            in_specs=[ANY] * nlat_dev
            + ([] if first else [VM] * nlat_dev)
            + [VM] * 2
            + [ANY] * 2
            + [VM] * 4
            + [ANY] * 4,
            out_specs=[VM] * len(outs),
            out_shape=outs,
            scratch_shapes=[
                pltpu.VMEM((half_count, nlat, slots), F32),
                pltpu.VMEM((nlat, slots), F32),
                pltpu.VMEM((nchunks, nlat, quarter), jnp.int32),
                pltpu.VMEM((lon, lon), BF16),
                pltpu.VMEM((lon, lon), BF16),
                pltpu.VMEM((2, half_count, levels, rows, lon), F32),
            ]
            + [pltpu.VMEM((half_count, nlat, quarter), BF16)] * 4
            + [pltpu.VMEM((2 * tall, lon), BF16)] * 2
            + [
                pltpu.SemaphoreType.DMA((4,)),
                pltpu.SemaphoreType.DMA((nlat_dev,)),
                pltpu.SemaphoreType.DMA((nchunks, 2)),
            ],
            compiler_params=params(),
            cost_estimate=cost(12 * tall * lon * (nlat + lon), 30 * 2**20),
            name="apply_first" if first else "apply_next",
        )(
            *seens,
            *([] if first else pays),
            *values,
            *inverses,
            lhs_high,
            lhs_low,
            local,
            local_sib,
            cn_high,
            cn_low,
            members,
            members_sib,
        )

    def to_quarters(image):
        parts = image.reshape(levels, rows, nmem, quarter).transpose(2, 0, 1, 3)

        def part(hop):
            return lax.dynamic_index_in_dim(parts, (me_mem + hop) % nmem, keepdims=False)

        total = part(0)
        for hop in range(1, nmem):
            total = total + lax.ppermute(part(hop), "mem", [(i, (i + hop) % nmem) for i in range(nmem)])
        return total

    def gradient(backs):
        other = product(backs[1], backs[3], lon_high, lon_low)
        mine = product(backs[0], backs[2], lon_high, lon_low)
        field = (half_count, levels, rows, lon)
        return mine.reshape(field), other.reshape(field)

    seen_own, seen_sib, image_own, image_sib, *backs0 = apply(None)
    image0 = image_own + swap(image_sib, 1)
    pay, seen0 = pl.pallas_call(
        functools.partial(answer_kernel, width, nmem),
        in_specs=[VM] * (nmem + 1),
        out_specs=[VM] * 2,
        out_shape=[shape((rows + 8, slots), F32), shape((rows, slots), F32)],
        compiler_params=params(),
        name="answer",
    )(*around_mem(seen_own + swap(seen_sib, 1)), obs)
    pays = direct(pay)
    mine0, other0 = gradient(backs0)
    pays = pays + [swap(block, 1) for block in pays]
    pays, mine0, other0 = lax.optimization_barrier((pays, mine0, other0))
    other0 = swap(other0, 1)

    seen_own, seen_sib, image_own, image_sib, *backs1, length0 = apply(pays)
    image1 = image_own + swap(image_sib, 1)
    mine1, other1 = gradient(backs1)
    parts = around_mem(seen_own + swap(seen_sib, 1))
    parts, mine1, other1 = lax.optimization_barrier((parts, mine1, other1))
    dots = pl.pallas_call(
        functools.partial(last_kernel, nmem),
        in_specs=[VM] * (nmem + 3),
        out_specs=VM,
        out_shape=shape((8, slots), F32),
        compiler_params=params(),
        name="last_dots",
    )(*parts, obs, seen0, length0)
    other1 = swap(other1, 1)
    quarter0, quarter1 = to_quarters(image0), to_quarters(image1)
    for part in direct(dots)[1:]:
        dots = dots + part
    dots = dots + swap(dots, 1)

    small = pl.BlockSpec((8, slots), lambda i, par: (0, 0))
    tiny = pl.BlockSpec((8, LANES), lambda i, par: (0, 0))
    piece = pl.BlockSpec((levels, rows, quarter), lambda i, par: (0, 0, 0))
    near = pl.BlockSpec((1, levels, rows, lon), lambda i, par: (jnp.minimum(i, half_count - 1), 0, 0, 0))
    far = pl.BlockSpec((1, levels, rows, lon), lambda i, par: (jnp.maximum(i - half_count, 0), 0, 0, 0))
    put = pl.BlockSpec((1, levels, rows, lon), lambda i, par: ((i + par[0] * half_count) % count, 0, 0, 0))
    return pl.pallas_call(
        final_kernel,
        grid_spec=pltpu.PrefetchScalarGridSpec(
            num_scalar_prefetch=1,
            grid=(count,),
            in_specs=[small, tiny, piece, piece, near, far, near, far],
            out_specs=[piece, put],
            scratch_shapes=[pltpu.VMEM((2, 8, LANES), F32)],
        ),
        out_shape=[shape((levels, rows, quarter), F32), shape(members.shape, F32)],
        compiler_params=params(),
        name="final",
    )(parity[None], dots, length0, quarter0, quarter1, mine0, other0, mine1, other1)


def solution(mesh):
    return jax.shard_map(
        per_device,
        mesh=mesh,
        in_specs=(
            P("mem", None, "lat", None),
            P(),
            P(),
            P("lat", "mem"),
            P("lat", "mem"),
            P("lat", "mem"),
            P("lat", "mem"),
        ),
        out_specs=(P(None, "lat", "mem"), P("mem", None, "lat", None)),
        check_vma=False,
    )
```

```python
import functools
import jax
import jax.numpy as jnp
from jax import lax
from jax.experimental import pallas as pl
from jax.experimental.pallas import tpu as pltpu
from jax.sharding import PartitionSpec as P


LANES = 128
HIGHEST = lax.Precision.HIGHEST
F32 = jnp.float32
BF16 = jnp.bfloat16
VMEM_LIMIT = 60 * 1024 * 1024


VM = pl.BlockSpec(memory_space=pltpu.VMEM)
ANY = pl.BlockSpec(memory_space=pl.ANY)


def params():
    return pltpu.CompilerParams(vmem_limit_bytes=VMEM_LIMIT)


def cost(flops, nbytes):
    return pl.CostEstimate(flops=flops, bytes_accessed=nbytes, transcendentals=0)


def take_lanes(values, index):
    numbers = lax.GatherDimensionNumbers(
        offset_dims=(),
        collapsed_slice_dims=(1,),
        start_index_map=(1,),
        operand_batching_dims=(0,),
        start_indices_batching_dims=(0,),
    )
    return lax.gather(
        values, index[..., None], numbers, slice_sizes=(1, 1), mode=lax.GatherScatterMode.PROMISE_IN_BOUNDS
    )


def split(value):
    high = value.astype(BF16)
    return high, (value - high.astype(F32)).astype(BF16)


def lane_iota(rows):
    return lax.broadcasted_iota(jnp.int32, (rows, LANES), 1)


def dot(a, b):
    return jnp.dot(a, b, preferred_element_type=F32)


def sort_kernel(cell_ref, weight_ref, mask_ref, innovation_ref, out_ref, cell, weight, value):
    rows, width = cell_ref.shape
    for scratch in (cell, weight, value):
        scratch[...] = jnp.zeros(scratch.shape, scratch.dtype)
    cell[:, :width] = cell_ref[...]
    used = weight_ref[...] * mask_ref[...].astype(F32)
    weight[:, :width] = used
    value[:, :width] = -(used * innovation_ref[...])
    lane = lane_iota(rows)
    key = cell[...] * width + lane % width
    block = 2
    while block <= width:
        hop = block // 2
        while hop:
            other = take_lanes(key, lane ^ hop)
            keep_low = ((lane & block) == 0) == ((lane & hop) == 0)
            if block == width:
                keep_low = (lane & hop) == 0
            key = jnp.where(keep_low, jnp.minimum(key, other), jnp.maximum(key, other))
            hop //= 2
        block *= 2
    slot = key % width
    per = LANES // width
    part = rows // per
    sorted_values = (
        (key // width).astype(F32),
        take_lanes(weight[...], slot),
        take_lanes(value[...], slot),
    )
    for kind, values in enumerate(sorted_values):
        values = jnp.where(lane < width, values, 0.0)
        total = values[:part]
        for side in range(1, per):
            total = total + pltpu.roll(values[side * part : (side + 1) * part], side * width, axis=1)
        out_ref[kind] = total


def run_totals(cells, values, width):
    hop = 1
    while hop < width:
        same = pltpu.roll(cells, LANES - hop, axis=1) == cells
        values = values + jnp.where(same, pltpu.roll(values, LANES - hop, axis=1), 0.0)
        hop *= 2
    return values


def pick_cells(cells, reads, width, levels, quarter, lon):
    per = LANES // width
    halves = quarter // LANES
    lane = lane_iota(cells.shape[0])
    position = cells % LANES
    kind = (cells // lon) * halves + (cells % quarter) // LANES
    outs = [jnp.zeros(cells.shape, F32) for _ in reads]
    for side in range(per):
        here = (lane // width) == side
        for level in range(levels):
            for half in range(halves):
                use = here & (kind == level * halves + half)
                outs = [
                    jnp.where(use, take_lanes(read(side, level, half), position), out)
                    for read, out in zip(reads, outs)
                ]
    return outs


def observe_kernel(width, nmem, *refs):
    block_refs, (members_ref, obs_ref, local_ref, mine_ref, other_ref, blocks) = refs[:nmem], refs[nmem:]
    _, part, _ = block_refs[0].shape
    count, levels, rows, lon = members_ref.shape
    me = lax.axis_index("mem")
    parity = lax.axis_index("lat") % 2
    per = LANES // width
    quarter = lon // nmem
    for hop, ref in enumerate(block_refs):
        blocks[lax.rem(me - hop + nmem, nmem)] = ref[...]
    lane = lane_iota(part)
    for group in range(nmem // per):
        columns = slice(group * LANES, (group + 1) * LANES)
        for kind in range(3):
            for piece in range(per):
                total = jnp.zeros((part, LANES), F32)
                for side in range(per):
                    raw = blocks[group * per + side, kind]
                    turn = ((side - piece) * width) % LANES
                    if turn:
                        raw = pltpu.roll(raw, turn, axis=1)
                    total = jnp.where(lane // width == side, raw, total)
                obs_ref[kind, piece * part : (piece + 1) * part, columns] = total
        cells = obs_ref[0, :, columns].astype(jnp.int32)
        local_ref[0, :, columns] = obs_ref[0, :, columns]
        local_ref[1, :, columns] = run_totals(cells, obs_ref[2, :, columns], width)

    step = 8
    half_count = count // 2

    def one(index, carry):
        start = pl.multiple_of(index * step, step)
        here = pl.ds(start, step)
        for group in range(nmem // per):
            columns = slice(group * LANES, (group + 1) * LANES)
            cells = obs_ref[0, here, columns].astype(jnp.int32)

            def reader(member):
                def read(side, level, half):
                    first = (group * per + side) * quarter + half * LANES
                    return members_ref[member, level, here, first : first + LANES]

                return read

            order = [parity * half_count + i for i in range(half_count)]
            order += [(1 - parity) * half_count + i for i in range(half_count)]
            outs = pick_cells(cells, [reader(member) for member in order], width, levels, quarter, lon)
            for i in range(half_count):
                mine_ref[i, here, columns] = outs[i]
                other_ref[i, here, columns] = outs[half_count + i]
        return carry

    lax.fori_loop(0, rows // step, one, 0)


def inverse_kernel(width, levels, lon, nblocks_lat, *refs):
    local_refs, (inverse_ref, value_ref, cells_all) = refs[:nblocks_lat], refs[nblocks_lat:]
    _, rows, slots = local_refs[0].shape
    nblocks = slots // width
    quarter = lon // nblocks
    per = LANES // width
    tall = 16
    for number, local_ref in enumerate(local_refs):
        value_ref[number * rows : (number + 1) * rows, :] = local_ref[1]
        cells_all[number * rows : (number + 1) * rows, :] = local_ref[0].astype(jnp.int32)

    def one(index, carry):
        here = pl.ds(pl.multiple_of(index * tall, tall), tall)
        lane = lane_iota(tall)
        for block in range(nblocks):
            group, offset = block // per, (block % per) * width
            cells = cells_all[here, group * LANES : (group + 1) * LANES]
            nothing = (offset - 1) % LANES
            for level in range(levels):
                for half in range(quarter // LANES):
                    target = lane + (level * lon + block * quarter + half * LANES)
                    place = jnp.full((tall, LANES), offset, jnp.int32)
                    hop = width // 2
                    while hop:
                        place = jnp.where(take_lanes(cells, place + (hop - 1)) < target, place + hop, place)
                        hop //= 2
                    found = take_lanes(cells, place) == target
                    inverse_ref[level * nblocks + block, here, half * LANES : (half + 1) * LANES] = jnp.where(
                        found, place, nothing
                    )
        return carry

    lax.fori_loop(0, cells_all.shape[0] // tall, one, 0)


def apply_kernel(width, levels, nlat_blocks, first, *refs):
    seen_refs = refs[:nlat_blocks]
    refs = refs[nlat_blocks:]
    if not first:
        pay_refs = refs[:nlat_blocks]
        refs = refs[nlat_blocks:]
    value_refs, inverse_refs = refs[:2], refs[2:4]
    lhs_high_ref, lhs_low_ref, local_refs, cn_high_ref, cn_low_ref = refs[4], refs[5], refs[6:8], refs[8], refs[9]
    members_ref, members_sib_ref = refs[10], refs[11]
    refs = refs[12:]
    seen_out_refs, image_refs = refs[:2], refs[2:4]
    back_high_refs, back_low_refs = refs[4:6], refs[6:8]
    refs = refs[8:]
    if not first:
        length_ref = refs[0]
        refs = refs[1:]
    (seen, value, inverse, cn_high, cn_low, members, xa_high, xa_low, xb_high, xb_low, w_high, w_low,
     back_high, back_low, sems, seen_sems, inv_sems, back_sems) = refs
    count, nlat, slots = seen.shape
    rows = nlat // nlat_blocks
    wide = 2 * rows
    nblocks = slots // width
    per = LANES // width
    nchunks = levels * nblocks
    quarter = inverse.shape[2]
    lon = quarter * nblocks
    parity = lax.axis_index("lat") % 2
    me_mem = lax.axis_index("mem")

    def rotated(block):
        return lax.rem(block - me_mem + nblocks, nblocks)

    seen_copies = [
        pltpu.make_async_copy(ref, seen.at[:, pl.ds(number * rows, rows)], seen_sems.at[number])
        for number, ref in enumerate(seen_refs)
    ]

    def inverse_copies(chunk):
        return [
            pltpu.make_async_copy(
                ref.at[chunk], inverse.at[chunk, pl.ds(side * (nlat // 2), nlat // 2)], inv_sems.at[chunk, side]
            )
            for side, ref in enumerate(inverse_refs)
        ]

    late = [
        pltpu.make_async_copy(cn_high_ref, cn_high, sems.at[0]),
        pltpu.make_async_copy(cn_low_ref, cn_low, sems.at[1]),
        pltpu.make_async_copy(members_ref.at[pl.ds(parity * count, count)], members.at[0], sems.at[2]),
        pltpu.make_async_copy(members_sib_ref.at[pl.ds(parity * count, count)], members.at[1], sems.at[3]),
    ]
    for copy in inverse_copies(0) + seen_copies:
        copy.start()
    for chunk in range(1, nchunks):
        for copy in inverse_copies(chunk):
            copy.start()
    for copy in late:
        copy.start()

    if first:
        for side, ref in enumerate(value_refs):
            value[side * (nlat // 2) : (side + 1) * (nlat // 2), :] = ref[...]
    else:
        top = jnp.zeros((1, slots), F32)
        bottom = jnp.zeros((1, slots), F32)
        for ref in pay_refs:
            top = top + ref[rows : rows + 1, :]
            bottom = bottom + ref[rows + 1 : rows + 2, :]
        length = jnp.sum(top, axis=1, keepdims=True) / jnp.sum(bottom, axis=1, keepdims=True)
        length_ref[...] = jnp.broadcast_to(length, length_ref.shape)
        per_side = nlat_blocks // 2
        for number, ref in enumerate(pay_refs):
            inside = (number % per_side) * rows
            old = value_refs[number // per_side][inside : inside + rows, :]
            value[number * rows : (number + 1) * rows, :] = old - length * (old + ref[:rows, :])

    tall = 16
    lane = lane_iota(tall)

    def build(chunk, x_high, x_low):
        block = lax.rem(chunk, nblocks)
        offset = lax.rem(block, per) * width
        columns = pl.ds(pl.multiple_of((block // per) * LANES, LANES), LANES)
        inside = (lane >= offset) & (lane < offset + width)
        for start in range(0, nlat, tall):
            part = slice(start, start + tall)
            numbers = value[part, columns]
            sources = [jnp.where(inside, seen[m, part, columns] * numbers, 0.0) for m in range(count)]
            for half in range(quarter // LANES):
                cols = slice(half * LANES, (half + 1) * LANES)
                index = inverse[chunk, part, cols]
                for m in range(count):
                    high, low = split(take_lanes(sources[m], index))
                    x_high[m, part, cols] = high
                    x_low[m, part, cols] = low

    def multiply(chunk, x_high, x_low):
        level = chunk // nblocks
        cols = pl.ds(pl.multiple_of(lax.rem(chunk, nblocks) * quarter, quarter), quarter)
        for m in range(count):
            both = (
                dot(lhs_high_ref[...], x_high[m])
                + dot(lhs_low_ref[...], x_high[m])
                + dot(lhs_high_ref[...], x_low[m])
            )
            high, low = split(both[:wide])
            where = pl.ds(pl.multiple_of((m * levels + level) * wide, wide), wide)
            w_high[where, cols] = high
            w_low[where, cols] = low
            where = pl.ds(pl.multiple_of((m * levels + level) * rows, rows), rows)
            for side in range(2):
                high, low = split(both[wide + side * rows : wide + (side + 1) * rows])
                back_high[side, where, cols] = high
                back_low[side, where, cols] = low

    for copy in inverse_copies(0) + seen_copies:
        copy.wait()
    build(0, xa_high, xa_low)

    def one(pair, carry):
        chunk = pair * 2
        for copy in inverse_copies(chunk + 1):
            copy.wait()

        @pl.when(chunk + 2 < nchunks)
        def _():
            for copy in inverse_copies(chunk + 2):
                copy.wait()

        build(chunk + 1, xb_high, xb_low)
        multiply(chunk, xa_high, xa_low)
        build(jnp.minimum(chunk + 2, nchunks - 1), xa_high, xa_low)
        multiply(chunk + 1, xb_high, xb_low)
        return carry

    lax.fori_loop(0, nchunks // 2, one, 0)

    back_copies = [
        pltpu.make_async_copy(source.at[side], refs_[side], back_sems.at[kind, side])
        for kind, (source, refs_) in enumerate(((back_high, back_high_refs), (back_low, back_low_refs)))
        for side in range(2)
    ]
    for copy in back_copies:
        copy.start()
    for copy in late:
        copy.wait()
    tile = 2 * LANES
    deep = levels * wide

    for column in range(lon // tile):
        cols = slice(column * tile, (column + 1) * tile)
        place = rotated(column * tile // quarter)
        inner = slice(column * tile % quarter, column * tile % quarter + tile)
        for member in range(count):
            part = slice(member * deep, (member + 1) * deep)
            product = (
                dot(w_high[part, :], cn_high[:, cols])
                + dot(w_low[part, :], cn_high[:, cols])
                + dot(w_high[part, :], cn_low[:, cols])
            )
            for level in range(levels):
                for side in range(2):
                    begin = level * wide + side * rows
                    term = members[side, member, level, :, cols] * product[begin : begin + rows]
                    if member == 0:
                        image_refs[side][place, level, :, inner] = term
                    else:
                        image_refs[side][place, level, :, inner] += term

    step = 8
    for side in range(2):
        for start in range(0, rows, step):
            part = slice(start, start + step)
            for group in range(nblocks // per):
                columns = slice(group * LANES, (group + 1) * LANES)
                cells = local_refs[side][0, part, columns].astype(jnp.int32)

                def read(piece, level, half):
                    return image_refs[side][
                        rotated(group * per + piece), level, part, half * LANES : (half + 1) * LANES
                    ]

                seen_out_refs[side][part, columns] = pick_cells(cells, [read], width, levels, quarter, lon)[0]
    for copy in back_copies:
        copy.wait()


def answer_kernel(width, nparts, *refs):
    parts, (obs_ref, pay_ref, seen_ref) = refs[:nparts], refs[nparts:]
    rows = obs_ref.shape[1]
    seen = parts[0][...]
    for part in parts[1:]:
        seen = seen + part[...]
    seen_ref[...] = seen
    weighted = obs_ref[1] * seen
    value = obs_ref[2]
    for group in range(seen.shape[1] // LANES):
        columns = slice(group * LANES, (group + 1) * LANES)
        cells = obs_ref[0, :, columns].astype(jnp.int32)
        pay_ref[:rows, columns] = run_totals(cells, weighted[:, columns], width)
    pay_ref[rows:, :] = jnp.zeros((8, seen.shape[1]), F32)
    pay_ref[rows : rows + 1, :] = jnp.sum(value * seen, axis=0, keepdims=True)
    pay_ref[rows + 1 : rows + 2, :] = jnp.sum(seen * (value + weighted), axis=0, keepdims=True)


def last_kernel(nparts, *refs):
    parts, (obs_ref, before_ref, length_ref, dots_ref) = refs[:nparts], refs[nparts:]
    seen = parts[0][...]
    for part in parts[1:]:
        seen = seen + part[...]
    weight, value = obs_ref[1], obs_ref[2]
    length = length_ref[:1, :1]
    value = value - length * (value + weight * before_ref[...])
    dots_ref[...] = jnp.zeros(dots_ref.shape, F32)
    dots_ref[:1, :] = jnp.sum(value * seen, axis=0, keepdims=True)
    dots_ref[1:2, :] = jnp.sum(seen * (value + weight * seen), axis=0, keepdims=True)


def lat_kernel(order, root_ref, high_ref, low_ref, turned, chip, columns, ordered):
    rows = chip.shape[0] // 2
    me = lax.axis_index("lat")
    turned[...] = root_ref[...].T
    for side in range(2):
        here = pl.ds(pl.multiple_of((me ^ side) * rows, rows), rows)
        chip[side * rows : (side + 1) * rows, :] = root_ref[here, :]
        columns[side * rows : (side + 1) * rows, :] = turned[here, :]
    covariance = lax.dot_general(
        chip[...], root_ref[...], (((1,), (1,)), ((), ())), precision=HIGHEST, preferred_element_type=F32
    )
    both = jnp.concatenate([covariance, columns[...]]).T
    turned[:, : both.shape[1]] = both
    for number, bits in enumerate(order):
        here = pl.ds(pl.multiple_of((me ^ bits) * rows, rows), rows)
        ordered[number * rows : (number + 1) * rows, :] = turned[here, : both.shape[1]]
    high_ref[...], low_ref[...] = split(ordered[...].T)


def covariance_kernel(root_ref, high_ref, low_ref, root_high_ref, root_low_ref):
    lon = root_ref.shape[0]
    root_high_ref[...], root_low_ref[...] = split(root_ref[...])
    tile = 2 * LANES
    numbers = (((1,), (1,)), ((), ()))

    def times(a, b):
        return lax.dot_general(a, b, numbers, preferred_element_type=F32)

    for column in range(lon // tile):
        cols = slice(column * tile, (column + 1) * tile)
        high, low = root_high_ref[cols, :], root_low_ref[cols, :]
        total = times(root_high_ref[...], high) + times(root_low_ref[...], high) + times(root_high_ref[...], low)
        high_ref[:, cols], low_ref[:, cols] = split(total)


def product_kernel(a_high_ref, a_low_ref, b_high_ref, b_low_ref, out_ref):
    out_ref[...] = (
        dot(a_high_ref[...], b_high_ref[...])
        + dot(a_low_ref[...], b_high_ref[...])
        + dot(a_high_ref[...], b_low_ref[...])
    )


def product(a_high, a_low, b_high, b_low):
    rows, deep = a_high.shape
    wide = b_high.shape[1]
    tile = 2 * LANES
    whole = pl.BlockSpec((rows, deep), lambda i: (0, 0))
    panel = pl.BlockSpec((deep, tile), lambda i: (0, i))
    return pl.pallas_call(
        product_kernel,
        grid=(wide // tile,),
        in_specs=[whole, whole, panel, panel],
        out_specs=pl.BlockSpec((rows, tile), lambda i: (0, i)),
        out_shape=jax.ShapeDtypeStruct((rows, wide), F32),
        compiler_params=params(),
        cost_estimate=cost(6 * rows * deep * wide, 4 * (rows * deep + deep * wide + rows * wide)),
        name="lon_product",
    )(a_high, a_low, b_high, b_low)


def final_kernel(parity_ref, dots_ref, length_ref, q0_ref, q1_ref, a0_ref, b0_ref, a1_ref, b1_ref,
                 increment_ref, control_ref, lengths):
    index = pl.program_id(0)

    @pl.when(index == 0)
    def _():
        top = jnp.sum(dots_ref[:1, :], axis=1, keepdims=True)
        bottom = jnp.sum(dots_ref[1:2, :], axis=1, keepdims=True)
        lengths[0] = length_ref[...]
        lengths[1] = jnp.broadcast_to(top / bottom, length_ref.shape)
        increment_ref[...] = -(lengths[0, :1, :1] * q0_ref[...] + lengths[1, :1, :1] * q1_ref[...])

    half = pl.num_programs(0) // 2

    @pl.when(index < half)
    def _():
        control_ref[...] = -(lengths[0, :1, :1] * a0_ref[...] + lengths[1, :1, :1] * a1_ref[...])

    @pl.when(index >= half)
    def _():
        control_ref[...] = -(lengths[0, :1, :1] * b0_ref[...] + lengths[1, :1, :1] * b1_ref[...])


def per_device(members, lat_root, lon_root, innovation, obs_weight, obs_mask, obs_cell):
    count, levels, rows, lon = members.shape
    half_count = count // 2
    nmem, nlat_dev = lax.axis_size("mem"), lax.axis_size("lat")
    nlat = lat_root.shape[0]
    width = obs_cell.shape[1]
    slots = width * nmem
    quarter = lon // nmem
    me_lat = lax.axis_index("lat")
    parity = me_lat % 2
    shape = jax.ShapeDtypeStruct
    chips = list(range(0, nlat_dev, 2))
    order = chips + [bits + 1 for bits in chips]

    def swap(value, bits):
        return lax.ppermute(value, "lat", [(i, i ^ bits) for i in range(nlat_dev)])

    def direct(value):
        return [value] + [swap(value, bits) for bits in chips[1:]]

    def around_mem(value):
        return [value] + [
            lax.ppermute(value, "mem", [(i, (i + hop) % nmem) for i in range(nmem)]) for hop in range(1, nmem)
        ]

    block = pl.pallas_call(
        sort_kernel,
        in_specs=[VM] * 4,
        out_specs=VM,
        out_shape=shape((3, rows * width // LANES, LANES), F32),
        scratch_shapes=[pltpu.VMEM((rows, LANES), jnp.int32)] + [pltpu.VMEM((rows, LANES), F32)] * 2,
        compiler_params=params(),
        name="sort_slots",
    )(obs_cell, obs_weight, obs_mask, innovation)
    blocks = around_mem(block)
    obs, local, mine, other = pl.pallas_call(
        functools.partial(observe_kernel, width, nmem),
        in_specs=[VM] * (nmem + 1),
        out_specs=[VM] * 4,
        out_shape=[
            shape((3, rows, slots), F32),
            shape((2, rows, slots), F32),
            shape((half_count, rows, slots), F32),
            shape((half_count, rows, slots), F32),
        ],
        scratch_shapes=[pltpu.VMEM((nmem, *block.shape), F32)],
        compiler_params=params(),
        cost_estimate=cost(10**8, 4 * members.size),
        name="members_at_slots",
    )(*blocks, members)

    locals_ = direct(local)
    local_sib = swap(local, 1)
    received = swap(other, 1)
    seens = direct(mine) + direct(received)
    members_sib = swap(members, 1)

    lhs_high, lhs_low = pl.pallas_call(
        functools.partial(lat_kernel, order),
        in_specs=[VM],
        out_specs=[VM] * 2,
        out_shape=[shape((4 * rows, nlat), BF16)] * 2,
        scratch_shapes=[
            pltpu.VMEM((nlat, nlat), F32),
            pltpu.VMEM((2 * rows, nlat), F32),
            pltpu.VMEM((2 * rows, nlat), F32),
            pltpu.VMEM((nlat, 4 * rows), F32),
        ],
        compiler_params=params(),
        cost_estimate=cost(3 * 10**9, 8 * nlat * nlat),
        name="lat_rows",
    )(lat_root)
    cn_high, cn_low, lon_high, lon_low = pl.pallas_call(
        covariance_kernel,
        in_specs=[VM],
        out_specs=[VM] * 4,
        out_shape=[shape((lon, lon), BF16)] * 4,
        compiler_params=params(),
        cost_estimate=cost(6 * lon**3, 12 * lon * lon),
        name="lon_covariance",
    )(lon_root)

    nchunks = levels * nmem
    inverse, value = pl.pallas_call(
        functools.partial(inverse_kernel, width, levels, lon, nlat_dev // 2),
        in_specs=[VM] * (nlat_dev // 2),
        out_specs=[VM] * 2,
        out_shape=[shape((nchunks, nlat // 2, quarter), jnp.int32), shape((nlat // 2, slots), F32)],
        scratch_shapes=[pltpu.VMEM((nlat // 2, slots), jnp.int32)],
        compiler_params=params(),
        cost_estimate=cost(10**10, 2 * nlat * lon * levels),
        name="inverse",
    )(*locals_)
    inverses, values = [inverse, swap(inverse, 1)], [value, swap(value, 1)]

    tall = half_count * levels * rows

    def apply(pays):
        first = pays is None
        outs = (
            [shape((rows, slots), F32)] * 2
            + [shape((nmem, levels, rows, quarter), F32)] * 2
            + [shape((tall, lon), BF16)] * 4
        )
        if not first:
            outs.append(shape((8, LANES), F32))
        return pl.pallas_call(
            functools.partial(apply_kernel, width, levels, nlat_dev, first),
            in_specs=[ANY] * nlat_dev
            + ([] if first else [VM] * nlat_dev)
            + [VM] * 2
            + [ANY] * 2
            + [VM] * 4
            + [ANY] * 4,
            out_specs=[VM] * 4 + [ANY] * 4 + [VM] * (len(outs) - 8),
            out_shape=outs,
            scratch_shapes=[
                pltpu.VMEM((half_count, nlat, slots), F32),
                pltpu.VMEM((nlat, slots), F32),
                pltpu.VMEM((nchunks, nlat, quarter), jnp.int32),
                pltpu.VMEM((lon, lon), BF16),
                pltpu.VMEM((lon, lon), BF16),
                pltpu.VMEM((2, half_count, levels, rows, lon), F32),
            ]
            + [pltpu.VMEM((half_count, nlat, quarter), BF16)] * 4
            + [pltpu.VMEM((2 * tall, lon), BF16)] * 2
            + [pltpu.VMEM((2, tall, lon), BF16)] * 2
            + [
                pltpu.SemaphoreType.DMA((4,)),
                pltpu.SemaphoreType.DMA((nlat_dev,)),
                pltpu.SemaphoreType.DMA((nchunks, 2)),
                pltpu.SemaphoreType.DMA((2, 2)),
            ],
            compiler_params=params(),
            cost_estimate=cost(12 * tall * lon * (nlat + lon), 30 * 2**20),
            name="apply_first" if first else "apply_next",
        )(
            *seens,
            *([] if first else pays),
            *values,
            *inverses,
            lhs_high,
            lhs_low,
            local,
            local_sib,
            cn_high,
            cn_low,
            members,
            members_sib,
        )

    def to_quarters(image):
        total = image[0]
        for hop in range(1, nmem):
            total = total + lax.ppermute(image[hop], "mem", [(i, (i + hop) % nmem) for i in range(nmem)])
        return total

    def gradient(backs):
        field = (half_count, levels, rows, lon)
        other = product(backs[1], backs[3], lon_high, lon_low)
        mine = product(backs[0], backs[2], lon_high, lon_low)
        return mine.reshape(field), other.reshape(field)

    seen_own, seen_sib, image_own, image_sib, *backs0 = apply(None)
    seen_own = seen_own + swap(seen_sib, 1)
    parts = around_mem(seen_own)
    image_sib = swap(image_sib, 1)
    pay, seen0 = pl.pallas_call(
        functools.partial(answer_kernel, width, nmem),
        in_specs=[VM] * (nmem + 1),
        out_specs=[VM] * 2,
        out_shape=[shape((rows + 8, slots), F32), shape((rows, slots), F32)],
        compiler_params=params(),
        name="answer",
    )(*parts, obs)
    pays = direct(pay)
    mine0, other0 = gradient(backs0)
    pays = pays + [swap(block, 1) for block in pays]
    other0 = swap(other0, 1)
    quarter0 = to_quarters(image_own + image_sib)

    seen_own, seen_sib, image_own, image_sib, *backs1, length0 = apply(pays)
    seen_own = seen_own + swap(seen_sib, 1)
    parts = around_mem(seen_own)
    mine1, other1 = gradient(backs1)
    image_sib = swap(image_sib, 1)
    dots = pl.pallas_call(
        functools.partial(last_kernel, nmem),
        in_specs=[VM] * (nmem + 3),
        out_specs=VM,
        out_shape=shape((8, slots), F32),
        compiler_params=params(),
        name="last_dots",
    )(*parts, obs, seen0, length0)
    other1 = swap(other1, 1)
    quarter1 = to_quarters(image_own + image_sib)
    dots_parts = direct(dots)
    dots = sum(dots_parts[1:], dots_parts[0])
    dots = dots + swap(dots, 1)

    small = pl.BlockSpec((8, slots), lambda i, par: (0, 0))
    tiny = pl.BlockSpec((8, LANES), lambda i, par: (0, 0))
    piece = pl.BlockSpec((levels, rows, quarter), lambda i, par: (0, 0, 0))
    near = pl.BlockSpec((1, levels, rows, lon), lambda i, par: (jnp.minimum(i, half_count - 1), 0, 0, 0))
    far = pl.BlockSpec((1, levels, rows, lon), lambda i, par: (jnp.maximum(i - half_count, 0), 0, 0, 0))
    put = pl.BlockSpec((1, levels, rows, lon), lambda i, par: ((i + par[0] * half_count) % count, 0, 0, 0))
    return pl.pallas_call(
        final_kernel,
        grid_spec=pltpu.PrefetchScalarGridSpec(
            num_scalar_prefetch=1,
            grid=(count,),
            in_specs=[small, tiny, piece, piece, near, far, near, far],
            out_specs=[piece, put],
            scratch_shapes=[pltpu.VMEM((2, 8, LANES), F32)],
        ),
        out_shape=[shape((levels, rows, quarter), F32), shape(members.shape, F32)],
        compiler_params=params(),
        name="final",
    )(parity[None], dots, length0, quarter0, quarter1, mine0, other0, mine1, other1)


def solution(mesh):
    return jax.shard_map(
        per_device,
        mesh=mesh,
        in_specs=(
            P("mem", None, "lat", None),
            P(),
            P(),
            P("lat", "mem"),
            P("lat", "mem"),
            P("lat", "mem"),
            P("lat", "mem"),
        ),
        out_specs=(P(None, "lat", "mem"), P("mem", None, "lat", None)),
        check_vma=False,
    )
```

```python
import functools
import jax
import jax.numpy as jnp
from jax import lax
from jax.experimental import pallas as pl
from jax.experimental.pallas import tpu as pltpu
from jax.sharding import PartitionSpec as P


LANES = 128
HIGHEST = lax.Precision.HIGHEST
F32 = jnp.float32
BF16 = jnp.bfloat16
VMEM_LIMIT = 60 * 1024 * 1024


VM = pl.BlockSpec(memory_space=pltpu.VMEM)
ANY = pl.BlockSpec(memory_space=pl.ANY)


def params():
    return pltpu.CompilerParams(vmem_limit_bytes=VMEM_LIMIT)


def cost(flops, nbytes):
    return pl.CostEstimate(flops=flops, bytes_accessed=nbytes, transcendentals=0)


def take_lanes(values, index):
    numbers = lax.GatherDimensionNumbers(
        offset_dims=(),
        collapsed_slice_dims=(1,),
        start_index_map=(1,),
        operand_batching_dims=(0,),
        start_indices_batching_dims=(0,),
    )
    return lax.gather(
        values, index[..., None], numbers, slice_sizes=(1, 1), mode=lax.GatherScatterMode.PROMISE_IN_BOUNDS
    )


def split(value):
    high = value.astype(BF16)
    return high, (value - high.astype(F32)).astype(BF16)


def lane_iota(rows):
    return lax.broadcasted_iota(jnp.int32, (rows, LANES), 1)


def dot(a, b):
    return jnp.dot(a, b, preferred_element_type=F32)


def sort_kernel(cell_ref, weight_ref, mask_ref, innovation_ref, out_ref, cell, weight, value):
    rows, width = cell_ref.shape
    for scratch in (cell, weight, value):
        scratch[...] = jnp.zeros(scratch.shape, scratch.dtype)
    cell[:, :width] = cell_ref[...]
    used = weight_ref[...] * mask_ref[...].astype(F32)
    weight[:, :width] = used
    value[:, :width] = -(used * innovation_ref[...])
    lane = lane_iota(rows)
    key = cell[...] * width + lane % width
    block = 2
    while block <= width:
        hop = block // 2
        while hop:
            other = take_lanes(key, lane ^ hop)
            keep_low = ((lane & block) == 0) == ((lane & hop) == 0)
            if block == width:
                keep_low = (lane & hop) == 0
            key = jnp.where(keep_low, jnp.minimum(key, other), jnp.maximum(key, other))
            hop //= 2
        block *= 2
    slot = key % width
    per = LANES // width
    part = rows // per
    sorted_values = (
        (key // width).astype(F32),
        take_lanes(weight[...], slot),
        take_lanes(value[...], slot),
    )
    for kind, values in enumerate(sorted_values):
        values = jnp.where(lane < width, values, 0.0)
        total = values[:part]
        for side in range(1, per):
            total = total + pltpu.roll(values[side * part : (side + 1) * part], side * width, axis=1)
        out_ref[kind] = total


def run_totals(cells, values, width):
    hop = 1
    while hop < width:
        same = pltpu.roll(cells, LANES - hop, axis=1) == cells
        values = values + jnp.where(same, pltpu.roll(values, LANES - hop, axis=1), 0.0)
        hop *= 2
    return values


def pick_cells(cells, reads, width, levels, quarter, lon):
    per = LANES // width
    halves = quarter // LANES
    lane = lane_iota(cells.shape[0])
    position = cells % LANES
    kind = (cells // lon) * halves + (cells % quarter) // LANES
    outs = [jnp.zeros(cells.shape, F32) for _ in reads]
    for side in range(per):
        here = (lane // width) == side
        for level in range(levels):
            for half in range(halves):
                use = here & (kind == level * halves + half)
                outs = [
                    jnp.where(use, take_lanes(read(side, level, half), position), out)
                    for read, out in zip(reads, outs)
                ]
    return outs


def observe_kernel(width, nmem, *refs):
    block_refs, (members_ref, obs_ref, joint_ref, other_ref, blocks) = refs[:nmem], refs[nmem:]
    _, part, _ = block_refs[0].shape
    count, levels, rows, lon = members_ref.shape
    me = lax.axis_index("mem")
    parity = lax.axis_index("lat") % 2
    per = LANES // width
    quarter = lon // nmem
    for hop, ref in enumerate(block_refs):
        blocks[lax.rem(me - hop + nmem, nmem)] = ref[...]
    lane = lane_iota(part)
    for group in range(nmem // per):
        columns = slice(group * LANES, (group + 1) * LANES)
        for kind in range(3):
            for piece in range(per):
                total = jnp.zeros((part, LANES), F32)
                for side in range(per):
                    raw = blocks[group * per + side, kind]
                    turn = ((side - piece) * width) % LANES
                    if turn:
                        raw = pltpu.roll(raw, turn, axis=1)
                    total = jnp.where(lane // width == side, raw, total)
                obs_ref[kind, piece * part : (piece + 1) * part, columns] = total
        cells = obs_ref[0, :, columns].astype(jnp.int32)
        joint_ref[0, :, columns] = obs_ref[0, :, columns]
        joint_ref[1, :, columns] = run_totals(cells, obs_ref[2, :, columns], width)

    step = 8
    half_count = count // 2

    def one(index, carry):
        start = pl.multiple_of(index * step, step)
        here = pl.ds(start, step)
        for group in range(nmem // per):
            columns = slice(group * LANES, (group + 1) * LANES)
            cells = obs_ref[0, here, columns].astype(jnp.int32)

            def reader(member):
                def read(side, level, half):
                    first = (group * per + side) * quarter + half * LANES
                    return members_ref[member, level, here, first : first + LANES]

                return read

            order = [parity * half_count + i for i in range(half_count)]
            order += [(1 - parity) * half_count + i for i in range(half_count)]
            outs = pick_cells(cells, [reader(member) for member in order], width, levels, quarter, lon)
            for i in range(half_count):
                joint_ref[2 + i, here, columns] = outs[i]
                other_ref[i, here, columns] = outs[half_count + i]
        return carry

    lax.fori_loop(0, rows // step, one, 0)


def inverse_kernel(width, levels, lon, nblocks_lat, *refs):
    local_refs, (inverse_ref, value_ref, cells_all, local, sems) = refs[:nblocks_lat], refs[nblocks_lat:]
    _, _, rows, slots = local.shape
    copies = [
        pltpu.make_async_copy(ref.at[pl.ds(0, 2)], local.at[number], sems.at[number])
        for number, ref in enumerate(local_refs)
    ]
    for copy in copies:
        copy.start()
    for copy in copies:
        copy.wait()
    nblocks = slots // width
    quarter = lon // nblocks
    per = LANES // width
    tall = 16
    for number in range(nblocks_lat):
        value_ref[number * rows : (number + 1) * rows, :] = local[number, 1]
        cells_all[number * rows : (number + 1) * rows, :] = local[number, 0].astype(jnp.int32)

    def one(index, carry):
        here = pl.ds(pl.multiple_of(index * tall, tall), tall)
        lane = lane_iota(tall)
        for block in range(nblocks):
            group, offset = block // per, (block % per) * width
            cells = cells_all[here, group * LANES : (group + 1) * LANES]
            nothing = (offset - 1) % LANES
            for level in range(levels):
                for half in range(quarter // LANES):
                    target = lane + (level * lon + block * quarter + half * LANES)
                    place = jnp.full((tall, LANES), offset, jnp.int32)
                    hop = width // 2
                    while hop:
                        place = jnp.where(take_lanes(cells, place + (hop - 1)) < target, place + hop, place)
                        hop //= 2
                    found = take_lanes(cells, place) == target
                    inverse_ref[level * nblocks + block, here, half * LANES : (half + 1) * LANES] = jnp.where(
                        found, place, nothing
                    )
        return carry

    lax.fori_loop(0, cells_all.shape[0] // tall, one, 0)


def apply_kernel(width, levels, nlat_blocks, first, *refs):
    seen_refs = refs[:nlat_blocks]
    refs = refs[nlat_blocks:]
    if not first:
        pay_refs = refs[:nlat_blocks]
        refs = refs[nlat_blocks:]
    value_refs, inverse_refs = refs[:2], refs[2:4]
    lhs_high_ref, lhs_low_ref, local_refs, cn_high_ref, cn_low_ref = refs[4], refs[5], refs[6:8], refs[8], refs[9]
    members_ref, members_sib_ref = refs[10], refs[11]
    refs = refs[12:]
    seen_out_refs, image_refs = refs[:2], refs[2:4]
    back_high_refs, back_low_refs = refs[4:6], refs[6:8]
    refs = refs[8:]
    if not first:
        length_ref = refs[0]
        refs = refs[1:]
    (seen, value, inverse, cn_high, cn_low, members, xa_high, xa_low, xb_high, xb_low, w_high, w_low,
     back_high, back_low, sems, seen_sems, inv_sems, back_sems) = refs
    count, nlat, slots = seen.shape
    rows = nlat // nlat_blocks
    wide = 2 * rows
    nblocks = slots // width
    per = LANES // width
    nchunks = levels * nblocks
    quarter = inverse.shape[2]
    lon = quarter * nblocks
    parity = lax.axis_index("lat") % 2
    me_mem = lax.axis_index("mem")

    def rotated(block):
        return lax.rem(block - me_mem + nblocks, nblocks)

    half_blocks = nlat_blocks // 2
    seen_copies = [
        pltpu.make_async_copy(
            ref.at[pl.ds(2, count)] if number < half_blocks else ref,
            seen.at[:, pl.ds(number * rows, rows)],
            seen_sems.at[number],
        )
        for number, ref in enumerate(seen_refs)
    ]

    def inverse_copies(chunk):
        return [
            pltpu.make_async_copy(
                ref.at[chunk], inverse.at[chunk, pl.ds(side * (nlat // 2), nlat // 2)], inv_sems.at[chunk, side]
            )
            for side, ref in enumerate(inverse_refs)
        ]

    late = [
        pltpu.make_async_copy(cn_high_ref, cn_high, sems.at[0]),
        pltpu.make_async_copy(cn_low_ref, cn_low, sems.at[1]),
        pltpu.make_async_copy(members_ref.at[pl.ds(parity * count, count)], members.at[0], sems.at[2]),
        pltpu.make_async_copy(members_sib_ref.at[pl.ds(parity * count, count)], members.at[1], sems.at[3]),
    ]
    for copy in inverse_copies(0) + seen_copies + inverse_copies(1):
        copy.start()

    if first:
        for side, ref in enumerate(value_refs):
            value[side * (nlat // 2) : (side + 1) * (nlat // 2), :] = ref[...]
    else:
        top = jnp.zeros((1, slots), F32)
        bottom = jnp.zeros((1, slots), F32)
        for ref in pay_refs:
            top = top + ref[rows : rows + 1, :]
            bottom = bottom + ref[rows + 1 : rows + 2, :]
        length = jnp.sum(top, axis=1, keepdims=True) / jnp.sum(bottom, axis=1, keepdims=True)
        length_ref[...] = jnp.broadcast_to(length, length_ref.shape)
        per_side = nlat_blocks // 2
        for number, ref in enumerate(pay_refs):
            inside = (number % per_side) * rows
            old = value_refs[number // per_side][inside : inside + rows, :]
            value[number * rows : (number + 1) * rows, :] = old - length * (old + ref[:rows, :])

    tall = 16
    lane = lane_iota(tall)

    def build(chunk, x_high, x_low):
        block = lax.rem(chunk, nblocks)
        offset = lax.rem(block, per) * width
        columns = pl.ds(pl.multiple_of((block // per) * LANES, LANES), LANES)
        inside = (lane >= offset) & (lane < offset + width)
        for start in range(0, nlat, tall):
            part = slice(start, start + tall)
            numbers = value[part, columns]
            sources = [jnp.where(inside, seen[m, part, columns] * numbers, 0.0) for m in range(count)]
            for half in range(quarter // LANES):
                cols = slice(half * LANES, (half + 1) * LANES)
                index = inverse[chunk, part, cols]
                for m in range(count):
                    high, low = split(take_lanes(sources[m], index))
                    x_high[m, part, cols] = high
                    x_low[m, part, cols] = low

    def multiply(chunk, x_high, x_low):
        level = chunk // nblocks
        cols = pl.ds(pl.multiple_of(lax.rem(chunk, nblocks) * quarter, quarter), quarter)
        for m in range(count):
            both = (
                dot(lhs_high_ref[...], x_high[m])
                + dot(lhs_low_ref[...], x_high[m])
                + dot(lhs_high_ref[...], x_low[m])
            )
            high, low = split(both[:wide])
            where = pl.ds(pl.multiple_of((m * levels + level) * wide, wide), wide)
            w_high[where, cols] = high
            w_low[where, cols] = low
            where = pl.ds(pl.multiple_of((m * levels + level) * rows, rows), rows)
            for side in range(2):
                high, low = split(both[wide + side * rows : wide + (side + 1) * rows])
                back_high[side, where, cols] = high
                back_low[side, where, cols] = low

    for copy in inverse_copies(0) + seen_copies:
        copy.wait()
    for copy in inverse_copies(2):
        copy.start()
    build(0, xa_high, xa_low)

    def one(pair, carry):
        chunk = pair * 2
        for copy in inverse_copies(chunk + 1):
            copy.wait()

        @pl.when(chunk + 2 < nchunks)
        def _():
            for copy in inverse_copies(chunk + 2):
                copy.wait()
            for copy in inverse_copies(chunk + 3):
                copy.start()

        @pl.when(chunk + 4 < nchunks)
        def _():
            for copy in inverse_copies(chunk + 4):
                copy.start()

        @pl.when(pair == 0)
        def _():
            for copy in late:
                copy.start()

        build(chunk + 1, xb_high, xb_low)
        multiply(chunk, xa_high, xa_low)
        build(jnp.minimum(chunk + 2, nchunks - 1), xa_high, xa_low)
        multiply(chunk + 1, xb_high, xb_low)
        return carry

    lax.fori_loop(0, nchunks // 2, one, 0)

    back_copies = [
        pltpu.make_async_copy(source.at[side], refs_[side], back_sems.at[kind, side])
        for kind, (source, refs_) in enumerate(((back_high, back_high_refs), (back_low, back_low_refs)))
        for side in range(2)
    ]
    for copy in back_copies:
        copy.start()
    for copy in late:
        copy.wait()
    tile = 2 * LANES
    deep = levels * wide

    def panel(column, carry):
        begin = column * tile
        cols = pl.ds(pl.multiple_of(begin, tile), tile)
        place = rotated(begin // quarter)
        inner = pl.ds(pl.multiple_of(lax.rem(begin, quarter), tile), tile)
        totals = [[None] * levels for _ in range(2)]
        for member in range(count):
            part = slice(member * deep, (member + 1) * deep)
            product = (
                dot(w_high[part, :], cn_high[:, cols])
                + dot(w_low[part, :], cn_high[:, cols])
                + dot(w_high[part, :], cn_low[:, cols])
            )
            for level in range(levels):
                for side in range(2):
                    top = level * wide + side * rows
                    term = members[side, member, level, :, cols] * product[top : top + rows]
                    old = totals[side][level]
                    totals[side][level] = term if old is None else old + term
        for side in range(2):
            for level in range(levels):
                image_refs[side][place, level, :, inner] = totals[side][level]
        return carry

    lax.fori_loop(0, lon // tile, panel, 0)

    step = 8
    for side in range(2):
        for start in range(0, rows, step):
            part = slice(start, start + step)
            for group in range(nblocks // per):
                columns = slice(group * LANES, (group + 1) * LANES)
                cells = local_refs[side][0, part, columns].astype(jnp.int32)

                def read(piece, level, half):
                    return image_refs[side][
                        rotated(group * per + piece), level, part, half * LANES : (half + 1) * LANES
                    ]

                seen_out_refs[side][part, columns] = pick_cells(cells, [read], width, levels, quarter, lon)[0]
    for copy in back_copies:
        copy.wait()


def answer_kernel(width, nparts, *refs):
    parts, (obs_ref, pay_ref, seen_ref) = refs[:nparts], refs[nparts:]
    rows = obs_ref.shape[1]
    seen = parts[0][...]
    for part in parts[1:]:
        seen = seen + part[...]
    seen_ref[...] = seen
    weighted = obs_ref[1] * seen
    value = obs_ref[2]
    for group in range(seen.shape[1] // LANES):
        columns = slice(group * LANES, (group + 1) * LANES)
        cells = obs_ref[0, :, columns].astype(jnp.int32)
        pay_ref[:rows, columns] = run_totals(cells, weighted[:, columns], width)
    pay_ref[rows:, :] = jnp.zeros((8, seen.shape[1]), F32)
    pay_ref[rows : rows + 1, :] = jnp.sum(value * seen, axis=0, keepdims=True)
    pay_ref[rows + 1 : rows + 2, :] = jnp.sum(seen * (value + weighted), axis=0, keepdims=True)


def last_kernel(nparts, *refs):
    parts, (obs_ref, before_ref, length_ref, dots_ref) = refs[:nparts], refs[nparts:]
    seen = parts[0][...]
    for part in parts[1:]:
        seen = seen + part[...]
    weight, value = obs_ref[1], obs_ref[2]
    length = length_ref[:1, :1]
    value = value - length * (value + weight * before_ref[...])
    dots_ref[...] = jnp.zeros(dots_ref.shape, F32)
    dots_ref[:1, :] = jnp.sum(value * seen, axis=0, keepdims=True)
    dots_ref[1:2, :] = jnp.sum(seen * (value + weight * seen), axis=0, keepdims=True)


def lat_kernel(order, root_ref, high_ref, low_ref, turned, chip, columns, ordered):
    rows = chip.shape[0] // 2
    me = lax.axis_index("lat")
    turned[...] = root_ref[...].T
    for side in range(2):
        here = pl.ds(pl.multiple_of((me ^ side) * rows, rows), rows)
        chip[side * rows : (side + 1) * rows, :] = root_ref[here, :]
        columns[side * rows : (side + 1) * rows, :] = turned[here, :]
    covariance = lax.dot_general(
        chip[...], root_ref[...], (((1,), (1,)), ((), ())), precision=HIGHEST, preferred_element_type=F32
    )
    both = jnp.concatenate([covariance, columns[...]]).T
    turned[:, : both.shape[1]] = both
    for number, bits in enumerate(order):
        here = pl.ds(pl.multiple_of((me ^ bits) * rows, rows), rows)
        ordered[number * rows : (number + 1) * rows, :] = turned[here, : both.shape[1]]
    high_ref[...], low_ref[...] = split(ordered[...].T)


def covariance_kernel(root_ref, high_ref, low_ref, root_high_ref, root_low_ref, root_high, root_low):
    tile = high_ref.shape[1]
    numbers = (((1,), (1,)), ((), ()))

    @pl.when(pl.program_id(0) == 0)
    def _():
        root_high[...], root_low[...] = split(root_ref[...])

    def times(a, b):
        return lax.dot_general(a, b, numbers, preferred_element_type=F32)

    here = pl.ds(pl.multiple_of(pl.program_id(0) * tile, tile), tile)
    high, low = root_high[here, :], root_low[here, :]
    root_high_ref[...], root_low_ref[...] = high, low
    total = times(root_high[...], high) + times(root_low[...], high) + times(root_high[...], low)
    high_ref[...], low_ref[...] = split(total)


def product_kernel(a_high_ref, a_low_ref, b_high_ref, b_low_ref, out_ref):
    out_ref[...] = (
        dot(a_high_ref[...], b_high_ref[...])
        + dot(a_low_ref[...], b_high_ref[...])
        + dot(a_high_ref[...], b_low_ref[...])
    )


def product(a_high, a_low, b_high, b_low):
    rows, deep = a_high.shape
    wide = b_high.shape[1]
    tile = 2 * LANES
    whole = pl.BlockSpec((rows, deep), lambda i: (0, 0))
    panel = pl.BlockSpec((deep, tile), lambda i: (0, i))
    return pl.pallas_call(
        product_kernel,
        grid=(wide // tile,),
        in_specs=[whole, whole, panel, panel],
        out_specs=pl.BlockSpec((rows, tile), lambda i: (0, i)),
        out_shape=jax.ShapeDtypeStruct((rows, wide), F32),
        compiler_params=params(),
        cost_estimate=cost(6 * rows * deep * wide, 4 * (rows * deep + deep * wide + rows * wide)),
        name="lon_product",
    )(a_high, a_low, b_high, b_low)


def final_kernel(parity_ref, dots_ref, length_ref, q0_ref, q1_ref, a0_ref, b0_ref, a1_ref, b1_ref,
                 increment_ref, control_ref, lengths):
    index = pl.program_id(0)

    @pl.when(index == 0)
    def _():
        top = jnp.sum(dots_ref[:1, :], axis=1, keepdims=True)
        bottom = jnp.sum(dots_ref[1:2, :], axis=1, keepdims=True)
        lengths[0] = length_ref[...]
        lengths[1] = jnp.broadcast_to(top / bottom, length_ref.shape)
        increment_ref[...] = -(lengths[0, :1, :1] * q0_ref[...] + lengths[1, :1, :1] * q1_ref[...])

    half = pl.num_programs(0) // 2

    @pl.when(index < half)
    def _():
        control_ref[...] = -(lengths[0, :1, :1] * a0_ref[...] + lengths[1, :1, :1] * a1_ref[...])

    @pl.when(index >= half)
    def _():
        control_ref[...] = -(lengths[0, :1, :1] * b0_ref[...] + lengths[1, :1, :1] * b1_ref[...])


def per_device(members, lat_root, lon_root, innovation, obs_weight, obs_mask, obs_cell):
    count, levels, rows, lon = members.shape
    half_count = count // 2
    nmem, nlat_dev = lax.axis_size("mem"), lax.axis_size("lat")
    nlat = lat_root.shape[0]
    width = obs_cell.shape[1]
    slots = width * nmem
    quarter = lon // nmem
    me_lat = lax.axis_index("lat")
    parity = me_lat % 2
    shape = jax.ShapeDtypeStruct
    chips = list(range(0, nlat_dev, 2))
    order = chips + [bits + 1 for bits in chips]

    def swap(value, bits):
        return lax.ppermute(value, "lat", [(i, i ^ bits) for i in range(nlat_dev)])

    def direct(value):
        return [value] + [swap(value, bits) for bits in chips[1:]]

    def around_mem(value):
        return [value] + [
            lax.ppermute(value, "mem", [(i, (i + hop) % nmem) for i in range(nmem)]) for hop in range(1, nmem)
        ]

    block = pl.pallas_call(
        sort_kernel,
        in_specs=[VM] * 4,
        out_specs=VM,
        out_shape=shape((3, rows * width // LANES, LANES), F32),
        scratch_shapes=[pltpu.VMEM((rows, LANES), jnp.int32)] + [pltpu.VMEM((rows, LANES), F32)] * 2,
        compiler_params=params(),
        name="sort_slots",
    )(obs_cell, obs_weight, obs_mask, innovation)
    blocks = around_mem(block)
    obs, joint, other = pl.pallas_call(
        functools.partial(observe_kernel, width, nmem),
        in_specs=[VM] * (nmem + 1),
        out_specs=[VM] * 3,
        out_shape=[
            shape((3, rows, slots), F32),
            shape((2 + half_count, rows, slots), F32),
            shape((half_count, rows, slots), F32),
        ],
        scratch_shapes=[pltpu.VMEM((nmem, *block.shape), F32)],
        compiler_params=params(),
        cost_estimate=cost(10**8, 4 * members.size),
        name="members_at_slots",
    )(*blocks, members)

    received = swap(other, 1)
    joints = direct(joint)
    seens = joints + direct(received)
    obs_sib = swap(obs, 1)
    members_sib = swap(members, 1)

    lhs_high, lhs_low = pl.pallas_call(
        functools.partial(lat_kernel, order),
        in_specs=[VM],
        out_specs=[VM] * 2,
        out_shape=[shape((4 * rows, nlat), BF16)] * 2,
        scratch_shapes=[
            pltpu.VMEM((nlat, nlat), F32),
            pltpu.VMEM((2 * rows, nlat), F32),
            pltpu.VMEM((2 * rows, nlat), F32),
            pltpu.VMEM((nlat, 4 * rows), F32),
        ],
        compiler_params=params(),
        cost_estimate=cost(3 * 10**9, 8 * nlat * nlat),
        name="lat_rows",
    )(lat_root)
    cn_high, cn_low, lon_high, lon_low = pl.pallas_call(
        covariance_kernel,
        grid=(lon // (2 * LANES),),
        in_specs=[pl.BlockSpec((lon, lon), lambda i: (0, 0))],
        out_specs=[pl.BlockSpec((lon, 2 * LANES), lambda i: (0, i))] * 2
        + [pl.BlockSpec((2 * LANES, lon), lambda i: (i, 0))] * 2,
        out_shape=[shape((lon, lon), BF16)] * 4,
        scratch_shapes=[pltpu.VMEM((lon, lon), BF16)] * 2,
        compiler_params=params(),
        cost_estimate=cost(6 * lon**3, 12 * lon * lon),
        name="lon_covariance",
    )(lon_root)

    nchunks = levels * nmem
    inverse, value = pl.pallas_call(
        functools.partial(inverse_kernel, width, levels, lon, nlat_dev // 2),
        in_specs=[ANY] * (nlat_dev // 2),
        out_specs=[VM] * 2,
        out_shape=[shape((nchunks, nlat // 2, quarter), jnp.int32), shape((nlat // 2, slots), F32)],
        scratch_shapes=[
            pltpu.VMEM((nlat // 2, slots), jnp.int32),
            pltpu.VMEM((nlat_dev // 2, 2, rows, slots), F32),
            pltpu.SemaphoreType.DMA((nlat_dev // 2,)),
        ],
        compiler_params=params(),
        cost_estimate=cost(10**10, 2 * nlat * lon * levels),
        name="inverse",
    )(*joints)
    inverses, values = [inverse, swap(inverse, 1)], [value, swap(value, 1)]

    tall = half_count * levels * rows

    def apply(pays):
        first = pays is None
        outs = (
            [shape((rows, slots), F32)] * 2
            + [shape((nmem, levels, rows, quarter), F32)] * 2
            + [shape((tall, lon), BF16)] * 4
        )
        if not first:
            outs.append(shape((8, LANES), F32))
        return pl.pallas_call(
            functools.partial(apply_kernel, width, levels, nlat_dev, first),
            in_specs=[ANY] * nlat_dev
            + ([] if first else [VM] * nlat_dev)
            + [VM] * 2
            + [ANY] * 2
            + [VM] * 4
            + [ANY] * 4,
            out_specs=[VM] * 4 + [ANY] * 4 + [VM] * (len(outs) - 8),
            out_shape=outs,
            scratch_shapes=[
                pltpu.VMEM((half_count, nlat, slots), F32),
                pltpu.VMEM((nlat, slots), F32),
                pltpu.VMEM((nchunks, nlat, quarter), jnp.int32),
                pltpu.VMEM((lon, lon), BF16),
                pltpu.VMEM((lon, lon), BF16),
                pltpu.VMEM((2, half_count, levels, rows, lon), F32),
            ]
            + [pltpu.VMEM((half_count, nlat, quarter), BF16)] * 4
            + [pltpu.VMEM((2 * tall, lon), BF16)] * 2
            + [pltpu.VMEM((2, tall, lon), BF16)] * 2
            + [
                pltpu.SemaphoreType.DMA((4,)),
                pltpu.SemaphoreType.DMA((nlat_dev,)),
                pltpu.SemaphoreType.DMA((nchunks, 2)),
                pltpu.SemaphoreType.DMA((2, 2)),
            ],
            compiler_params=params(),
            cost_estimate=cost(12 * tall * lon * (nlat + lon), 30 * 2**20),
            name="apply_first" if first else "apply_next",
        )(
            *seens,
            *([] if first else pays),
            *values,
            *inverses,
            lhs_high,
            lhs_low,
            obs,
            obs_sib,
            cn_high,
            cn_low,
            members,
            members_sib,
        )

    def to_quarters(image):
        total = image[0]
        for hop in range(1, nmem):
            total = total + lax.ppermute(image[hop], "mem", [(i, (i + hop) % nmem) for i in range(nmem)])
        return total

    def gradient(backs):
        field = (half_count, levels, rows, lon)
        other = product(backs[1], backs[3], lon_high, lon_low)
        mine = product(backs[0], backs[2], lon_high, lon_low)
        return mine.reshape(field), other.reshape(field)

    seen_own, seen_sib, image_own, image_sib, *backs0 = apply(None)
    seen_own = seen_own + swap(seen_sib, 1)
    parts = around_mem(seen_own)
    image_sib = swap(image_sib, 1)
    pay, seen0 = pl.pallas_call(
        functools.partial(answer_kernel, width, nmem),
        in_specs=[VM] * (nmem + 1),
        out_specs=[VM] * 2,
        out_shape=[shape((rows + 8, slots), F32), shape((rows, slots), F32)],
        compiler_params=params(),
        name="answer",
    )(*parts, obs)
    pays = direct(pay)
    mine0, other0 = gradient(backs0)
    pays = pays + [swap(block, 1) for block in pays]
    other0 = swap(other0, 1)
    quarter0 = to_quarters(image_own + image_sib)

    seen_own, seen_sib, image_own, image_sib, *backs1, length0 = apply(pays)
    seen_own = seen_own + swap(seen_sib, 1)
    parts = around_mem(seen_own)
    mine1, other1 = gradient(backs1)
    image_sib = swap(image_sib, 1)
    dots = pl.pallas_call(
        functools.partial(last_kernel, nmem),
        in_specs=[VM] * (nmem + 3),
        out_specs=VM,
        out_shape=shape((8, slots), F32),
        compiler_params=params(),
        name="last_dots",
    )(*parts, obs, seen0, length0)
    other1 = swap(other1, 1)
    quarter1 = to_quarters(image_own + image_sib)
    dots_parts = direct(dots)
    dots = sum(dots_parts[1:], dots_parts[0])
    dots = dots + swap(dots, 1)

    small = pl.BlockSpec((8, slots), lambda i, par: (0, 0))
    tiny = pl.BlockSpec((8, LANES), lambda i, par: (0, 0))
    piece = pl.BlockSpec((levels, rows, quarter), lambda i, par: (0, 0, 0))
    near = pl.BlockSpec((1, levels, rows, lon), lambda i, par: (jnp.minimum(i, half_count - 1), 0, 0, 0))
    far = pl.BlockSpec((1, levels, rows, lon), lambda i, par: (jnp.maximum(i - half_count, 0), 0, 0, 0))
    put = pl.BlockSpec((1, levels, rows, lon), lambda i, par: ((i + par[0] * half_count) % count, 0, 0, 0))
    return pl.pallas_call(
        final_kernel,
        grid_spec=pltpu.PrefetchScalarGridSpec(
            num_scalar_prefetch=1,
            grid=(count,),
            in_specs=[small, tiny, piece, piece, near, far, near, far],
            out_specs=[piece, put],
            scratch_shapes=[pltpu.VMEM((2, 8, LANES), F32)],
        ),
        out_shape=[shape((levels, rows, quarter), F32), shape(members.shape, F32)],
        compiler_params=params(),
        name="final",
    )(parity[None], dots, length0, quarter0, quarter1, mine0, other0, mine1, other1)


def solution(mesh):
    return jax.shard_map(
        per_device,
        mesh=mesh,
        in_specs=(
            P("mem", None, "lat", None),
            P(),
            P(),
            P("lat", "mem"),
            P("lat", "mem"),
            P("lat", "mem"),
            P("lat", "mem"),
        ),
        out_specs=(P(None, "lat", "mem"), P("mem", None, "lat", None)),
        check_vma=False,
    )
```

```python
import functools
import jax
import jax.numpy as jnp
from jax import lax
from jax.experimental import pallas as pl
from jax.experimental.pallas import tpu as pltpu
from jax.sharding import PartitionSpec as P


LANES = 128
HIGHEST = lax.Precision.HIGHEST
F32 = jnp.float32
BF16 = jnp.bfloat16
MIB = 1024 * 1024
APPLY_LIMIT = 16


VM = pl.BlockSpec(memory_space=pltpu.VMEM)
ANY = pl.BlockSpec(memory_space=pl.ANY)


def params(limit=4):
    return pltpu.CompilerParams(vmem_limit_bytes=limit * MIB)


def cost(flops, nbytes):
    return pl.CostEstimate(flops=flops, bytes_accessed=nbytes, transcendentals=0)


def take_lanes(values, index):
    numbers = lax.GatherDimensionNumbers(
        offset_dims=(),
        collapsed_slice_dims=(1,),
        start_index_map=(1,),
        operand_batching_dims=(0,),
        start_indices_batching_dims=(0,),
    )
    return lax.gather(
        values, index[..., None], numbers, slice_sizes=(1, 1), mode=lax.GatherScatterMode.PROMISE_IN_BOUNDS
    )


def split(value):
    high = value.astype(BF16)
    return high, (value - high.astype(F32)).astype(BF16)


def lane_iota(rows):
    return lax.broadcasted_iota(jnp.int32, (rows, LANES), 1)


def dot(a, b):
    return jnp.dot(a, b, preferred_element_type=F32)


def sort_kernel(cell_ref, weight_ref, mask_ref, innovation_ref, out_ref, cell, weight, value):
    rows, width = cell_ref.shape
    for scratch in (cell, weight, value):
        scratch[...] = jnp.zeros(scratch.shape, scratch.dtype)
    cell[:, :width] = cell_ref[...]
    used = weight_ref[...] * mask_ref[...].astype(F32)
    weight[:, :width] = used
    value[:, :width] = -(used * innovation_ref[...])
    lane = lane_iota(rows)
    key = cell[...] * width + lane % width
    block = 2
    while block <= width:
        hop = block // 2
        while hop:
            other = take_lanes(key, lane ^ hop)
            keep_low = ((lane & block) == 0) == ((lane & hop) == 0)
            if block == width:
                keep_low = (lane & hop) == 0
            key = jnp.where(keep_low, jnp.minimum(key, other), jnp.maximum(key, other))
            hop //= 2
        block *= 2
    slot = key % width
    per = LANES // width
    part = rows // per
    sorted_values = (
        (key // width).astype(F32),
        take_lanes(weight[...], slot),
        take_lanes(value[...], slot),
    )
    for kind, values in enumerate(sorted_values):
        values = jnp.where(lane < width, values, 0.0)
        total = values[:part]
        for side in range(1, per):
            total = total + pltpu.roll(values[side * part : (side + 1) * part], side * width, axis=1)
        out_ref[kind] = total


def run_totals(cells, values, width):
    hop = 1
    while hop < width:
        same = pltpu.roll(cells, LANES - hop, axis=1) == cells
        values = values + jnp.where(same, pltpu.roll(values, LANES - hop, axis=1), 0.0)
        hop *= 2
    return values


def pick_cells(cells, reads, width, levels, quarter, lon):
    per = LANES // width
    halves = quarter // LANES
    lane = lane_iota(cells.shape[0])
    position = cells % LANES
    kind = (cells // lon) * halves + (cells % quarter) // LANES
    outs = [jnp.zeros(cells.shape, F32) for _ in reads]
    for side in range(per):
        here = (lane // width) == side
        for level in range(levels):
            for half in range(halves):
                use = here & (kind == level * halves + half)
                outs = [
                    jnp.where(use, take_lanes(read(side, level, half), position), out)
                    for read, out in zip(reads, outs)
                ]
    return outs


def observe_kernel(width, nmem, *refs):
    block_refs = refs[:nmem]
    members_ref, obs_ref, joint_ref, other_ref, members_mine_ref, members_other_ref, blocks = refs[nmem:]
    _, part, _ = block_refs[0].shape
    count, levels, rows, lon = members_ref.shape
    me = lax.axis_index("mem")
    parity = lax.axis_index("lat") % 2
    per = LANES // width
    quarter = lon // nmem
    for hop, ref in enumerate(block_refs):
        blocks[lax.rem(me - hop + nmem, nmem)] = ref[...]
    lane = lane_iota(part)
    for group in range(nmem // per):
        columns = slice(group * LANES, (group + 1) * LANES)
        for kind in range(3):
            for piece in range(per):
                total = jnp.zeros((part, LANES), F32)
                for side in range(per):
                    raw = blocks[group * per + side, kind]
                    turn = ((side - piece) * width) % LANES
                    if turn:
                        raw = pltpu.roll(raw, turn, axis=1)
                    total = jnp.where(lane // width == side, raw, total)
                obs_ref[kind, piece * part : (piece + 1) * part, columns] = total
        cells = obs_ref[0, :, columns].astype(jnp.int32)
        joint_ref[0, :, columns] = obs_ref[0, :, columns]
        joint_ref[1, :, columns] = run_totals(cells, obs_ref[2, :, columns], width)

    step = 8
    half_count = count // 2
    for i in range(half_count):
        members_mine_ref[i] = members_ref[parity * half_count + i]
        members_other_ref[i] = members_ref[(1 - parity) * half_count + i]

    def one(index, carry):
        start = pl.multiple_of(index * step, step)
        here = pl.ds(start, step)
        for group in range(nmem // per):
            columns = slice(group * LANES, (group + 1) * LANES)
            cells = obs_ref[0, here, columns].astype(jnp.int32)

            def reader(member):
                def read(side, level, half):
                    first = (group * per + side) * quarter + half * LANES
                    return members_ref[member, level, here, first : first + LANES]

                return read

            order = [parity * half_count + i for i in range(half_count)]
            order += [(1 - parity) * half_count + i for i in range(half_count)]
            outs = pick_cells(cells, [reader(member) for member in order], width, levels, quarter, lon)
            for i in range(half_count):
                joint_ref[2 + i, here, columns] = outs[i]
                other_ref[i, here, columns] = outs[half_count + i]
        return carry

    lax.fori_loop(0, rows // step, one, 0)


def inverse_kernel(width, levels, lon, nblocks_lat, *refs):
    local_refs, (inverse_ref, value_ref, cells_all, local, sems) = refs[:nblocks_lat], refs[nblocks_lat:]
    _, _, rows, slots = local.shape
    copies = [
        pltpu.make_async_copy(ref.at[pl.ds(0, 2)], local.at[number], sems.at[number])
        for number, ref in enumerate(local_refs)
    ]
    for copy in copies:
        copy.start()
    for copy in copies:
        copy.wait()
    nblocks = slots // width
    quarter = lon // nblocks
    per = LANES // width
    tall = 16
    for number in range(nblocks_lat):
        value_ref[number * rows : (number + 1) * rows, :] = local[number, 1]
        cells_all[number * rows : (number + 1) * rows, :] = local[number, 0].astype(jnp.int32)

    def one(index, carry):
        here = pl.ds(pl.multiple_of(index * tall, tall), tall)
        lane = lane_iota(tall)
        for block in range(nblocks):
            group, offset = block // per, (block % per) * width
            cells = cells_all[here, group * LANES : (group + 1) * LANES]
            nothing = (offset - 1) % LANES
            for level in range(levels):
                for half in range(quarter // LANES):
                    target = lane + (level * lon + block * quarter + half * LANES)
                    place = jnp.full((tall, LANES), offset, jnp.int32)
                    hop = width // 2
                    while hop:
                        place = jnp.where(take_lanes(cells, place + (hop - 1)) < target, place + hop, place)
                        hop //= 2
                    found = take_lanes(cells, place) == target
                    inverse_ref[level * nblocks + block, here, half * LANES : (half + 1) * LANES] = jnp.where(
                        found, place, nothing
                    )
        return carry

    lax.fori_loop(0, cells_all.shape[0] // tall, one, 0)


def apply_kernel(width, levels, nlat_blocks, first, *refs):
    seen_refs = refs[:nlat_blocks]
    refs = refs[nlat_blocks:]
    if not first:
        pay_refs = refs[:nlat_blocks]
        refs = refs[nlat_blocks:]
    value_refs, inverse_refs = refs[:2], refs[2:4]
    lhs_high_ref, lhs_low_ref, local_refs, cn_high_ref, cn_low_ref = refs[4], refs[5], refs[6:8], refs[8], refs[9]
    members_ref, members_sib_ref = refs[10], refs[11]
    refs = refs[12:]
    seen_out_refs, image_refs = refs[:2], refs[2:4]
    back_high_refs, back_low_refs = refs[4:6], refs[6:8]
    refs = refs[8:]
    if not first:
        length_ref = refs[0]
        refs = refs[1:]
    seen, value, xa_high, xa_low, xb_high, xb_low, w_high, w_low = refs
    count, nlat, slots = seen.shape
    rows = nlat // nlat_blocks
    wide = 2 * rows
    nblocks = slots // width
    per = LANES // width
    nchunks = levels * nblocks
    quarter = inverse_refs[0].shape[2]
    lon = quarter * nblocks
    me_mem = lax.axis_index("mem")
    members_refs = (members_ref, members_sib_ref)

    def rotated(block):
        return lax.rem(block - me_mem + nblocks, nblocks)

    half_blocks = nlat_blocks // 2
    for number, ref in enumerate(seen_refs):
        for m in range(count):
            seen[m, number * rows : (number + 1) * rows, :] = ref[m + 2 if number < half_blocks else m]
    if first:
        for side, ref in enumerate(value_refs):
            value[side * (nlat // 2) : (side + 1) * (nlat // 2), :] = ref[...]
    else:
        top = jnp.zeros((1, slots), F32)
        bottom = jnp.zeros((1, slots), F32)
        for ref in pay_refs:
            top = top + ref[rows : rows + 1, :]
            bottom = bottom + ref[rows + 1 : rows + 2, :]
        length = jnp.sum(top, axis=1, keepdims=True) / jnp.sum(bottom, axis=1, keepdims=True)
        length_ref[...] = jnp.broadcast_to(length, length_ref.shape)
        per_side = nlat_blocks // 2
        for number, ref in enumerate(pay_refs):
            inside = (number % per_side) * rows
            old = value_refs[number // per_side][inside : inside + rows, :]
            value[number * rows : (number + 1) * rows, :] = old - length * (old + ref[:rows, :])

    tall = 16
    lane = lane_iota(tall)

    def build(chunk, x_high, x_low):
        block = lax.rem(chunk, nblocks)
        offset = lax.rem(block, per) * width
        columns = pl.ds(pl.multiple_of((block // per) * LANES, LANES), LANES)
        inside = (lane >= offset) & (lane < offset + width)
        for start in range(0, nlat, tall):
            part = slice(start, start + tall)
            numbers = value[part, columns]
            sources = [jnp.where(inside, seen[m, part, columns] * numbers, 0.0) for m in range(count)]
            for half in range(quarter // LANES):
                cols = slice(half * LANES, (half + 1) * LANES)
                inner = start % (nlat // 2)
                index = inverse_refs[start // (nlat // 2)][chunk, inner : inner + tall, cols]
                for m in range(count):
                    high, low = split(take_lanes(sources[m], index))
                    x_high[m, part, cols] = high
                    x_low[m, part, cols] = low

    def multiply(chunk, x_high, x_low):
        level = chunk // nblocks
        cols = pl.ds(pl.multiple_of(lax.rem(chunk, nblocks) * quarter, quarter), quarter)
        for m in range(count):
            both = (
                dot(lhs_high_ref[...], x_high[m])
                + dot(lhs_low_ref[...], x_high[m])
                + dot(lhs_high_ref[...], x_low[m])
            )
            high, low = split(both[:wide])
            where = pl.ds(pl.multiple_of((m * levels + level) * wide, wide), wide)
            w_high[where, cols] = high
            w_low[where, cols] = low
            where = pl.ds(pl.multiple_of((m * levels + level) * rows, rows), rows)
            for side in range(2):
                high, low = split(both[wide + side * rows : wide + (side + 1) * rows])
                back_high_refs[side][where, cols] = high
                back_low_refs[side][where, cols] = low

    build(0, xa_high, xa_low)

    def one(pair, carry):
        chunk = pair * 2
        build(chunk + 1, xb_high, xb_low)
        multiply(chunk, xa_high, xa_low)
        build(jnp.minimum(chunk + 2, nchunks - 1), xa_high, xa_low)
        multiply(chunk + 1, xb_high, xb_low)
        return carry

    lax.fori_loop(0, nchunks // 2, one, 0)

    tile = 2 * LANES
    deep = levels * wide

    def panel(column, carry):
        begin = column * tile
        cols = pl.ds(pl.multiple_of(begin, tile), tile)
        place = rotated(begin // quarter)
        inner = pl.ds(pl.multiple_of(lax.rem(begin, quarter), tile), tile)
        totals = [[None] * levels for _ in range(2)]
        for member in range(count):
            part = slice(member * deep, (member + 1) * deep)
            product = (
                dot(w_high[part, :], cn_high_ref[:, cols])
                + dot(w_low[part, :], cn_high_ref[:, cols])
                + dot(w_high[part, :], cn_low_ref[:, cols])
            )
            for level in range(levels):
                for side in range(2):
                    top = level * wide + side * rows
                    term = members_refs[side][member, level, :, cols] * product[top : top + rows]
                    old = totals[side][level]
                    totals[side][level] = term if old is None else old + term
        for side in range(2):
            for level in range(levels):
                image_refs[side][place, level, :, inner] = totals[side][level]
        return carry

    lax.fori_loop(0, lon // tile, panel, 0)

    step = 8
    for side in range(2):
        for start in range(0, rows, step):
            part = slice(start, start + step)
            for group in range(nblocks // per):
                columns = slice(group * LANES, (group + 1) * LANES)
                cells = local_refs[side][0, part, columns].astype(jnp.int32)

                def read(piece, level, half):
                    return image_refs[side][
                        rotated(group * per + piece), level, part, half * LANES : (half + 1) * LANES
                    ]

                seen_out_refs[side][part, columns] = pick_cells(cells, [read], width, levels, quarter, lon)[0]


def answer_kernel(width, nparts, *refs):
    parts, (obs_ref, pay_ref, seen_ref) = refs[:nparts], refs[nparts:]
    rows = obs_ref.shape[1]
    seen = parts[0][...]
    for part in parts[1:]:
        seen = seen + part[...]
    seen_ref[...] = seen
    weighted = obs_ref[1] * seen
    value = obs_ref[2]
    for group in range(seen.shape[1] // LANES):
        columns = slice(group * LANES, (group + 1) * LANES)
        cells = obs_ref[0, :, columns].astype(jnp.int32)
        pay_ref[:rows, columns] = run_totals(cells, weighted[:, columns], width)
    pay_ref[rows:, :] = jnp.zeros((8, seen.shape[1]), F32)
    pay_ref[rows : rows + 1, :] = jnp.sum(value * seen, axis=0, keepdims=True)
    pay_ref[rows + 1 : rows + 2, :] = jnp.sum(seen * (value + weighted), axis=0, keepdims=True)


def last_kernel(nparts, *refs):
    parts, (obs_ref, before_ref, length_ref, dots_ref) = refs[:nparts], refs[nparts:]
    seen = parts[0][...]
    for part in parts[1:]:
        seen = seen + part[...]
    weight, value = obs_ref[1], obs_ref[2]
    length = length_ref[:1, :1]
    value = value - length * (value + weight * before_ref[...])
    dots_ref[...] = jnp.zeros(dots_ref.shape, F32)
    dots_ref[:1, :] = jnp.sum(value * seen, axis=0, keepdims=True)
    dots_ref[1:2, :] = jnp.sum(seen * (value + weight * seen), axis=0, keepdims=True)


def lat_kernel(order, root_ref, high_ref, low_ref, turned, chip, columns, ordered):
    rows = chip.shape[0] // 2
    me = lax.axis_index("lat")
    turned[...] = root_ref[...].T
    for side in range(2):
        here = pl.ds(pl.multiple_of((me ^ side) * rows, rows), rows)
        chip[side * rows : (side + 1) * rows, :] = root_ref[here, :]
        columns[side * rows : (side + 1) * rows, :] = turned[here, :]
    covariance = lax.dot_general(
        chip[...], root_ref[...], (((1,), (1,)), ((), ())), precision=HIGHEST, preferred_element_type=F32
    )
    both = jnp.concatenate([covariance, columns[...]]).T
    turned[:, : both.shape[1]] = both
    for number, bits in enumerate(order):
        here = pl.ds(pl.multiple_of((me ^ bits) * rows, rows), rows)
        ordered[number * rows : (number + 1) * rows, :] = turned[here, : both.shape[1]]
    high_ref[...], low_ref[...] = split(ordered[...].T)


def covariance_kernel(root_ref, high_ref, low_ref, root_high_ref, root_low_ref):
    tile = 2 * LANES
    numbers = (((1,), (1,)), ((), ()))
    root_high_ref[...], root_low_ref[...] = split(root_ref[...])

    def times(a, b):
        return lax.dot_general(a, b, numbers, preferred_element_type=F32)

    def panel(column, carry):
        here = pl.ds(pl.multiple_of(column * tile, tile), tile)
        high, low = root_high_ref[here, :], root_low_ref[here, :]
        total = times(root_high_ref[...], high) + times(root_low_ref[...], high) + times(root_high_ref[...], low)
        high_ref[:, here], low_ref[:, here] = split(total)
        return carry

    lax.fori_loop(0, root_ref.shape[0] // tile, panel, 0)


def product_kernel(a_high_ref, a_low_ref, b_high_ref, b_low_ref, out_ref):
    tile = 2 * LANES

    def panel(column, carry):
        here = pl.ds(pl.multiple_of(column * tile, tile), tile)
        out_ref[:, here] = (
            dot(a_high_ref[...], b_high_ref[:, here])
            + dot(a_low_ref[...], b_high_ref[:, here])
            + dot(a_high_ref[...], b_low_ref[:, here])
        )
        return carry

    lax.fori_loop(0, b_high_ref.shape[1] // tile, panel, 0)


def product(a_high, a_low, b_high, b_low):
    rows, deep = a_high.shape
    wide = b_high.shape[1]
    return pl.pallas_call(
        product_kernel,
        in_specs=[VM] * 4,
        out_specs=VM,
        out_shape=jax.ShapeDtypeStruct((rows, wide), F32),
        compiler_params=params(6),
        cost_estimate=cost(6 * rows * deep * wide, 4 * (rows * deep + deep * wide + rows * wide)),
        name="lon_product",
    )(a_high, a_low, b_high, b_low)


def final_kernel(dots_ref, length_ref, q0_ref, q1_ref, a0_ref, b0_ref, a1_ref, b1_ref,
                 increment_ref, control_ref, control, sems):
    parity = lax.axis_index("lat") % 2
    half = a0_ref.shape[0]
    length0 = length_ref[:1, :1]
    length1 = jnp.sum(dots_ref[:1, :], axis=1, keepdims=True) / jnp.sum(dots_ref[1:2, :], axis=1, keepdims=True)
    copies = []
    for side, (first_ref, second_ref) in enumerate(((a0_ref, a1_ref), (b0_ref, b1_ref))):
        for i in range(half):
            number = side * half + i
            member = (parity ^ side) * half + i
            control[number] = -(length0 * first_ref[i] + length1 * second_ref[i])
            copies.append(pltpu.make_async_copy(control.at[number], control_ref.at[member], sems.at[number]))
            copies[-1].start()
    increment_ref[...] = -(length0 * q0_ref[...] + length1 * q1_ref[...])
    for copy in copies:
        copy.wait()


def per_device(members, lat_root, lon_root, innovation, obs_weight, obs_mask, obs_cell):
    count, levels, rows, lon = members.shape
    half_count = count // 2
    nmem, nlat_dev = lax.axis_size("mem"), lax.axis_size("lat")
    nlat = lat_root.shape[0]
    width = obs_cell.shape[1]
    slots = width * nmem
    quarter = lon // nmem
    shape = jax.ShapeDtypeStruct
    chips = list(range(0, nlat_dev, 2))
    order = chips + [bits + 1 for bits in chips]

    def swap(value, bits):
        return lax.ppermute(value, "lat", [(i, i ^ bits) for i in range(nlat_dev)])

    def direct(value):
        return [value] + [swap(value, bits) for bits in chips[1:]]

    def around_mem(value):
        return [value] + [
            lax.ppermute(value, "mem", [(i, (i + hop) % nmem) for i in range(nmem)]) for hop in range(1, nmem)
        ]

    block = pl.pallas_call(
        sort_kernel,
        in_specs=[VM] * 4,
        out_specs=VM,
        out_shape=shape((3, rows * width // LANES, LANES), F32),
        scratch_shapes=[pltpu.VMEM((rows, LANES), jnp.int32)] + [pltpu.VMEM((rows, LANES), F32)] * 2,
        compiler_params=params(2),
        name="sort_slots",
    )(obs_cell, obs_weight, obs_mask, innovation)
    blocks = around_mem(block)
    obs, joint, other, members_mine, members_sib = pl.pallas_call(
        functools.partial(observe_kernel, width, nmem),
        in_specs=[VM] * (nmem + 1),
        out_specs=[VM] * 5,
        out_shape=[
            shape((3, rows, slots), F32),
            shape((2 + half_count, rows, slots), F32),
            shape((half_count, rows, slots), F32),
            shape((half_count, levels, rows, lon), F32),
            shape((half_count, levels, rows, lon), F32),
        ],
        scratch_shapes=[pltpu.VMEM((nmem, *block.shape), F32)],
        compiler_params=params(),
        cost_estimate=cost(10**8, 4 * members.size),
        name="members_at_slots",
    )(*blocks, members)

    received = swap(other, 1)
    joints = direct(joint)
    seens = joints + direct(received)
    obs_sib = swap(obs, 1)
    members_sib = swap(members_sib, 1)

    lhs_high, lhs_low = pl.pallas_call(
        functools.partial(lat_kernel, order),
        in_specs=[VM],
        out_specs=[VM] * 2,
        out_shape=[shape((4 * rows, nlat), BF16)] * 2,
        scratch_shapes=[
            pltpu.VMEM((nlat, nlat), F32),
            pltpu.VMEM((2 * rows, nlat), F32),
            pltpu.VMEM((2 * rows, nlat), F32),
            pltpu.VMEM((nlat, 4 * rows), F32),
        ],
        compiler_params=params(),
        cost_estimate=cost(3 * 10**9, 8 * nlat * nlat),
        name="lat_rows",
    )(lat_root)
    cn_high, cn_low, lon_high, lon_low = pl.pallas_call(
        covariance_kernel,
        in_specs=[VM],
        out_specs=[VM] * 4,
        out_shape=[shape((lon, lon), BF16)] * 4,
        compiler_params=params(6),
        cost_estimate=cost(6 * lon**3, 12 * lon * lon),
        name="lon_covariance",
    )(lon_root)

    nchunks = levels * nmem
    inverse, value = pl.pallas_call(
        functools.partial(inverse_kernel, width, levels, lon, nlat_dev // 2),
        in_specs=[ANY] * (nlat_dev // 2),
        out_specs=[VM] * 2,
        out_shape=[shape((nchunks, nlat // 2, quarter), jnp.int32), shape((nlat // 2, slots), F32)],
        scratch_shapes=[
            pltpu.VMEM((nlat // 2, slots), jnp.int32),
            pltpu.VMEM((nlat_dev // 2, 2, rows, slots), F32),
            pltpu.SemaphoreType.DMA((nlat_dev // 2,)),
        ],
        compiler_params=params(),
        cost_estimate=cost(10**10, 2 * nlat * lon * levels),
        name="inverse",
    )(*joints)
    inverses, values = [inverse, swap(inverse, 1)], [value, swap(value, 1)]

    tall = half_count * levels * rows

    def apply(pays):
        first = pays is None
        outs = (
            [shape((rows, slots), F32)] * 2
            + [shape((nmem, levels, rows, quarter), F32)] * 2
            + [shape((tall, lon), BF16)] * 4
        )
        if not first:
            outs.append(shape((8, LANES), F32))
        return pl.pallas_call(
            functools.partial(apply_kernel, width, levels, nlat_dev, first),
            in_specs=[VM] * (nlat_dev * (1 if first else 2) + 12),
            out_specs=[VM] * len(outs),
            out_shape=outs,
            scratch_shapes=[pltpu.VMEM((half_count, nlat, slots), F32), pltpu.VMEM((nlat, slots), F32)]
            + [pltpu.VMEM((half_count, nlat, quarter), BF16)] * 4
            + [pltpu.VMEM((2 * tall, lon), BF16)] * 2,
            compiler_params=params(APPLY_LIMIT),
            cost_estimate=cost(12 * tall * lon * (nlat + lon), 30 * 2**20),
            name="apply_first" if first else "apply_next",
        )(
            *seens,
            *([] if first else pays),
            *values,
            *inverses,
            lhs_high,
            lhs_low,
            obs,
            obs_sib,
            cn_high,
            cn_low,
            members_mine,
            members_sib,
        )

    def to_quarters(image):
        total = image[0]
        for hop in range(1, nmem):
            total = total + lax.ppermute(image[hop], "mem", [(i, (i + hop) % nmem) for i in range(nmem)])
        return total

    def gradient(backs):
        field = (half_count, levels, rows, lon)
        other = product(backs[1], backs[3], lon_high, lon_low)
        mine = product(backs[0], backs[2], lon_high, lon_low)
        return mine.reshape(field), other.reshape(field)

    seen_own, seen_sib, image_own, image_sib, *backs0 = apply(None)
    seen_own = seen_own + swap(seen_sib, 1)
    parts = around_mem(seen_own)
    image_sib = swap(image_sib, 1)
    pay, seen0 = pl.pallas_call(
        functools.partial(answer_kernel, width, nmem),
        in_specs=[VM] * (nmem + 1),
        out_specs=[VM] * 2,
        out_shape=[shape((rows + 8, slots), F32), shape((rows, slots), F32)],
        compiler_params=params(),
        name="answer",
    )(*parts, obs)
    pays = direct(pay)
    mine0, other0 = gradient(backs0)
    pays = pays + [swap(block, 1) for block in pays]
    other0 = swap(other0, 1)
    quarter0 = to_quarters(image_own + image_sib)

    seen_own, seen_sib, image_own, image_sib, *backs1, length0 = apply(pays)
    seen_own = seen_own + swap(seen_sib, 1)
    parts = around_mem(seen_own)
    mine1, other1 = gradient(backs1)
    image_sib = swap(image_sib, 1)
    dots = pl.pallas_call(
        functools.partial(last_kernel, nmem),
        in_specs=[VM] * (nmem + 3),
        out_specs=VM,
        out_shape=shape((8, slots), F32),
        compiler_params=params(),
        name="last_dots",
    )(*parts, obs, seen0, length0)
    other1 = swap(other1, 1)
    quarter1 = to_quarters(image_own + image_sib)
    dots_parts = direct(dots)
    dots = sum(dots_parts[1:], dots_parts[0])
    dots = dots + swap(dots, 1)

    return pl.pallas_call(
        final_kernel,
        in_specs=[VM] * 8,
        out_specs=[VM, ANY],
        out_shape=[shape((levels, rows, quarter), F32), shape(members.shape, F32)],
        scratch_shapes=[pltpu.VMEM(members.shape, F32), pltpu.SemaphoreType.DMA((count,))],
        compiler_params=params(8),
        name="final",
    )(dots, length0, quarter0, quarter1, mine0, other0, mine1, other1)


def solution(mesh):
    return jax.shard_map(
        per_device,
        mesh=mesh,
        in_specs=(
            P("mem", None, "lat", None),
            P(),
            P(),
            P("lat", "mem"),
            P("lat", "mem"),
            P("lat", "mem"),
            P("lat", "mem"),
        ),
        out_specs=(P(None, "lat", "mem"), P("mem", None, "lat", None)),
        check_vma=False,
    )
```

```python
import functools
import jax
import jax.numpy as jnp
from jax import lax
from jax.experimental import pallas as pl
from jax.experimental.pallas import tpu as pltpu
from jax.sharding import PartitionSpec as P


LANES = 128
HIGHEST = lax.Precision.HIGHEST
F32 = jnp.float32
BF16 = jnp.bfloat16
MIB = 1024 * 1024
APPLY_LIMIT = 16


VM = pl.BlockSpec(memory_space=pltpu.VMEM)
ANY = pl.BlockSpec(memory_space=pl.ANY)


def params(limit=4):
    return pltpu.CompilerParams(vmem_limit_bytes=limit * MIB)


def cost(flops, nbytes):
    return pl.CostEstimate(flops=flops, bytes_accessed=nbytes, transcendentals=0)


def take_lanes(values, index):
    numbers = lax.GatherDimensionNumbers(
        offset_dims=(),
        collapsed_slice_dims=(1,),
        start_index_map=(1,),
        operand_batching_dims=(0,),
        start_indices_batching_dims=(0,),
    )
    return lax.gather(
        values, index[..., None], numbers, slice_sizes=(1, 1), mode=lax.GatherScatterMode.PROMISE_IN_BOUNDS
    )


def split(value):
    high = value.astype(BF16)
    return high, (value - high.astype(F32)).astype(BF16)


def lane_iota(rows):
    return lax.broadcasted_iota(jnp.int32, (rows, LANES), 1)


def dot(a, b):
    return jnp.dot(a, b, preferred_element_type=F32)


def sort_kernel(*refs):
    sources, (out_ref, cell, weight, value), scratch, sems = refs[:4], refs[4:8], refs[8:12], refs[12]
    copies = [
        pltpu.make_async_copy(source, target, sems.at[i])
        for i, (source, target) in enumerate(zip(sources, scratch))
    ]
    for copy in copies:
        copy.start()
    for copy in copies:
        copy.wait()
    cell_ref, weight_ref, mask_ref, innovation_ref = scratch
    rows, width = cell_ref.shape
    for padded in (cell, weight, value):
        padded[...] = jnp.zeros(padded.shape, padded.dtype)
    cell[:, :width] = cell_ref[...]
    used = weight_ref[...] * mask_ref[...].astype(F32)
    weight[:, :width] = used
    value[:, :width] = -(used * innovation_ref[...])
    lane = lane_iota(rows)
    key = cell[...] * width + lane % width
    block = 2
    while block <= width:
        hop = block // 2
        while hop:
            other = take_lanes(key, lane ^ hop)
            keep_low = ((lane & block) == 0) == ((lane & hop) == 0)
            if block == width:
                keep_low = (lane & hop) == 0
            key = jnp.where(keep_low, jnp.minimum(key, other), jnp.maximum(key, other))
            hop //= 2
        block *= 2
    slot = key % width
    per = LANES // width
    part = rows // per
    sorted_values = (
        (key // width).astype(F32),
        take_lanes(weight[...], slot),
        take_lanes(value[...], slot),
    )
    for kind, values in enumerate(sorted_values):
        values = jnp.where(lane < width, values, 0.0)
        total = values[:part]
        for side in range(1, per):
            total = total + pltpu.roll(values[side * part : (side + 1) * part], side * width, axis=1)
        out_ref[kind] = total


def run_totals(cells, values, width):
    hop = 1
    while hop < width:
        same = pltpu.roll(cells, LANES - hop, axis=1) == cells
        values = values + jnp.where(same, pltpu.roll(values, LANES - hop, axis=1), 0.0)
        hop *= 2
    return values


def pick_cells(cells, reads, width, levels, quarter, lon):
    per = LANES // width
    halves = quarter // LANES
    lane = lane_iota(cells.shape[0])
    position = cells % LANES
    kind = (cells // lon) * halves + (cells % quarter) // LANES
    outs = [jnp.zeros(cells.shape, F32) for _ in reads]
    for side in range(per):
        here = (lane // width) == side
        for level in range(levels):
            for half in range(halves):
                use = here & (kind == level * halves + half)
                outs = [
                    jnp.where(use, take_lanes(read(side, level, half), position), out)
                    for read, out in zip(reads, outs)
                ]
    return outs


def observe_kernel(width, nmem, *refs):
    block_refs = refs[:nmem]
    members_ref, obs_ref, local_ref, mine_ref, other_ref, members_mine_ref, members_other_ref, blocks = refs[nmem:]
    _, part, _ = block_refs[0].shape
    count, levels, rows, lon = members_ref.shape
    me = lax.axis_index("mem")
    parity = lax.axis_index("lat") % 2
    per = LANES // width
    quarter = lon // nmem
    for hop, ref in enumerate(block_refs):
        blocks[lax.rem(me - hop + nmem, nmem)] = ref[...]
    lane = lane_iota(part)
    for group in range(nmem // per):
        columns = slice(group * LANES, (group + 1) * LANES)
        for kind in range(3):
            for piece in range(per):
                total = jnp.zeros((part, LANES), F32)
                for side in range(per):
                    raw = blocks[group * per + side, kind]
                    turn = ((side - piece) * width) % LANES
                    if turn:
                        raw = pltpu.roll(raw, turn, axis=1)
                    total = jnp.where(lane // width == side, raw, total)
                obs_ref[kind, piece * part : (piece + 1) * part, columns] = total
        cells = obs_ref[0, :, columns].astype(jnp.int32)
        local_ref[0, :, columns] = obs_ref[0, :, columns]
        local_ref[1, :, columns] = run_totals(cells, obs_ref[2, :, columns], width)

    step = 8
    half_count = count // 2
    for i in range(half_count):
        members_mine_ref[i] = members_ref[parity * half_count + i]
        members_other_ref[i] = members_ref[(1 - parity) * half_count + i]

    def one(index, carry):
        start = pl.multiple_of(index * step, step)
        here = pl.ds(start, step)
        for group in range(nmem // per):
            columns = slice(group * LANES, (group + 1) * LANES)
            cells = obs_ref[0, here, columns].astype(jnp.int32)

            def reader(member):
                def read(side, level, half):
                    first = (group * per + side) * quarter + half * LANES
                    return members_ref[member, level, here, first : first + LANES]

                return read

            order = [parity * half_count + i for i in range(half_count)]
            order += [(1 - parity) * half_count + i for i in range(half_count)]
            outs = pick_cells(cells, [reader(member) for member in order], width, levels, quarter, lon)
            for i in range(half_count):
                mine_ref[i, here, columns] = outs[i]
                other_ref[i, here, columns] = outs[half_count + i]
        return carry

    lax.fori_loop(0, rows // step, one, 0)


def inverse_kernel(width, levels, lon, nblocks_lat, *refs):
    local_refs, (inverse_ref, value_ref, cells_all) = refs[:nblocks_lat], refs[nblocks_lat:]
    _, rows, slots = local_refs[0].shape
    nblocks = slots // width
    quarter = lon // nblocks
    per = LANES // width
    tall = 16
    for number in range(nblocks_lat):
        value_ref[number * rows : (number + 1) * rows, :] = local_refs[number][1]
        cells_all[number * rows : (number + 1) * rows, :] = local_refs[number][0].astype(jnp.int32)

    def one(index, carry):
        here = pl.ds(pl.multiple_of(index * tall, tall), tall)
        lane = lane_iota(tall)
        for block in range(nblocks):
            group, offset = block // per, (block % per) * width
            cells = cells_all[here, group * LANES : (group + 1) * LANES]
            nothing = (offset - 1) % LANES
            for level in range(levels):
                for half in range(quarter // LANES):
                    target = lane + (level * lon + block * quarter + half * LANES)
                    place = jnp.full((tall, LANES), offset, jnp.int32)
                    hop = width // 2
                    while hop:
                        place = jnp.where(take_lanes(cells, place + (hop - 1)) < target, place + hop, place)
                        hop //= 2
                    found = take_lanes(cells, place) == target
                    inverse_ref[level * nblocks + block, here, half * LANES : (half + 1) * LANES] = jnp.where(
                        found, place, nothing
                    )
        return carry

    lax.fori_loop(0, cells_all.shape[0] // tall, one, 0)


def apply_kernel(width, levels, nlat_blocks, first, *refs):
    seen_refs = refs[:nlat_blocks]
    refs = refs[nlat_blocks:]
    if not first:
        pay_refs = refs[:nlat_blocks]
        refs = refs[nlat_blocks:]
    value_refs, inverse_refs = refs[:2], refs[2:4]
    lhs_high_ref, lhs_low_ref, local_refs, cn_high_ref, cn_low_ref = refs[4], refs[5], refs[6:8], refs[8], refs[9]
    members_ref, members_sib_ref = refs[10], refs[11]
    refs = refs[12:]
    seen_out_refs, image_refs = refs[:2], refs[2:4]
    back_high_refs, back_low_refs = refs[4:6], refs[6:8]
    refs = refs[8:]
    if not first:
        length_ref = refs[0]
        refs = refs[1:]
    seen, value, xa_high, xa_low, xb_high, xb_low, w_high, w_low = refs
    count, nlat, slots = seen.shape
    rows = nlat // nlat_blocks
    wide = 2 * rows
    nblocks = slots // width
    per = LANES // width
    nchunks = levels * nblocks
    quarter = inverse_refs[0].shape[2]
    lon = quarter * nblocks
    me_mem = lax.axis_index("mem")
    members_refs = (members_ref, members_sib_ref)

    def rotated(block):
        return lax.rem(block - me_mem + nblocks, nblocks)

    for number, ref in enumerate(seen_refs):
        seen[:, number * rows : (number + 1) * rows, :] = ref[...]
    if first:
        for side, ref in enumerate(value_refs):
            value[side * (nlat // 2) : (side + 1) * (nlat // 2), :] = ref[...]
    else:
        top = jnp.zeros((1, slots), F32)
        bottom = jnp.zeros((1, slots), F32)
        for ref in pay_refs:
            top = top + ref[rows : rows + 1, :]
            bottom = bottom + ref[rows + 1 : rows + 2, :]
        length = jnp.sum(top, axis=1, keepdims=True) / jnp.sum(bottom, axis=1, keepdims=True)
        length_ref[...] = jnp.broadcast_to(length, length_ref.shape)
        per_side = nlat_blocks // 2
        for number, ref in enumerate(pay_refs):
            inside = (number % per_side) * rows
            old = value_refs[number // per_side][inside : inside + rows, :]
            value[number * rows : (number + 1) * rows, :] = old - length * (old + ref[:rows, :])

    tall = 16
    lane = lane_iota(tall)

    def build(chunk, x_high, x_low):
        block = lax.rem(chunk, nblocks)
        offset = lax.rem(block, per) * width
        columns = pl.ds(pl.multiple_of((block // per) * LANES, LANES), LANES)
        inside = (lane >= offset) & (lane < offset + width)
        for start in range(0, nlat, tall):
            part = slice(start, start + tall)
            numbers = value[part, columns]
            sources = [jnp.where(inside, seen[m, part, columns] * numbers, 0.0) for m in range(count)]
            for half in range(quarter // LANES):
                cols = slice(half * LANES, (half + 1) * LANES)
                inner = start % (nlat // 2)
                index = inverse_refs[start // (nlat // 2)][chunk, inner : inner + tall, cols]
                for m in range(count):
                    high, low = split(take_lanes(sources[m], index))
                    x_high[m, part, cols] = high
                    x_low[m, part, cols] = low

    def multiply(chunk, x_high, x_low):
        level = chunk // nblocks
        cols = pl.ds(pl.multiple_of(lax.rem(chunk, nblocks) * quarter, quarter), quarter)
        for m in range(count):
            both = (
                dot(lhs_high_ref[...], x_high[m])
                + dot(lhs_low_ref[...], x_high[m])
                + dot(lhs_high_ref[...], x_low[m])
            )
            high, low = split(both[:wide])
            where = pl.ds(pl.multiple_of((m * levels + level) * wide, wide), wide)
            w_high[where, cols] = high
            w_low[where, cols] = low
            where = pl.ds(pl.multiple_of((m * levels + level) * rows, rows), rows)
            for side in range(2):
                high, low = split(both[wide + side * rows : wide + (side + 1) * rows])
                back_high_refs[side][where, cols] = high
                back_low_refs[side][where, cols] = low

    build(0, xa_high, xa_low)

    def one(pair, carry):
        chunk = pair * 2
        build(chunk + 1, xb_high, xb_low)
        multiply(chunk, xa_high, xa_low)
        build(jnp.minimum(chunk + 2, nchunks - 1), xa_high, xa_low)
        multiply(chunk + 1, xb_high, xb_low)
        return carry

    lax.fori_loop(0, nchunks // 2, one, 0)

    tile = 2 * LANES
    deep = levels * wide

    def panel(column, carry):
        begin = column * tile
        cols = pl.ds(pl.multiple_of(begin, tile), tile)
        place = rotated(begin // quarter)
        inner = pl.ds(pl.multiple_of(lax.rem(begin, quarter), tile), tile)
        totals = [[None] * levels for _ in range(2)]
        for member in range(count):
            part = slice(member * deep, (member + 1) * deep)
            product = (
                dot(w_high[part, :], cn_high_ref[:, cols])
                + dot(w_low[part, :], cn_high_ref[:, cols])
                + dot(w_high[part, :], cn_low_ref[:, cols])
            )
            for level in range(levels):
                for side in range(2):
                    top = level * wide + side * rows
                    term = members_refs[side][member, level, :, cols] * product[top : top + rows]
                    old = totals[side][level]
                    totals[side][level] = term if old is None else old + term
        for side in range(2):
            for level in range(levels):
                image_refs[side][place, level, :, inner] = totals[side][level]
        return carry

    lax.fori_loop(0, lon // tile, panel, 0)

    step = 8
    for side in range(2):
        for start in range(0, rows, step):
            part = slice(start, start + step)
            for group in range(nblocks // per):
                columns = slice(group * LANES, (group + 1) * LANES)
                cells = local_refs[side][0, part, columns].astype(jnp.int32)

                def read(piece, level, half):
                    return image_refs[side][
                        rotated(group * per + piece), level, part, half * LANES : (half + 1) * LANES
                    ]

                seen_out_refs[side][part, columns] = pick_cells(cells, [read], width, levels, quarter, lon)[0]


def answer_kernel(width, nparts, *refs):
    parts, (obs_ref, pay_ref, seen_ref) = refs[:nparts], refs[nparts:]
    rows = obs_ref.shape[1]
    seen = parts[0][...]
    for part in parts[1:]:
        seen = seen + part[...]
    seen_ref[...] = seen
    weighted = obs_ref[1] * seen
    value = obs_ref[2]
    for group in range(seen.shape[1] // LANES):
        columns = slice(group * LANES, (group + 1) * LANES)
        cells = obs_ref[0, :, columns].astype(jnp.int32)
        pay_ref[:rows, columns] = run_totals(cells, weighted[:, columns], width)
    pay_ref[rows:, :] = jnp.zeros((8, seen.shape[1]), F32)
    pay_ref[rows : rows + 1, :] = jnp.sum(value * seen, axis=0, keepdims=True)
    pay_ref[rows + 1 : rows + 2, :] = jnp.sum(seen * (value + weighted), axis=0, keepdims=True)


def last_kernel(nparts, *refs):
    parts, (obs_ref, before_ref, length_ref, dots_ref) = refs[:nparts], refs[nparts:]
    seen = parts[0][...]
    for part in parts[1:]:
        seen = seen + part[...]
    weight, value = obs_ref[1], obs_ref[2]
    length = length_ref[:1, :1]
    value = value - length * (value + weight * before_ref[...])
    dots_ref[...] = jnp.zeros(dots_ref.shape, F32)
    dots_ref[:1, :] = jnp.sum(value * seen, axis=0, keepdims=True)
    dots_ref[1:2, :] = jnp.sum(seen * (value + weight * seen), axis=0, keepdims=True)


def lat_kernel(order, root_ref, high_ref, low_ref, turned, chip, columns, ordered):
    rows = chip.shape[0] // 2
    me = lax.axis_index("lat")
    turned[...] = root_ref[...].T
    for side in range(2):
        here = pl.ds(pl.multiple_of((me ^ side) * rows, rows), rows)
        chip[side * rows : (side + 1) * rows, :] = root_ref[here, :]
        columns[side * rows : (side + 1) * rows, :] = turned[here, :]
    covariance = lax.dot_general(
        chip[...], root_ref[...], (((1,), (1,)), ((), ())), precision=HIGHEST, preferred_element_type=F32
    )
    both = jnp.concatenate([covariance, columns[...]]).T
    turned[:, : both.shape[1]] = both
    for number, bits in enumerate(order):
        here = pl.ds(pl.multiple_of((me ^ bits) * rows, rows), rows)
        ordered[number * rows : (number + 1) * rows, :] = turned[here, : both.shape[1]]
    high_ref[...], low_ref[...] = split(ordered[...].T)


def covariance_kernel(root_ref, high_ref, low_ref, root_high_ref, root_low_ref):
    tile = 2 * LANES
    numbers = (((1,), (1,)), ((), ()))
    root_high_ref[...], root_low_ref[...] = split(root_ref[...])

    def times(a, b):
        return lax.dot_general(a, b, numbers, preferred_element_type=F32)

    def panel(column, carry):
        here = pl.ds(pl.multiple_of(column * tile, tile), tile)
        high, low = root_high_ref[here, :], root_low_ref[here, :]
        total = times(root_high_ref[...], high) + times(root_low_ref[...], high) + times(root_high_ref[...], low)
        high_ref[:, here], low_ref[:, here] = split(total)
        return carry

    lax.fori_loop(0, root_ref.shape[0] // tile, panel, 0)


def product_kernel(a_high_ref, a_low_ref, b_high_ref, b_low_ref, out_ref):
    tile = 2 * LANES

    def panel(column, carry):
        here = pl.ds(pl.multiple_of(column * tile, tile), tile)
        out_ref[:, here] = (
            dot(a_high_ref[...], b_high_ref[:, here])
            + dot(a_low_ref[...], b_high_ref[:, here])
            + dot(a_high_ref[...], b_low_ref[:, here])
        )
        return carry

    lax.fori_loop(0, b_high_ref.shape[1] // tile, panel, 0)


def product(a_high, a_low, b_high, b_low):
    rows, deep = a_high.shape
    wide = b_high.shape[1]
    return pl.pallas_call(
        product_kernel,
        in_specs=[VM] * 4,
        out_specs=VM,
        out_shape=jax.ShapeDtypeStruct((rows, wide), F32),
        compiler_params=params(6),
        cost_estimate=cost(6 * rows * deep * wide, 4 * (rows * deep + deep * wide + rows * wide)),
        name="lon_product",
    )(a_high, a_low, b_high, b_low)


def final_kernel(dots_ref, length_ref, q0_ref, q1_ref, a0_ref, b0_ref, a1_ref, b1_ref,
                 increment_ref, control_ref, control, sems):
    parity = lax.axis_index("lat") % 2
    half = a0_ref.shape[0]
    length0 = length_ref[:1, :1]
    length1 = jnp.sum(dots_ref[:1, :], axis=1, keepdims=True) / jnp.sum(dots_ref[1:2, :], axis=1, keepdims=True)
    copies = []
    for side, (first_ref, second_ref) in enumerate(((a0_ref, a1_ref), (b0_ref, b1_ref))):
        for i in range(half):
            number = side * half + i
            member = (parity ^ side) * half + i
            control[number] = -(length0 * first_ref[i] + length1 * second_ref[i])
            copies.append(pltpu.make_async_copy(control.at[number], control_ref.at[member], sems.at[number]))
            copies[-1].start()
    increment_ref[...] = -(length0 * q0_ref[...] + length1 * q1_ref[...])
    for copy in copies:
        copy.wait()


def per_device(members, lat_root, lon_root, innovation, obs_weight, obs_mask, obs_cell):
    count, levels, rows, lon = members.shape
    half_count = count // 2
    nmem, nlat_dev = lax.axis_size("mem"), lax.axis_size("lat")
    nlat = lat_root.shape[0]
    width = obs_cell.shape[1]
    slots = width * nmem
    quarter = lon // nmem
    shape = jax.ShapeDtypeStruct
    chips = list(range(0, nlat_dev, 2))
    order = chips + [bits + 1 for bits in chips]

    def swap(value, bits):
        return lax.ppermute(value, "lat", [(i, i ^ bits) for i in range(nlat_dev)])

    def direct(value):
        return [value] + [swap(value, bits) for bits in chips[1:]]

    def around_mem(value):
        return [value] + [
            lax.ppermute(value, "mem", [(i, (i + hop) % nmem) for i in range(nmem)]) for hop in range(1, nmem)
        ]

    block = pl.pallas_call(
        sort_kernel,
        in_specs=[ANY] * 4,
        out_specs=VM,
        out_shape=shape((3, rows * width // LANES, LANES), F32),
        scratch_shapes=[pltpu.VMEM((rows, LANES), jnp.int32)]
        + [pltpu.VMEM((rows, LANES), F32)] * 2
        + [pltpu.VMEM(value.shape, value.dtype) for value in (obs_cell, obs_weight, obs_mask, innovation)]
        + [pltpu.SemaphoreType.DMA((4,))],
        compiler_params=params(2),
        name="sort_slots",
    )(obs_cell, obs_weight, obs_mask, innovation)
    blocks = around_mem(block)
    obs, local, mine, other, members_mine, members_sib = pl.pallas_call(
        functools.partial(observe_kernel, width, nmem),
        in_specs=[VM] * (nmem + 1),
        out_specs=[VM] * 6,
        out_shape=[
            shape((3, rows, slots), F32),
            shape((2, rows, slots), F32),
            shape((half_count, rows, slots), F32),
            shape((half_count, rows, slots), F32),
            shape((half_count, levels, rows, lon), F32),
            shape((half_count, levels, rows, lon), F32),
        ],
        scratch_shapes=[pltpu.VMEM((nmem, *block.shape), F32)],
        compiler_params=params(),
        cost_estimate=cost(10**8, 4 * members.size),
        name="members_at_slots",
    )(*blocks, members)

    locals_ = direct(local)
    received = swap(other, 1)
    seens = direct(mine)
    seens = seens + direct(received)
    obs_sib = swap(obs, 1)
    members_sib = swap(members_sib, 1)

    lhs_high, lhs_low = pl.pallas_call(
        functools.partial(lat_kernel, order),
        in_specs=[VM],
        out_specs=[VM] * 2,
        out_shape=[shape((4 * rows, nlat), BF16)] * 2,
        scratch_shapes=[
            pltpu.VMEM((nlat, nlat), F32),
            pltpu.VMEM((2 * rows, nlat), F32),
            pltpu.VMEM((2 * rows, nlat), F32),
            pltpu.VMEM((nlat, 4 * rows), F32),
        ],
        compiler_params=params(),
        cost_estimate=cost(3 * 10**9, 8 * nlat * nlat),
        name="lat_rows",
    )(lat_root)
    cn_high, cn_low, lon_high, lon_low = pl.pallas_call(
        covariance_kernel,
        in_specs=[VM],
        out_specs=[VM] * 4,
        out_shape=[shape((lon, lon), BF16)] * 4,
        compiler_params=params(6),
        cost_estimate=cost(6 * lon**3, 12 * lon * lon),
        name="lon_covariance",
    )(lon_root)

    nchunks = levels * nmem
    inverse, value = pl.pallas_call(
        functools.partial(inverse_kernel, width, levels, lon, nlat_dev // 2),
        in_specs=[VM] * (nlat_dev // 2),
        out_specs=[VM] * 2,
        out_shape=[shape((nchunks, nlat // 2, quarter), jnp.int32), shape((nlat // 2, slots), F32)],
        scratch_shapes=[pltpu.VMEM((nlat // 2, slots), jnp.int32)],
        compiler_params=params(),
        cost_estimate=cost(10**10, 2 * nlat * lon * levels),
        name="inverse",
    )(*locals_)
    inverses, values = [inverse, swap(inverse, 1)], [value, swap(value, 1)]

    tall = half_count * levels * rows

    def apply(pays):
        first = pays is None
        outs = (
            [shape((rows, slots), F32)] * 2
            + [shape((nmem, levels, rows, quarter), F32)] * 2
            + [shape((tall, lon), BF16)] * 4
        )
        if not first:
            outs.append(shape((8, LANES), F32))
        return pl.pallas_call(
            functools.partial(apply_kernel, width, levels, nlat_dev, first),
            in_specs=[VM] * (nlat_dev * (1 if first else 2) + 12),
            out_specs=[VM] * len(outs),
            out_shape=outs,
            scratch_shapes=[pltpu.VMEM((half_count, nlat, slots), F32), pltpu.VMEM((nlat, slots), F32)]
            + [pltpu.VMEM((half_count, nlat, quarter), BF16)] * 4
            + [pltpu.VMEM((2 * tall, lon), BF16)] * 2,
            compiler_params=params(APPLY_LIMIT),
            cost_estimate=cost(12 * tall * lon * (nlat + lon), 30 * 2**20),
            name="apply_first" if first else "apply_next",
        )(
            *seens,
            *([] if first else pays),
            *values,
            *inverses,
            lhs_high,
            lhs_low,
            obs,
            obs_sib,
            cn_high,
            cn_low,
            members_mine,
            members_sib,
        )

    def to_quarters(image):
        total = image[0]
        for hop in range(1, nmem):
            total = total + lax.ppermute(image[hop], "mem", [(i, (i + hop) % nmem) for i in range(nmem)])
        return total

    def gradient(backs):
        field = (half_count, levels, rows, lon)
        other = product(backs[1], backs[3], lon_high, lon_low)
        mine = product(backs[0], backs[2], lon_high, lon_low)
        return mine.reshape(field), other.reshape(field)

    seen_own, seen_sib, image_own, image_sib, *backs0 = apply(None)
    seen_own = seen_own + swap(seen_sib, 1)
    parts = around_mem(seen_own)
    image_sib = swap(image_sib, 1)
    pay, seen0 = pl.pallas_call(
        functools.partial(answer_kernel, width, nmem),
        in_specs=[VM] * (nmem + 1),
        out_specs=[VM] * 2,
        out_shape=[shape((rows + 8, slots), F32), shape((rows, slots), F32)],
        compiler_params=params(),
        name="answer",
    )(*parts, obs)
    pays = direct(pay)
    mine0, other0 = gradient(backs0)
    pays = pays + [swap(block, 1) for block in pays]
    other0 = swap(other0, 1)
    quarter0 = to_quarters(image_own + image_sib)

    seen_own, seen_sib, image_own, image_sib, *backs1, length0 = apply(pays)
    seen_own = seen_own + swap(seen_sib, 1)
    parts = around_mem(seen_own)
    mine1, other1 = gradient(backs1)
    image_sib = swap(image_sib, 1)
    dots = pl.pallas_call(
        functools.partial(last_kernel, nmem),
        in_specs=[VM] * (nmem + 3),
        out_specs=VM,
        out_shape=shape((8, slots), F32),
        compiler_params=params(),
        name="last_dots",
    )(*parts, obs, seen0, length0)
    other1 = swap(other1, 1)
    quarter1 = to_quarters(image_own + image_sib)
    dots_parts = direct(dots)
    dots = sum(dots_parts[1:], dots_parts[0])
    dots = dots + swap(dots, 1)

    return pl.pallas_call(
        final_kernel,
        in_specs=[VM] * 8,
        out_specs=[VM, ANY],
        out_shape=[shape((levels, rows, quarter), F32), shape(members.shape, F32)],
        scratch_shapes=[pltpu.VMEM(members.shape, F32), pltpu.SemaphoreType.DMA((count,))],
        compiler_params=params(8),
        name="final",
    )(dots, length0, quarter0, quarter1, mine0, other0, mine1, other1)


def solution(mesh):
    return jax.shard_map(
        per_device,
        mesh=mesh,
        in_specs=(
            P("mem", None, "lat", None),
            P(),
            P(),
            P("lat", "mem"),
            P("lat", "mem"),
            P("lat", "mem"),
            P("lat", "mem"),
        ),
        out_specs=(P(None, "lat", "mem"), P("mem", None, "lat", None)),
        check_vma=False,
    )
```

```python
import functools
import jax
import jax.numpy as jnp
from jax import lax
from jax.experimental import pallas as pl
from jax.experimental.pallas import tpu as pltpu
from jax.sharding import PartitionSpec as P


LANES = 128
HIGHEST = lax.Precision.HIGHEST
F32 = jnp.float32
BF16 = jnp.bfloat16
MIB = 1024 * 1024
APPLY_LIMIT = 16


VM = pl.BlockSpec(memory_space=pltpu.VMEM)
ANY = pl.BlockSpec(memory_space=pl.ANY)


def params(limit=4):
    return pltpu.CompilerParams(vmem_limit_bytes=limit * MIB)


def cost(flops, nbytes):
    return pl.CostEstimate(flops=flops, bytes_accessed=nbytes, transcendentals=0)


def take_lanes(values, index):
    numbers = lax.GatherDimensionNumbers(
        offset_dims=(),
        collapsed_slice_dims=(1,),
        start_index_map=(1,),
        operand_batching_dims=(0,),
        start_indices_batching_dims=(0,),
    )
    return lax.gather(
        values, index[..., None], numbers, slice_sizes=(1, 1), mode=lax.GatherScatterMode.PROMISE_IN_BOUNDS
    )


def split(value):
    high = value.astype(BF16)
    return high, (value - high.astype(F32)).astype(BF16)


def lane_iota(rows):
    return lax.broadcasted_iota(jnp.int32, (rows, LANES), 1)


def dot(a, b):
    return jnp.dot(a, b, preferred_element_type=F32)


def sort_kernel(*refs):
    sources, (out_ref, cell, weight, value), scratch, sems = refs[:4], refs[4:8], refs[8:12], refs[12]
    copies = [
        pltpu.make_async_copy(source, target, sems.at[i])
        for i, (source, target) in enumerate(zip(sources, scratch))
    ]
    for copy in copies:
        copy.start()
    for copy in copies:
        copy.wait()
    cell_ref, weight_ref, mask_ref, innovation_ref = scratch
    rows, width = cell_ref.shape
    for padded in (cell, weight, value):
        padded[...] = jnp.zeros(padded.shape, padded.dtype)
    cell[:, :width] = cell_ref[...]
    used = weight_ref[...] * mask_ref[...].astype(F32)
    weight[:, :width] = used
    value[:, :width] = -(used * innovation_ref[...])
    lane = lane_iota(rows)
    key = cell[...] * width + lane % width
    block = 2
    while block <= width:
        hop = block // 2
        while hop:
            other = take_lanes(key, lane ^ hop)
            keep_low = ((lane & block) == 0) == ((lane & hop) == 0)
            if block == width:
                keep_low = (lane & hop) == 0
            key = jnp.where(keep_low, jnp.minimum(key, other), jnp.maximum(key, other))
            hop //= 2
        block *= 2
    slot = key % width
    per = LANES // width
    part = rows // per
    sorted_values = (
        (key // width).astype(F32),
        take_lanes(weight[...], slot),
        take_lanes(value[...], slot),
    )
    for kind, values in enumerate(sorted_values):
        values = jnp.where(lane < width, values, 0.0)
        total = values[:part]
        for side in range(1, per):
            total = total + pltpu.roll(values[side * part : (side + 1) * part], side * width, axis=1)
        out_ref[kind] = total


def run_totals(cells, values, width):
    hop = 1
    while hop < width:
        same = pltpu.roll(cells, LANES - hop, axis=1) == cells
        values = values + jnp.where(same, pltpu.roll(values, LANES - hop, axis=1), 0.0)
        hop *= 2
    return values


def pick_cells(cells, reads, width, levels, quarter, lon):
    per = LANES // width
    halves = quarter // LANES
    lane = lane_iota(cells.shape[0])
    position = cells % LANES
    kind = (cells // lon) * halves + (cells % quarter) // LANES
    outs = [jnp.zeros(cells.shape, F32) for _ in reads]
    for side in range(per):
        here = (lane // width) == side
        for level in range(levels):
            for half in range(halves):
                use = here & (kind == level * halves + half)
                outs = [
                    jnp.where(use, take_lanes(read(side, level, half), position), out)
                    for read, out in zip(reads, outs)
                ]
    return outs


def observe_kernel(width, nmem, *refs):
    block_refs = refs[:nmem]
    members_ref, obs_ref, local_ref, mine_ref, other_ref, members_mine_ref, members_other_ref, blocks = refs[nmem:]
    _, part, _ = block_refs[0].shape
    count, levels, rows, lon = members_ref.shape
    me = lax.axis_index("mem")
    parity = lax.axis_index("lat") % 2
    per = LANES // width
    quarter = lon // nmem
    for hop, ref in enumerate(block_refs):
        blocks[lax.rem(me - hop + nmem, nmem)] = ref[...]
    lane = lane_iota(part)
    for group in range(nmem // per):
        columns = slice(group * LANES, (group + 1) * LANES)
        for kind in range(3):
            for piece in range(per):
                total = jnp.zeros((part, LANES), F32)
                for side in range(per):
                    raw = blocks[group * per + side, kind]
                    turn = ((side - piece) * width) % LANES
                    if turn:
                        raw = pltpu.roll(raw, turn, axis=1)
                    total = jnp.where(lane // width == side, raw, total)
                obs_ref[kind, piece * part : (piece + 1) * part, columns] = total
        cells = obs_ref[0, :, columns].astype(jnp.int32)
        local_ref[0, :, columns] = obs_ref[0, :, columns]
        local_ref[1, :, columns] = run_totals(cells, obs_ref[2, :, columns], width)

    step = 8
    half_count = count // 2
    for i in range(half_count):
        members_mine_ref[i] = members_ref[parity * half_count + i]
        members_other_ref[i] = members_ref[(1 - parity) * half_count + i]

    def one(index, carry):
        start = pl.multiple_of(index * step, step)
        here = pl.ds(start, step)
        for group in range(nmem // per):
            columns = slice(group * LANES, (group + 1) * LANES)
            cells = obs_ref[0, here, columns].astype(jnp.int32)

            def reader(member):
                def read(side, level, half):
                    first = (group * per + side) * quarter + half * LANES
                    return members_ref[member, level, here, first : first + LANES]

                return read

            order = [parity * half_count + i for i in range(half_count)]
            order += [(1 - parity) * half_count + i for i in range(half_count)]
            outs = pick_cells(cells, [reader(member) for member in order], width, levels, quarter, lon)
            for i in range(half_count):
                mine_ref[i, here, columns] = outs[i]
                other_ref[i, here, columns] = outs[half_count + i]
        return carry

    lax.fori_loop(0, rows // step, one, 0)


def inverse_kernel(width, levels, lon, nblocks_lat, *refs):
    local_refs, (inverse_ref, value_ref, cells_all) = refs[:nblocks_lat], refs[nblocks_lat:]
    _, rows, slots = local_refs[0].shape
    nblocks = slots // width
    quarter = lon // nblocks
    per = LANES // width
    tall = 16
    for number in range(nblocks_lat):
        value_ref[number * rows : (number + 1) * rows, :] = local_refs[number][1]
        cells_all[number * rows : (number + 1) * rows, :] = local_refs[number][0].astype(jnp.int32)

    def one(index, carry):
        here = pl.ds(pl.multiple_of(index * tall, tall), tall)
        lane = lane_iota(tall)
        for block in range(nblocks):
            group, offset = block // per, (block % per) * width
            cells = cells_all[here, group * LANES : (group + 1) * LANES]
            nothing = (offset - 1) % LANES
            for level in range(levels):
                for half in range(quarter // LANES):
                    target = lane + (level * lon + block * quarter + half * LANES)
                    place = jnp.full((tall, LANES), offset, jnp.int32)
                    hop = width // 2
                    while hop:
                        place = jnp.where(take_lanes(cells, place + (hop - 1)) < target, place + hop, place)
                        hop //= 2
                    found = take_lanes(cells, place) == target
                    inverse_ref[level * nblocks + block, here, half * LANES : (half + 1) * LANES] = jnp.where(
                        found, place, nothing
                    )
        return carry

    lax.fori_loop(0, cells_all.shape[0] // tall, one, 0)


def apply_kernel(width, levels, nlat_blocks, first, *refs):
    seen_refs = refs[: nlat_blocks // 2]
    refs = refs[nlat_blocks // 2 :]
    if not first:
        pay_refs = refs[:nlat_blocks]
        refs = refs[nlat_blocks:]
    value_refs, inverse_refs = refs[:2], refs[2:4]
    lhs_high_ref, lhs_low_ref, local_refs, cn_high_ref, cn_low_ref = refs[4], refs[5], refs[6:8], refs[8], refs[9]
    members_ref, members_sib_ref = refs[10], refs[11]
    refs = refs[12:]
    seen_out_refs, image_refs = refs[:2], refs[2:4]
    back_high_refs, back_low_refs = refs[4:6], refs[6:8]
    refs = refs[8:]
    if not first:
        length_ref = refs[0]
        refs = refs[1:]
    seen, value, xa_high, xa_low, xb_high, xb_low, w_high, w_low = refs
    count, nlat, slots = seen.shape
    rows = nlat // nlat_blocks
    wide = 2 * rows
    nblocks = slots // width
    per = LANES // width
    nchunks = levels * nblocks
    quarter = inverse_refs[0].shape[2]
    lon = quarter * nblocks
    me_mem = lax.axis_index("mem")
    members_refs = (members_ref, members_sib_ref)

    def rotated(block):
        return lax.rem(block - me_mem + nblocks, nblocks)

    half_blocks = nlat_blocks // 2
    for number, ref in enumerate(seen_refs):
        for side in range(2):
            begin = (side * half_blocks + number) * rows
            seen[:, begin : begin + rows, :] = ref[side * count : (side + 1) * count]
    if first:
        for side, ref in enumerate(value_refs):
            value[side * (nlat // 2) : (side + 1) * (nlat // 2), :] = ref[...]
    else:
        top = jnp.zeros((1, slots), F32)
        bottom = jnp.zeros((1, slots), F32)
        for ref in pay_refs:
            top = top + ref[rows : rows + 1, :]
            bottom = bottom + ref[rows + 1 : rows + 2, :]
        length = jnp.sum(top, axis=1, keepdims=True) / jnp.sum(bottom, axis=1, keepdims=True)
        length_ref[...] = jnp.broadcast_to(length, length_ref.shape)
        per_side = nlat_blocks // 2
        for number, ref in enumerate(pay_refs):
            inside = (number % per_side) * rows
            old = value_refs[number // per_side][inside : inside + rows, :]
            value[number * rows : (number + 1) * rows, :] = old - length * (old + ref[:rows, :])

    tall = 16
    lane = lane_iota(tall)

    def build(chunk, x_high, x_low):
        block = lax.rem(chunk, nblocks)
        offset = lax.rem(block, per) * width
        columns = pl.ds(pl.multiple_of((block // per) * LANES, LANES), LANES)
        inside = (lane >= offset) & (lane < offset + width)
        for start in range(0, nlat, tall):
            part = slice(start, start + tall)
            numbers = value[part, columns]
            sources = [jnp.where(inside, seen[m, part, columns] * numbers, 0.0) for m in range(count)]
            for half in range(quarter // LANES):
                cols = slice(half * LANES, (half + 1) * LANES)
                inner = start % (nlat // 2)
                index = inverse_refs[start // (nlat // 2)][chunk, inner : inner + tall, cols]
                for m in range(count):
                    high, low = split(take_lanes(sources[m], index))
                    x_high[m, part, cols] = high
                    x_low[m, part, cols] = low

    def multiply(chunk, x_high, x_low):
        level = chunk // nblocks
        cols = pl.ds(pl.multiple_of(lax.rem(chunk, nblocks) * quarter, quarter), quarter)
        for m in range(count):
            both = (
                dot(lhs_high_ref[...], x_high[m])
                + dot(lhs_low_ref[...], x_high[m])
                + dot(lhs_high_ref[...], x_low[m])
            )
            high, low = split(both[:wide])
            where = pl.ds(pl.multiple_of((m * levels + level) * wide, wide), wide)
            w_high[where, cols] = high
            w_low[where, cols] = low
            where = pl.ds(pl.multiple_of((m * levels + level) * rows, rows), rows)
            for side in range(2):
                high, low = split(both[wide + side * rows : wide + (side + 1) * rows])
                back_high_refs[side][where, cols] = high
                back_low_refs[side][where, cols] = low

    build(0, xa_high, xa_low)

    def one(pair, carry):
        chunk = pair * 2
        build(chunk + 1, xb_high, xb_low)
        multiply(chunk, xa_high, xa_low)
        build(jnp.minimum(chunk + 2, nchunks - 1), xa_high, xa_low)
        multiply(chunk + 1, xb_high, xb_low)
        return carry

    lax.fori_loop(0, nchunks // 2, one, 0)

    tile = 2 * LANES
    deep = levels * wide

    def panel(column, carry):
        begin = column * tile
        cols = pl.ds(pl.multiple_of(begin, tile), tile)
        place = rotated(begin // quarter)
        inner = pl.ds(pl.multiple_of(lax.rem(begin, quarter), tile), tile)
        totals = [[None] * levels for _ in range(2)]
        for member in range(count):
            part = slice(member * deep, (member + 1) * deep)
            product = (
                dot(w_high[part, :], cn_high_ref[:, cols])
                + dot(w_low[part, :], cn_high_ref[:, cols])
                + dot(w_high[part, :], cn_low_ref[:, cols])
            )
            for level in range(levels):
                for side in range(2):
                    top = level * wide + side * rows
                    term = members_refs[side][member, level, :, cols] * product[top : top + rows]
                    old = totals[side][level]
                    totals[side][level] = term if old is None else old + term
        for side in range(2):
            for level in range(levels):
                image_refs[side][place, level, :, inner] = totals[side][level]
        return carry

    lax.fori_loop(0, lon // tile, panel, 0)

    step = 8
    for side in range(2):
        for start in range(0, rows, step):
            part = slice(start, start + step)
            for group in range(nblocks // per):
                columns = slice(group * LANES, (group + 1) * LANES)
                cells = local_refs[side][0, part, columns].astype(jnp.int32)

                def read(piece, level, half):
                    return image_refs[side][
                        rotated(group * per + piece), level, part, half * LANES : (half + 1) * LANES
                    ]

                seen_out_refs[side][part, columns] = pick_cells(cells, [read], width, levels, quarter, lon)[0]


def answer_kernel(width, nparts, *refs):
    parts, (obs_ref, pay_ref, seen_ref) = refs[:nparts], refs[nparts:]
    rows = obs_ref.shape[1]
    seen = parts[0][...]
    for part in parts[1:]:
        seen = seen + part[...]
    seen_ref[...] = seen
    weighted = obs_ref[1] * seen
    value = obs_ref[2]
    for group in range(seen.shape[1] // LANES):
        columns = slice(group * LANES, (group + 1) * LANES)
        cells = obs_ref[0, :, columns].astype(jnp.int32)
        pay_ref[:rows, columns] = run_totals(cells, weighted[:, columns], width)
    pay_ref[rows:, :] = jnp.zeros((8, seen.shape[1]), F32)
    pay_ref[rows : rows + 1, :] = jnp.sum(value * seen, axis=0, keepdims=True)
    pay_ref[rows + 1 : rows + 2, :] = jnp.sum(seen * (value + weighted), axis=0, keepdims=True)


def last_kernel(nparts, *refs):
    parts, (obs_ref, before_ref, length_ref, dots_ref) = refs[:nparts], refs[nparts:]
    seen = parts[0][...]
    for part in parts[1:]:
        seen = seen + part[...]
    weight, value = obs_ref[1], obs_ref[2]
    length = length_ref[:1, :1]
    value = value - length * (value + weight * before_ref[...])
    dots_ref[...] = jnp.zeros(dots_ref.shape, F32)
    dots_ref[:1, :] = jnp.sum(value * seen, axis=0, keepdims=True)
    dots_ref[1:2, :] = jnp.sum(seen * (value + weight * seen), axis=0, keepdims=True)


def lat_kernel(order, root_ref, high_ref, low_ref, turned, chip, columns, ordered):
    rows = chip.shape[0] // 2
    me = lax.axis_index("lat")
    turned[...] = root_ref[...].T
    for side in range(2):
        here = pl.ds(pl.multiple_of((me ^ side) * rows, rows), rows)
        chip[side * rows : (side + 1) * rows, :] = root_ref[here, :]
        columns[side * rows : (side + 1) * rows, :] = turned[here, :]
    covariance = lax.dot_general(
        chip[...], root_ref[...], (((1,), (1,)), ((), ())), precision=HIGHEST, preferred_element_type=F32
    )
    both = jnp.concatenate([covariance, columns[...]]).T
    turned[:, : both.shape[1]] = both
    for number, bits in enumerate(order):
        here = pl.ds(pl.multiple_of((me ^ bits) * rows, rows), rows)
        ordered[number * rows : (number + 1) * rows, :] = turned[here, : both.shape[1]]
    high_ref[...], low_ref[...] = split(ordered[...].T)


def covariance_kernel(root_ref, high_ref, low_ref, root_high_ref, root_low_ref):
    tile = 2 * LANES
    numbers = (((1,), (1,)), ((), ()))
    root_high_ref[...], root_low_ref[...] = split(root_ref[...])

    def times(a, b):
        return lax.dot_general(a, b, numbers, preferred_element_type=F32)

    def panel(column, carry):
        here = pl.ds(pl.multiple_of(column * tile, tile), tile)
        high, low = root_high_ref[here, :], root_low_ref[here, :]
        total = times(root_high_ref[...], high) + times(root_low_ref[...], high) + times(root_high_ref[...], low)
        high_ref[:, here], low_ref[:, here] = split(total)
        return carry

    lax.fori_loop(0, root_ref.shape[0] // tile, panel, 0)


def product_kernel(a_high_ref, a_low_ref, b_high_ref, b_low_ref, out_ref):
    tile = 2 * LANES

    def panel(column, carry):
        here = pl.ds(pl.multiple_of(column * tile, tile), tile)
        out_ref[:, here] = (
            dot(a_high_ref[...], b_high_ref[:, here])
            + dot(a_low_ref[...], b_high_ref[:, here])
            + dot(a_high_ref[...], b_low_ref[:, here])
        )
        return carry

    lax.fori_loop(0, b_high_ref.shape[1] // tile, panel, 0)


def product(a_high, a_low, b_high, b_low):
    rows, deep = a_high.shape
    wide = b_high.shape[1]
    return pl.pallas_call(
        product_kernel,
        in_specs=[VM] * 4,
        out_specs=VM,
        out_shape=jax.ShapeDtypeStruct((rows, wide), F32),
        compiler_params=params(6),
        cost_estimate=cost(6 * rows * deep * wide, 4 * (rows * deep + deep * wide + rows * wide)),
        name="lon_product",
    )(a_high, a_low, b_high, b_low)


def final_kernel(dots_ref, length_ref, q0_ref, q1_ref, a0_ref, b0_ref, a1_ref, b1_ref,
                 increment_ref, control_ref, control, sems):
    parity = lax.axis_index("lat") % 2
    half = a0_ref.shape[0]
    length0 = length_ref[:1, :1]
    length1 = jnp.sum(dots_ref[:1, :], axis=1, keepdims=True) / jnp.sum(dots_ref[1:2, :], axis=1, keepdims=True)
    copies = []
    for side, (first_ref, second_ref) in enumerate(((a0_ref, a1_ref), (b0_ref, b1_ref))):
        for i in range(half):
            number = side * half + i
            member = (parity ^ side) * half + i
            control[number] = -(length0 * first_ref[i] + length1 * second_ref[i])
            copies.append(pltpu.make_async_copy(control.at[number], control_ref.at[member], sems.at[number]))
            copies[-1].start()
    increment_ref[...] = -(length0 * q0_ref[...] + length1 * q1_ref[...])
    for copy in copies:
        copy.wait()


def per_device(members, lat_root, lon_root, innovation, obs_weight, obs_mask, obs_cell):
    count, levels, rows, lon = members.shape
    half_count = count // 2
    nmem, nlat_dev = lax.axis_size("mem"), lax.axis_size("lat")
    nlat = lat_root.shape[0]
    width = obs_cell.shape[1]
    slots = width * nmem
    quarter = lon // nmem
    shape = jax.ShapeDtypeStruct
    chips = list(range(0, nlat_dev, 2))
    order = chips + [bits + 1 for bits in chips]

    def swap(value, bits):
        return lax.ppermute(value, "lat", [(i, i ^ bits) for i in range(nlat_dev)])

    def direct(value):
        return [value] + [swap(value, bits) for bits in chips[1:]]

    def around_mem(value):
        return [value] + [
            lax.ppermute(value, "mem", [(i, (i + hop) % nmem) for i in range(nmem)]) for hop in range(1, nmem)
        ]

    block = pl.pallas_call(
        sort_kernel,
        in_specs=[ANY] * 4,
        out_specs=VM,
        out_shape=shape((3, rows * width // LANES, LANES), F32),
        scratch_shapes=[pltpu.VMEM((rows, LANES), jnp.int32)]
        + [pltpu.VMEM((rows, LANES), F32)] * 2
        + [pltpu.VMEM(value.shape, value.dtype) for value in (obs_cell, obs_weight, obs_mask, innovation)]
        + [pltpu.SemaphoreType.DMA((4,))],
        compiler_params=params(2),
        name="sort_slots",
    )(obs_cell, obs_weight, obs_mask, innovation)
    blocks = around_mem(block)
    obs, local, mine, other, members_mine, members_sib = pl.pallas_call(
        functools.partial(observe_kernel, width, nmem),
        in_specs=[VM] * (nmem + 1),
        out_specs=[VM] * 6,
        out_shape=[
            shape((3, rows, slots), F32),
            shape((2, rows, slots), F32),
            shape((half_count, rows, slots), F32),
            shape((half_count, rows, slots), F32),
            shape((half_count, levels, rows, lon), F32),
            shape((half_count, levels, rows, lon), F32),
        ],
        scratch_shapes=[pltpu.VMEM((nmem, *block.shape), F32)],
        compiler_params=params(),
        cost_estimate=cost(10**8, 4 * members.size),
        name="members_at_slots",
    )(*blocks, members)

    locals_ = direct(local)
    received = swap(other, 1)
    seens = direct(jnp.concatenate([mine, received]))
    obs_sib = swap(obs, 1)
    members_sib = swap(members_sib, 1)

    lhs_high, lhs_low = pl.pallas_call(
        functools.partial(lat_kernel, order),
        in_specs=[VM],
        out_specs=[VM] * 2,
        out_shape=[shape((4 * rows, nlat), BF16)] * 2,
        scratch_shapes=[
            pltpu.VMEM((nlat, nlat), F32),
            pltpu.VMEM((2 * rows, nlat), F32),
            pltpu.VMEM((2 * rows, nlat), F32),
            pltpu.VMEM((nlat, 4 * rows), F32),
        ],
        compiler_params=params(),
        cost_estimate=cost(3 * 10**9, 8 * nlat * nlat),
        name="lat_rows",
    )(lat_root)
    cn_high, cn_low, lon_high, lon_low = pl.pallas_call(
        covariance_kernel,
        in_specs=[VM],
        out_specs=[VM] * 4,
        out_shape=[shape((lon, lon), BF16)] * 4,
        compiler_params=params(6),
        cost_estimate=cost(6 * lon**3, 12 * lon * lon),
        name="lon_covariance",
    )(lon_root)

    nchunks = levels * nmem
    inverse, value = pl.pallas_call(
        functools.partial(inverse_kernel, width, levels, lon, nlat_dev // 2),
        in_specs=[VM] * (nlat_dev // 2),
        out_specs=[VM] * 2,
        out_shape=[shape((nchunks, nlat // 2, quarter), jnp.int32), shape((nlat // 2, slots), F32)],
        scratch_shapes=[pltpu.VMEM((nlat // 2, slots), jnp.int32)],
        compiler_params=params(),
        cost_estimate=cost(10**10, 2 * nlat * lon * levels),
        name="inverse",
    )(*locals_)
    inverses, values = [inverse, swap(inverse, 1)], [value, swap(value, 1)]

    tall = half_count * levels * rows

    def apply(pays):
        first = pays is None
        outs = (
            [shape((rows, slots), F32)] * 2
            + [shape((nmem, levels, rows, quarter), F32)] * 2
            + [shape((tall, lon), BF16)] * 4
        )
        if not first:
            outs.append(shape((8, LANES), F32))
        return pl.pallas_call(
            functools.partial(apply_kernel, width, levels, nlat_dev, first),
            in_specs=[VM] * (nlat_dev // 2 + (0 if first else nlat_dev) + 12),
            out_specs=[VM] * len(outs),
            out_shape=outs,
            scratch_shapes=[pltpu.VMEM((half_count, nlat, slots), F32), pltpu.VMEM((nlat, slots), F32)]
            + [pltpu.VMEM((half_count, nlat, quarter), BF16)] * 4
            + [pltpu.VMEM((2 * tall, lon), BF16)] * 2,
            compiler_params=params(APPLY_LIMIT),
            cost_estimate=cost(12 * tall * lon * (nlat + lon), 30 * 2**20),
            name="apply_first" if first else "apply_next",
        )(
            *seens,
            *([] if first else pays),
            *values,
            *inverses,
            lhs_high,
            lhs_low,
            obs,
            obs_sib,
            cn_high,
            cn_low,
            members_mine,
            members_sib,
        )

    def to_quarters(image):
        total = image[0]
        for hop in range(1, nmem):
            total = total + lax.ppermute(image[hop], "mem", [(i, (i + hop) % nmem) for i in range(nmem)])
        return total

    def gradient(backs):
        field = (half_count, levels, rows, lon)
        other = product(backs[1], backs[3], lon_high, lon_low)
        mine = product(backs[0], backs[2], lon_high, lon_low)
        return mine.reshape(field), other.reshape(field)

    seen_own, seen_sib, image_own, image_sib, *backs0 = apply(None)
    seen_own = seen_own + swap(seen_sib, 1)
    parts = around_mem(seen_own)
    image_sib = swap(image_sib, 1)
    pay, seen0 = pl.pallas_call(
        functools.partial(answer_kernel, width, nmem),
        in_specs=[VM] * (nmem + 1),
        out_specs=[VM] * 2,
        out_shape=[shape((rows + 8, slots), F32), shape((rows, slots), F32)],
        compiler_params=params(),
        name="answer",
    )(*parts, obs)
    pays = direct(pay)
    mine0, other0 = gradient(backs0)
    pays = pays + [swap(block, 1) for block in pays]
    other0 = swap(other0, 1)
    quarter0 = to_quarters(image_own + image_sib)

    seen_own, seen_sib, image_own, image_sib, *backs1, length0 = apply(pays)
    seen_own = seen_own + swap(seen_sib, 1)
    parts = around_mem(seen_own)
    mine1, other1 = gradient(backs1)
    image_sib = swap(image_sib, 1)
    dots = pl.pallas_call(
        functools.partial(last_kernel, nmem),
        in_specs=[VM] * (nmem + 3),
        out_specs=VM,
        out_shape=shape((8, slots), F32),
        compiler_params=params(),
        name="last_dots",
    )(*parts, obs, seen0, length0)
    other1 = swap(other1, 1)
    quarter1 = to_quarters(image_own + image_sib)
    dots_parts = direct(dots)
    dots = sum(dots_parts[1:], dots_parts[0])
    dots = dots + swap(dots, 1)

    return pl.pallas_call(
        final_kernel,
        in_specs=[VM] * 8,
        out_specs=[VM, ANY],
        out_shape=[shape((levels, rows, quarter), F32), shape(members.shape, F32)],
        scratch_shapes=[pltpu.VMEM(members.shape, F32), pltpu.SemaphoreType.DMA((count,))],
        compiler_params=params(8),
        name="final",
    )(dots, length0, quarter0, quarter1, mine0, other0, mine1, other1)


def solution(mesh):
    return jax.shard_map(
        per_device,
        mesh=mesh,
        in_specs=(
            P("mem", None, "lat", None),
            P(),
            P(),
            P("lat", "mem"),
            P("lat", "mem"),
            P("lat", "mem"),
            P("lat", "mem"),
        ),
        out_specs=(P(None, "lat", "mem"), P("mem", None, "lat", None)),
        check_vma=False,
    )
```

```python
import functools
import jax
import jax.numpy as jnp
from jax import lax
from jax.experimental import pallas as pl
from jax.experimental.pallas import tpu as pltpu
from jax.sharding import PartitionSpec as P


LANES = 128
HIGHEST = lax.Precision.HIGHEST
F32 = jnp.float32
BF16 = jnp.bfloat16
MIB = 1024 * 1024
APPLY_LIMIT = 16


VM = pl.BlockSpec(memory_space=pltpu.VMEM)
ANY = pl.BlockSpec(memory_space=pl.ANY)


def params(limit=4):
    return pltpu.CompilerParams(vmem_limit_bytes=limit * MIB)


def cost(flops, nbytes):
    return pl.CostEstimate(flops=flops, bytes_accessed=nbytes, transcendentals=0)


def take_lanes(values, index):
    numbers = lax.GatherDimensionNumbers(
        offset_dims=(),
        collapsed_slice_dims=(1,),
        start_index_map=(1,),
        operand_batching_dims=(0,),
        start_indices_batching_dims=(0,),
    )
    return lax.gather(
        values, index[..., None], numbers, slice_sizes=(1, 1), mode=lax.GatherScatterMode.PROMISE_IN_BOUNDS
    )


def split(value):
    high = value.astype(BF16)
    return high, (value - high.astype(F32)).astype(BF16)


def lane_iota(rows):
    return lax.broadcasted_iota(jnp.int32, (rows, LANES), 1)


def dot(a, b):
    return jnp.dot(a, b, preferred_element_type=F32)


def sort_kernel(*refs):
    sources, (out_ref, cell, weight, value), scratch, sems = refs[:4], refs[4:8], refs[8:12], refs[12]
    copies = [
        pltpu.make_async_copy(source, target, sems.at[i])
        for i, (source, target) in enumerate(zip(sources, scratch))
    ]
    for copy in copies:
        copy.start()
    for copy in copies:
        copy.wait()
    cell_ref, weight_ref, mask_ref, innovation_ref = scratch
    rows, width = cell_ref.shape
    for padded in (cell, weight, value):
        padded[...] = jnp.zeros(padded.shape, padded.dtype)
    cell[:, :width] = cell_ref[...]
    used = weight_ref[...] * mask_ref[...].astype(F32)
    weight[:, :width] = used
    value[:, :width] = -(used * innovation_ref[...])
    lane = lane_iota(rows)
    key = cell[...] * width + lane % width
    block = 2
    while block <= width:
        hop = block // 2
        while hop:
            other = take_lanes(key, lane ^ hop)
            keep_low = ((lane & block) == 0) == ((lane & hop) == 0)
            if block == width:
                keep_low = (lane & hop) == 0
            key = jnp.where(keep_low, jnp.minimum(key, other), jnp.maximum(key, other))
            hop //= 2
        block *= 2
    slot = key % width
    per = LANES // width
    part = rows // per
    sorted_values = (
        (key // width).astype(F32),
        take_lanes(weight[...], slot),
        take_lanes(value[...], slot),
    )
    for kind, values in enumerate(sorted_values):
        values = jnp.where(lane < width, values, 0.0)
        total = values[:part]
        for side in range(1, per):
            total = total + pltpu.roll(values[side * part : (side + 1) * part], side * width, axis=1)
        out_ref[kind] = total


def run_totals(cells, values, width):
    hop = 1
    while hop < width:
        same = pltpu.roll(cells, LANES - hop, axis=1) == cells
        values = values + jnp.where(same, pltpu.roll(values, LANES - hop, axis=1), 0.0)
        hop *= 2
    return values


def pick_cells(cells, reads, width, levels, quarter, lon):
    per = LANES // width
    halves = quarter // LANES
    lane = lane_iota(cells.shape[0])
    position = cells % LANES
    kind = (cells // lon) * halves + (cells % quarter) // LANES
    outs = [jnp.zeros(cells.shape, F32) for _ in reads]
    for side in range(per):
        here = (lane // width) == side
        for level in range(levels):
            for half in range(halves):
                use = here & (kind == level * halves + half)
                outs = [
                    jnp.where(use, take_lanes(read(side, level, half), position), out)
                    for read, out in zip(reads, outs)
                ]
    return outs


def observe_kernel(width, nmem, *refs):
    block_refs = refs[:nmem]
    members_ref, obs_ref, local_ref, mine_ref, other_ref, members_mine_ref, members_other_ref, blocks = refs[nmem:]
    _, part, _ = block_refs[0].shape
    count, levels, rows, lon = members_ref.shape
    me = lax.axis_index("mem")
    parity = lax.axis_index("lat") % 2
    per = LANES // width
    quarter = lon // nmem
    for hop, ref in enumerate(block_refs):
        blocks[lax.rem(me - hop + nmem, nmem)] = ref[...]
    lane = lane_iota(part)
    for group in range(nmem // per):
        columns = slice(group * LANES, (group + 1) * LANES)
        for kind in range(3):
            for piece in range(per):
                total = jnp.zeros((part, LANES), F32)
                for side in range(per):
                    raw = blocks[group * per + side, kind]
                    turn = ((side - piece) * width) % LANES
                    if turn:
                        raw = pltpu.roll(raw, turn, axis=1)
                    total = jnp.where(lane // width == side, raw, total)
                obs_ref[kind, piece * part : (piece + 1) * part, columns] = total
        cells = obs_ref[0, :, columns].astype(jnp.int32)
        local_ref[0, :, columns] = obs_ref[0, :, columns]
        local_ref[1, :, columns] = run_totals(cells, obs_ref[2, :, columns], width)

    step = 8
    half_count = count // 2
    for i in range(half_count):
        members_mine_ref[i] = members_ref[parity * half_count + i]
        members_other_ref[i] = members_ref[(1 - parity) * half_count + i]

    def one(index, carry):
        start = pl.multiple_of(index * step, step)
        here = pl.ds(start, step)
        for group in range(nmem // per):
            columns = slice(group * LANES, (group + 1) * LANES)
            cells = obs_ref[0, here, columns].astype(jnp.int32)

            def reader(member):
                def read(side, level, half):
                    first = (group * per + side) * quarter + half * LANES
                    return members_ref[member, level, here, first : first + LANES]

                return read

            order = [parity * half_count + i for i in range(half_count)]
            order += [(1 - parity) * half_count + i for i in range(half_count)]
            outs = pick_cells(cells, [reader(member) for member in order], width, levels, quarter, lon)
            for i in range(half_count):
                mine_ref[i, here, columns] = outs[i]
                other_ref[i, here, columns] = outs[half_count + i]
        return carry

    lax.fori_loop(0, rows // step, one, 0)


def inverse_kernel(width, levels, lon, nblocks_lat, *refs):
    local_refs, (inverse_ref, value_ref, cells_all) = refs[:nblocks_lat], refs[nblocks_lat:]
    _, rows, slots = local_refs[0].shape
    nblocks = slots // width
    quarter = lon // nblocks
    per = LANES // width
    tall = 16
    for number in range(nblocks_lat):
        value_ref[number * rows : (number + 1) * rows, :] = local_refs[number][1]
        cells_all[number * rows : (number + 1) * rows, :] = local_refs[number][0].astype(jnp.int32)

    def one(index, carry):
        here = pl.ds(pl.multiple_of(index * tall, tall), tall)
        lane = lane_iota(tall)
        for block in range(nblocks):
            group, offset = block // per, (block % per) * width
            cells = cells_all[here, group * LANES : (group + 1) * LANES]
            nothing = (offset - 1) % LANES
            for level in range(levels):
                for half in range(quarter // LANES):
                    target = lane + (level * lon + block * quarter + half * LANES)
                    place = jnp.full((tall, LANES), offset, jnp.int32)
                    hop = width // 2
                    while hop:
                        place = jnp.where(take_lanes(cells, place + (hop - 1)) < target, place + hop, place)
                        hop //= 2
                    found = take_lanes(cells, place) == target
                    inverse_ref[level * nblocks + block, here, half * LANES : (half + 1) * LANES] = jnp.where(
                        found, place, nothing
                    )
        return carry

    lax.fori_loop(0, cells_all.shape[0] // tall, one, 0)


def apply_kernel(width, levels, nlat_blocks, first, *refs):
    seen_refs = refs[:nlat_blocks]
    refs = refs[nlat_blocks:]
    if not first:
        pay_refs = refs[:nlat_blocks]
        refs = refs[nlat_blocks:]
    value_refs, inverse_refs = refs[:2], refs[2:4]
    lhs_high_ref, lhs_low_ref, local_refs, cn_high_ref, cn_low_ref = refs[4], refs[5], refs[6:8], refs[8], refs[9]
    members_ref, members_sib_ref = refs[10], refs[11]
    refs = refs[12:]
    seen_out_refs, image_refs = refs[:2], refs[2:4]
    back_high_refs, back_low_refs = refs[4:6], refs[6:8]
    refs = refs[8:]
    if not first:
        length_ref = refs[0]
        refs = refs[1:]
    seen, value, xa_high, xa_low, xb_high, xb_low, w_high, w_low = refs
    count, nlat, slots = seen.shape
    rows = nlat // nlat_blocks
    wide = 2 * rows
    nblocks = slots // width
    per = LANES // width
    nchunks = levels * nblocks
    quarter = inverse_refs[0].shape[2]
    lon = quarter * nblocks
    me_mem = lax.axis_index("mem")
    members_refs = (members_ref, members_sib_ref)

    def rotated(block):
        return lax.rem(block - me_mem + nblocks, nblocks)

    for number, ref in enumerate(seen_refs):
        seen[:, number * rows : (number + 1) * rows, :] = ref[...]
    if first:
        for side, ref in enumerate(value_refs):
            value[side * (nlat // 2) : (side + 1) * (nlat // 2), :] = ref[...]
    else:
        top = jnp.zeros((1, slots), F32)
        bottom = jnp.zeros((1, slots), F32)
        for ref in pay_refs:
            top = top + ref[rows : rows + 1, :]
            bottom = bottom + ref[rows + 1 : rows + 2, :]
        length = jnp.sum(top, axis=1, keepdims=True) / jnp.sum(bottom, axis=1, keepdims=True)
        length_ref[...] = jnp.broadcast_to(length, length_ref.shape)
        per_side = nlat_blocks // 2
        for number, ref in enumerate(pay_refs):
            inside = (number % per_side) * rows
            old = value_refs[number // per_side][inside : inside + rows, :]
            value[number * rows : (number + 1) * rows, :] = old - length * (old + ref[:rows, :])

    tall = 16
    lane = lane_iota(tall)

    def build(chunk, x_high, x_low):
        block = lax.rem(chunk, nblocks)
        offset = lax.rem(block, per) * width
        columns = pl.ds(pl.multiple_of((block // per) * LANES, LANES), LANES)
        inside = (lane >= offset) & (lane < offset + width)
        for start in range(0, nlat, tall):
            part = slice(start, start + tall)
            numbers = value[part, columns]
            sources = [jnp.where(inside, seen[m, part, columns] * numbers, 0.0) for m in range(count)]
            for half in range(quarter // LANES):
                cols = slice(half * LANES, (half + 1) * LANES)
                inner = start % (nlat // 2)
                index = inverse_refs[start // (nlat // 2)][chunk, inner : inner + tall, cols]
                for m in range(count):
                    high, low = split(take_lanes(sources[m], index))
                    x_high[m, part, cols] = high
                    x_low[m, part, cols] = low

    def multiply(chunk, x_high, x_low):
        level = chunk // nblocks
        cols = pl.ds(pl.multiple_of(lax.rem(chunk, nblocks) * quarter, quarter), quarter)
        for m in range(count):
            both = (
                dot(lhs_high_ref[...], x_high[m])
                + dot(lhs_low_ref[...], x_high[m])
                + dot(lhs_high_ref[...], x_low[m])
            )
            high, low = split(both[:wide])
            where = pl.ds(pl.multiple_of((m * levels + level) * wide, wide), wide)
            w_high[where, cols] = high
            w_low[where, cols] = low
            where = pl.ds(pl.multiple_of((m * levels + level) * rows, rows), rows)
            for side in range(2):
                high, low = split(both[wide + side * rows : wide + (side + 1) * rows])
                back_high_refs[side][where, cols] = high
                back_low_refs[side][where, cols] = low

    build(0, xa_high, xa_low)

    def one(pair, carry):
        chunk = pair * 2
        build(chunk + 1, xb_high, xb_low)
        multiply(chunk, xa_high, xa_low)
        build(jnp.minimum(chunk + 2, nchunks - 1), xa_high, xa_low)
        multiply(chunk + 1, xb_high, xb_low)
        return carry

    lax.fori_loop(0, nchunks // 2, one, 0)

    tile = 2 * LANES
    deep = levels * wide

    def panel(column, carry):
        begin = column * tile
        cols = pl.ds(pl.multiple_of(begin, tile), tile)
        place = rotated(begin // quarter)
        inner = pl.ds(pl.multiple_of(lax.rem(begin, quarter), tile), tile)
        totals = [[None] * levels for _ in range(2)]
        for member in range(count):
            part = slice(member * deep, (member + 1) * deep)
            product = (
                dot(w_high[part, :], cn_high_ref[:, cols])
                + dot(w_low[part, :], cn_high_ref[:, cols])
                + dot(w_high[part, :], cn_low_ref[:, cols])
            )
            for level in range(levels):
                for side in range(2):
                    top = level * wide + side * rows
                    term = members_refs[side][member, level, :, cols] * product[top : top + rows]
                    old = totals[side][level]
                    totals[side][level] = term if old is None else old + term
        for side in range(2):
            for level in range(levels):
                image_refs[side][place, level, :, inner] = totals[side][level]
        return carry

    lax.fori_loop(0, lon // tile, panel, 0)

    step = 8
    for side in range(2):
        for start in range(0, rows, step):
            part = slice(start, start + step)
            for group in range(nblocks // per):
                columns = slice(group * LANES, (group + 1) * LANES)
                cells = local_refs[side][0, part, columns].astype(jnp.int32)

                def read(piece, level, half):
                    return image_refs[side][
                        rotated(group * per + piece), level, part, half * LANES : (half + 1) * LANES
                    ]

                seen_out_refs[side][part, columns] = pick_cells(cells, [read], width, levels, quarter, lon)[0]


def answer_kernel(width, nparts, *refs):
    parts, (obs_ref, pay_ref, seen_ref) = refs[:nparts], refs[nparts:]
    rows = obs_ref.shape[1]
    seen = parts[0][...]
    for part in parts[1:]:
        seen = seen + part[...]
    seen_ref[...] = seen
    weighted = obs_ref[1] * seen
    value = obs_ref[2]
    for group in range(seen.shape[1] // LANES):
        columns = slice(group * LANES, (group + 1) * LANES)
        cells = obs_ref[0, :, columns].astype(jnp.int32)
        pay_ref[:rows, columns] = run_totals(cells, weighted[:, columns], width)
    pay_ref[rows:, :] = jnp.zeros((8, seen.shape[1]), F32)
    pay_ref[rows : rows + 1, :] = jnp.sum(value * seen, axis=0, keepdims=True)
    pay_ref[rows + 1 : rows + 2, :] = jnp.sum(seen * (value + weighted), axis=0, keepdims=True)


def last_kernel(nparts, *refs):
    parts, (obs_ref, before_ref, length_ref, dots_ref) = refs[:nparts], refs[nparts:]
    seen = parts[0][...]
    for part in parts[1:]:
        seen = seen + part[...]
    weight, value = obs_ref[1], obs_ref[2]
    length = length_ref[:1, :1]
    value = value - length * (value + weight * before_ref[...])
    dots_ref[...] = jnp.zeros(dots_ref.shape, F32)
    dots_ref[:1, :] = jnp.sum(value * seen, axis=0, keepdims=True)
    dots_ref[1:2, :] = jnp.sum(seen * (value + weight * seen), axis=0, keepdims=True)


def lat_kernel(order, root_ref, high_ref, low_ref, turned, chip, columns, ordered):
    rows = chip.shape[0] // 2
    me = lax.axis_index("lat")
    turned[...] = root_ref[...].T
    for side in range(2):
        here = pl.ds(pl.multiple_of((me ^ side) * rows, rows), rows)
        chip[side * rows : (side + 1) * rows, :] = root_ref[here, :]
        columns[side * rows : (side + 1) * rows, :] = turned[here, :]
    covariance = lax.dot_general(
        chip[...], root_ref[...], (((1,), (1,)), ((), ())), precision=HIGHEST, preferred_element_type=F32
    )
    both = jnp.concatenate([covariance, columns[...]]).T
    turned[:, : both.shape[1]] = both
    for number, bits in enumerate(order):
        here = pl.ds(pl.multiple_of((me ^ bits) * rows, rows), rows)
        ordered[number * rows : (number + 1) * rows, :] = turned[here, : both.shape[1]]
    high_ref[...], low_ref[...] = split(ordered[...].T)


def covariance_kernel(root_ref, high_ref, low_ref, root_high_ref, root_low_ref):
    tile = 2 * LANES
    numbers = (((1,), (1,)), ((), ()))
    root_high_ref[...], root_low_ref[...] = split(root_ref[...])

    def times(a, b):
        return lax.dot_general(a, b, numbers, preferred_element_type=F32)

    def panel(column, carry):
        here = pl.ds(pl.multiple_of(column * tile, tile), tile)
        high, low = root_high_ref[here, :], root_low_ref[here, :]
        total = times(root_high_ref[...], high) + times(root_low_ref[...], high) + times(root_high_ref[...], low)
        high_ref[:, here], low_ref[:, here] = split(total)
        return carry

    lax.fori_loop(0, root_ref.shape[0] // tile, panel, 0)


def product_kernel(a_high_ref, a_low_ref, b_high_ref, b_low_ref, out_ref):
    tile = 2 * LANES

    def panel(column, carry):
        here = pl.ds(pl.multiple_of(column * tile, tile), tile)
        out_ref[:, here] = (
            dot(a_high_ref[...], b_high_ref[:, here])
            + dot(a_low_ref[...], b_high_ref[:, here])
            + dot(a_high_ref[...], b_low_ref[:, here])
        )
        return carry

    lax.fori_loop(0, b_high_ref.shape[1] // tile, panel, 0)


def product(a_high, a_low, b_high, b_low):
    rows, deep = a_high.shape
    wide = b_high.shape[1]
    return pl.pallas_call(
        product_kernel,
        in_specs=[VM] * 4,
        out_specs=VM,
        out_shape=jax.ShapeDtypeStruct((rows, wide), F32),
        compiler_params=params(6),
        cost_estimate=cost(6 * rows * deep * wide, 4 * (rows * deep + deep * wide + rows * wide)),
        name="lon_product",
    )(a_high, a_low, b_high, b_low)


def final_kernel(dots_ref, length_ref, q0_ref, q1_ref, a0_ref, b0_ref, a1_ref, b1_ref,
                 increment_ref, control_ref, control, sems):
    parity = lax.axis_index("lat") % 2
    half = a0_ref.shape[0]
    length0 = length_ref[:1, :1]
    length1 = jnp.sum(dots_ref[:1, :], axis=1, keepdims=True) / jnp.sum(dots_ref[1:2, :], axis=1, keepdims=True)
    copies = []
    for side, (first_ref, second_ref) in enumerate(((a0_ref, a1_ref), (b0_ref, b1_ref))):
        for i in range(half):
            number = side * half + i
            member = (parity ^ side) * half + i
            control[number] = -(length0 * first_ref[i] + length1 * second_ref[i])
            copies.append(pltpu.make_async_copy(control.at[number], control_ref.at[member], sems.at[number]))
            copies[-1].start()
    increment_ref[...] = -(length0 * q0_ref[...] + length1 * q1_ref[...])
    for copy in copies:
        copy.wait()


def per_device(members, lat_root, lon_root, innovation, obs_weight, obs_mask, obs_cell):
    count, levels, rows, lon = members.shape
    half_count = count // 2
    nmem, nlat_dev = lax.axis_size("mem"), lax.axis_size("lat")
    nlat = lat_root.shape[0]
    width = obs_cell.shape[1]
    slots = width * nmem
    quarter = lon // nmem
    shape = jax.ShapeDtypeStruct
    chips = list(range(0, nlat_dev, 2))
    order = chips + [bits + 1 for bits in chips]
    steps = [2**k for k in range(1, (nlat_dev - 1).bit_length())]

    def swap(value, bits):
        return lax.ppermute(value, "lat", [(i, i ^ bits) for i in range(nlat_dev)])

    def direct(value):
        return [value] + [swap(value, bits) for bits in chips[1:]]

    def relayed(value, hops):
        blocks = {0: value}
        for hop in hops:
            arrived = {}
            for bits, block in blocks.items():
                arrived[bits ^ hop] = swap(block, hop)
            blocks.update(arrived)
        return [blocks[bits] for bits in chips]

    def around_mem(value):
        return [value] + [
            lax.ppermute(value, "mem", [(i, (i + hop) % nmem) for i in range(nmem)]) for hop in range(1, nmem)
        ]

    block = pl.pallas_call(
        sort_kernel,
        in_specs=[ANY] * 4,
        out_specs=VM,
        out_shape=shape((3, rows * width // LANES, LANES), F32),
        scratch_shapes=[pltpu.VMEM((rows, LANES), jnp.int32)]
        + [pltpu.VMEM((rows, LANES), F32)] * 2
        + [pltpu.VMEM(value.shape, value.dtype) for value in (obs_cell, obs_weight, obs_mask, innovation)]
        + [pltpu.SemaphoreType.DMA((4,))],
        compiler_params=params(2),
        name="sort_slots",
    )(obs_cell, obs_weight, obs_mask, innovation)
    blocks = around_mem(block)
    obs, local, mine, other, members_mine, members_sib = pl.pallas_call(
        functools.partial(observe_kernel, width, nmem),
        in_specs=[VM] * (nmem + 1),
        out_specs=[VM] * 6,
        out_shape=[
            shape((3, rows, slots), F32),
            shape((2, rows, slots), F32),
            shape((half_count, rows, slots), F32),
            shape((half_count, rows, slots), F32),
            shape((half_count, levels, rows, lon), F32),
            shape((half_count, levels, rows, lon), F32),
        ],
        scratch_shapes=[pltpu.VMEM((nmem, *block.shape), F32)],
        compiler_params=params(),
        cost_estimate=cost(10**8, 4 * members.size),
        name="members_at_slots",
    )(*blocks, members)

    locals_ = direct(local)
    received = swap(other, 1)
    seens = relayed(mine, steps) + relayed(received, steps[::-1])
    obs_sib = swap(obs, 1)
    members_sib = swap(members_sib, 1)

    lhs_high, lhs_low = pl.pallas_call(
        functools.partial(lat_kernel, order),
        in_specs=[VM],
        out_specs=[VM] * 2,
        out_shape=[shape((4 * rows, nlat), BF16)] * 2,
        scratch_shapes=[
            pltpu.VMEM((nlat, nlat), F32),
            pltpu.VMEM((2 * rows, nlat), F32),
            pltpu.VMEM((2 * rows, nlat), F32),
            pltpu.VMEM((nlat, 4 * rows), F32),
        ],
        compiler_params=params(),
        cost_estimate=cost(3 * 10**9, 8 * nlat * nlat),
        name="lat_rows",
    )(lat_root)
    cn_high, cn_low, lon_high, lon_low = pl.pallas_call(
        covariance_kernel,
        in_specs=[VM],
        out_specs=[VM] * 4,
        out_shape=[shape((lon, lon), BF16)] * 4,
        compiler_params=params(6),
        cost_estimate=cost(6 * lon**3, 12 * lon * lon),
        name="lon_covariance",
    )(lon_root)

    nchunks = levels * nmem
    inverse, value = pl.pallas_call(
        functools.partial(inverse_kernel, width, levels, lon, nlat_dev // 2),
        in_specs=[VM] * (nlat_dev // 2),
        out_specs=[VM] * 2,
        out_shape=[shape((nchunks, nlat // 2, quarter), jnp.int32), shape((nlat // 2, slots), F32)],
        scratch_shapes=[pltpu.VMEM((nlat // 2, slots), jnp.int32)],
        compiler_params=params(),
        cost_estimate=cost(10**10, 2 * nlat * lon * levels),
        name="inverse",
    )(*locals_)
    inverses, values = [inverse, swap(inverse, 1)], [value, swap(value, 1)]

    tall = half_count * levels * rows

    def apply(pays):
        first = pays is None
        outs = (
            [shape((rows, slots), F32)] * 2
            + [shape((nmem, levels, rows, quarter), F32)] * 2
            + [shape((tall, lon), BF16)] * 4
        )
        if not first:
            outs.append(shape((8, LANES), F32))
        return pl.pallas_call(
            functools.partial(apply_kernel, width, levels, nlat_dev, first),
            in_specs=[VM] * (nlat_dev * (1 if first else 2) + 12),
            out_specs=[VM] * len(outs),
            out_shape=outs,
            scratch_shapes=[pltpu.VMEM((half_count, nlat, slots), F32), pltpu.VMEM((nlat, slots), F32)]
            + [pltpu.VMEM((half_count, nlat, quarter), BF16)] * 4
            + [pltpu.VMEM((2 * tall, lon), BF16)] * 2,
            compiler_params=params(APPLY_LIMIT),
            cost_estimate=cost(12 * tall * lon * (nlat + lon), 30 * 2**20),
            name="apply_first" if first else "apply_next",
        )(
            *seens,
            *([] if first else pays),
            *values,
            *inverses,
            lhs_high,
            lhs_low,
            obs,
            obs_sib,
            cn_high,
            cn_low,
            members_mine,
            members_sib,
        )

    def to_quarters(image):
        total = image[0]
        for hop in range(1, nmem):
            total = total + lax.ppermute(image[hop], "mem", [(i, (i + hop) % nmem) for i in range(nmem)])
        return total

    def gradient(backs):
        field = (half_count, levels, rows, lon)
        other = product(backs[1], backs[3], lon_high, lon_low)
        mine = product(backs[0], backs[2], lon_high, lon_low)
        return mine.reshape(field), other.reshape(field)

    seen_own, seen_sib, image_own, image_sib, *backs0 = apply(None)
    seen_own = seen_own + swap(seen_sib, 1)
    parts = around_mem(seen_own)
    image_sib = swap(image_sib, 1)
    pay, seen0 = pl.pallas_call(
        functools.partial(answer_kernel, width, nmem),
        in_specs=[VM] * (nmem + 1),
        out_specs=[VM] * 2,
        out_shape=[shape((rows + 8, slots), F32), shape((rows, slots), F32)],
        compiler_params=params(),
        name="answer",
    )(*parts, obs)
    pays = direct(pay)
    mine0, other0 = gradient(backs0)
    pays = pays + [swap(block, 1) for block in pays]
    other0 = swap(other0, 1)
    quarter0 = to_quarters(image_own + image_sib)

    seen_own, seen_sib, image_own, image_sib, *backs1, length0 = apply(pays)
    seen_own = seen_own + swap(seen_sib, 1)
    parts = around_mem(seen_own)
    mine1, other1 = gradient(backs1)
    image_sib = swap(image_sib, 1)
    dots = pl.pallas_call(
        functools.partial(last_kernel, nmem),
        in_specs=[VM] * (nmem + 3),
        out_specs=VM,
        out_shape=shape((8, slots), F32),
        compiler_params=params(),
        name="last_dots",
    )(*parts, obs, seen0, length0)
    other1 = swap(other1, 1)
    quarter1 = to_quarters(image_own + image_sib)
    dots_parts = direct(dots)
    dots = sum(dots_parts[1:], dots_parts[0])
    dots = dots + swap(dots, 1)

    return pl.pallas_call(
        final_kernel,
        in_specs=[VM] * 8,
        out_specs=[VM, ANY],
        out_shape=[shape((levels, rows, quarter), F32), shape(members.shape, F32)],
        scratch_shapes=[pltpu.VMEM(members.shape, F32), pltpu.SemaphoreType.DMA((count,))],
        compiler_params=params(8),
        name="final",
    )(dots, length0, quarter0, quarter1, mine0, other0, mine1, other1)


def solution(mesh):
    return jax.shard_map(
        per_device,
        mesh=mesh,
        in_specs=(
            P("mem", None, "lat", None),
            P(),
            P(),
            P("lat", "mem"),
            P("lat", "mem"),
            P("lat", "mem"),
            P("lat", "mem"),
        ),
        out_specs=(P(None, "lat", "mem"), P("mem", None, "lat", None)),
        check_vma=False,
    )
```
